32 devices in a mesh: sky: 8 (over z, y), band: 4 (over x, core).
Axes of the slice: x: 2, y: 2, z: 4, core: 2. Of those that a mesh axis runs over, the one named last changes fastest.
Arguments:
- magnitudes: float32 [4, 8, 16384], P('band', None, 'sky'), may hold values from -7 to 7
- weights: float32 [4, 8, 16384], P('band', None, 'sky'), may hold values from 0.25 to 4
- slots: int32 [4, 8, 16384], P('band', None, 'sky'), may hold values from 0 to 31, as said below
- block_fields: int32 [64, 32], P('sky'), may hold values from 0 to 4096, as said below
- owner: int32 [4096], replicated, may hold values from 0 to 7, as said below
- colors: int32 [4096], replicated, may hold values from 0 to 7
- color_terms: float32 [4, 4], replicated, may hold values from -0.25 to 0.25
Outputs:
- zero_points: float32 [4, 4096], P('band', 'sky')
- star_mags: float32 [4, 16384], P('band', 'sky')
- misfit: float32 [4, 4], P(None, 'band')
The draws below stay inside these ranges and needn't reach their ends.
Inputs may be any that keep to these rules, and one draw needn't show every extreme that they name: `block_fields`: the live entries of each list come first, are distinct, and name fields owned by the block's own sky tile or by the tiles one index below or above it, cyclically over 8 tiles; the remaining entries equal 4096. A list holds 16 or more live entries, and every tile has a block with all 32 live. `owner`: each sky tile owns exactly 512 fields. `slots`: each observation names a live entry of its block's list.
All inputs are finite; a program needn't handle non-finite values.
Results may differ from the reference program's by a relative error of at most 0.00023.
Values sent between devices are 32-bit elements; how exact they have to be, the bound alone decides.
A program may use at most 64 MiB of HBM per device.

```python
import math
import jax
import jax.numpy as jnp
from jax import lax

F = 4096
COLORS = 8
SWEEPS = 4
OBS = 8
LIST = 32
ROWS = 256
BLK_DEV = 8
NBANDS = 4
TILES = 8
F_OWN = 512
NBLOCKS = 64
NSTARS = 16384


def layout(key):
    permuted = jax.random.permutation(jax.random.fold_in(key, 1), F)
    owner = (permuted // F_OWN).astype(jnp.int32)
    inverse = jnp.argsort(permuted, stable=True)
    tile_of = jnp.arange(NBLOCKS) // BLK_DEV
    offsets = jnp.arange(3 * F_OWN)
    nearby = (tile_of[:, None] + offsets[None, :] // F_OWN - 1) % TILES * F_OWN + offsets[None, :] % F_OWN
    candidates = inverse[nearby]
    pick_keys = jax.random.split(jax.random.fold_in(key, 2), NBLOCKS)
    shuffles = jax.vmap(lambda block_key: jax.random.permutation(block_key, 3 * F_OWN))(pick_keys)[:, :LIST]
    picked = jnp.take_along_axis(candidates, shuffles, axis=1)
    live_count = jax.random.randint(jax.random.fold_in(key, 3), (NBLOCKS,), LIST // 2, LIST + 1)
    full_block = tile_of * BLK_DEV + tile_of * 5 % BLK_DEV
    live_count = live_count.at[full_block].set(LIST)
    lists = jnp.where(jnp.arange(LIST)[None, :] < live_count[:, None], picked, F).astype(jnp.int32)
    raw_bits = jax.random.randint(jax.random.fold_in(key, 4), (NBANDS, OBS, NSTARS), 0, 1 << 20)
    star_live = jnp.repeat(live_count, ROWS)
    slot_values = (raw_bits % star_live[None, None, :]).astype(jnp.int32)
    return (owner, lists, slot_values)


def draw_block_fields(key, part):
    return layout(key)[1]


def draw_owner(key, part):
    return layout(key)[0]


def draw_slots(key, part):
    return layout(key)[2]


def draw_magnitudes(key, part):
    owner, lists, slot_values = layout(key)
    expanded = jnp.broadcast_to(lists[None, None, :, :], (NBANDS, OBS, NBLOCKS, LIST))
    field_ids = jnp.take_along_axis(expanded, slot_values.reshape(NBANDS, OBS, NBLOCKS, ROWS), axis=3).reshape(NBANDS, OBS, NSTARS)
    star_tint = jax.random.uniform(jax.random.fold_in(key, 11), (NSTARS,), jnp.float32, -1.0, 1.0)
    band_slope = jax.random.uniform(jax.random.fold_in(key, 12), (NBANDS,), jnp.float32, -1.0, 1.0)
    base_mag = jax.random.uniform(jax.random.fold_in(key, 13), (NSTARS,), jnp.float32, -3.0, 3.0)
    field_off = jax.random.uniform(jax.random.fold_in(key, 14), (NBANDS, F), jnp.float32, -1.0, 1.0)
    noise_term = 0.05 * jnp.clip(jax.random.normal(jax.random.fold_in(key, 15), (NBANDS, OBS, NSTARS), jnp.float32), -2.0, 2.0)
    star_part = base_mag[None, :] + band_slope[:, None] * star_tint[None, :]
    field_part = jax.vmap(jnp.take)(field_off, field_ids)
    return (star_part[:, None, :] + field_part + noise_term).astype(jnp.float32)


def place_ends(result, own_key, least, largest):
    place = [jax.random.randint(jax.random.fold_in(own_key, axis), (), 0, length) for axis, length in enumerate(result.shape)]
    widest = result.shape.index(max(result.shape))
    next_to = place[:widest] + [(place[widest] + 1) % result.shape[widest]] + place[widest + 1:]
    return result.at[tuple(place)].set(least).at[tuple(next_to)].set(largest)


def block_scale(stream_key, extent, cuts, smallest, largest):
    gain, own = 1.0, jax.random.fold_in(stream_key, 6)
    for position, blocks in cuts:
        draws = jnp.exp(jax.random.uniform(jax.random.fold_in(own, position), (blocks,), jnp.float32, smallest / len(cuts), largest / len(cuts)))
        gain = gain * jnp.repeat(draws, extent[position] // blocks).reshape([-1 if axis == position else 1 for axis in range(len(extent))])
    return gain


def setup_inputs(seed: int = 0) -> dict:
    seeds = jax.random.split(jax.random.key(seed), 8)
    magnitudes = draw_magnitudes(jax.random.fold_in(seeds[7], 71), 0)
    weights = jnp.clip(jnp.exp(math.log(4.0) - 2.7725887 * jax.random.uniform(seeds[1], (NBANDS, OBS, NSTARS), jnp.float32) ** block_scale(seeds[1], (NBANDS, OBS, NSTARS), ((0, 4), (2, 8)), -0.2, 0.2)), 0.25, 4.0)
    slots = draw_slots(jax.random.fold_in(seeds[7], 71), 0)
    block_fields = draw_block_fields(jax.random.fold_in(seeds[7], 71), 0)
    owner = draw_owner(jax.random.fold_in(seeds[7], 71), 0)
    colors = place_ends(jax.random.randint(seeds[5], (F,), 0, COLORS), jax.random.fold_in(seeds[5], 1), 0, COLORS - 1).astype(jnp.int32)
    color_terms = jnp.clip(jax.random.uniform(seeds[6], (NBANDS, NBANDS), jnp.float32, -0.25, 0.25), -0.25, 0.25)
    return {"magnitudes": magnitudes, "weights": weights, "slots": slots, "block_fields": block_fields, "owner": owner, "colors": colors, "color_terms": color_terms}


PRIOR_WEIGHT = 1.0


def field_table(block_fields, slots):
    band_count, obs_count, star_count = slots.shape
    block_count, list_len = block_fields.shape
    block_rows = star_count // block_count
    block_slots = slots.reshape(band_count, obs_count, block_count, block_rows)
    expanded = jnp.broadcast_to(block_fields[None, None, :, :], (band_count, obs_count, block_count, list_len))
    picked = jnp.take_along_axis(expanded, block_slots, axis=3)
    return picked.reshape(band_count, obs_count, star_count).astype(jnp.int32)


def reference(magnitudes, weights, slots, block_fields, owner, colors, color_terms):
    band_count, obs_count, star_count = magnitudes.shape
    fields = owner.shape[0]
    field_ids = field_table(block_fields, slots)
    star_weight = jnp.sum(weights, axis=1)

    def segment_one(band_values, band_ids):
        return jax.ops.segment_sum(band_values.reshape(-1), band_ids.reshape(-1), num_segments=fields)

    def field_sums(values):
        return jax.vmap(segment_one)(values, field_ids)

    denominators = field_sums(weights) + PRIOR_WEIGHT
    mixing = jnp.eye(band_count, dtype=jnp.float32) + color_terms - jnp.diag(jnp.sum(color_terms, axis=1))

    def predict(zero_pts):
        zp_obs = jax.vmap(jnp.take)(zero_pts, field_ids)
        star_means = jnp.sum(weights * (magnitudes - zp_obs), axis=1) / star_weight
        predicted = jnp.dot(mixing, star_means, precision=lax.Precision.HIGHEST)
        return zp_obs, star_means, predicted

    zero_pts = jnp.zeros((band_count, fields), jnp.float32)
    misfits = []
    for sweep_no in range(SWEEPS):
        for color_no in range(COLORS):
            zp_obs, star_means, predicted = predict(zero_pts)
            residual = magnitudes - predicted[:, None, :]
            if color_no == 0 and sweep_no > 0:
                misfits.append(jnp.sum(weights * (residual - zp_obs) ** 2, axis=(1, 2)))
            updated = field_sums(weights * residual) / denominators
            zero_pts = jnp.where((colors == color_no)[None, :], updated, zero_pts)
    zp_obs, star_means, predicted = predict(zero_pts)
    residual = magnitudes - predicted[:, None, :]
    misfits.append(jnp.sum(weights * (residual - zp_obs) ** 2, axis=(1, 2)))
    misfit = jnp.stack(misfits) / (obs_count * star_count)
    owner_order = jnp.argsort(owner, stable=True)
    return jnp.take(zero_pts, owner_order, axis=1), star_means, misfit
```

```python
import functools

import jax
import jax.numpy as jnp
from jax import lax
from jax.experimental import pallas as pl
from jax.experimental.pallas import tpu as pltpu
from jax.sharding import PartitionSpec as P

COLORS = 8
SWEEPS = 4
PRIOR_WEIGHT = 1.0
REACH = 2
HIGHEST = lax.Precision.HIGHEST
LANES = 128
EXTRA = 8
MESH = pl.DeviceIdType.MESH


def contract_lanes(left, right):
    dims = (((1,), (1,)), ((), ()))
    return lax.dot_general(left, right, dims, precision=HIGHEST, preferred_element_type=jnp.float32)


def couple_kernel(bands, obs, list_len, rows, mix_ref, mix_grid_ref, data_ref, places_ref, out_ref):
    blocks = data_ref.shape[3] // rows
    full = []
    entry = lax.broadcasted_iota(jnp.int32, (list_len, rows), 0)
    for block in range(blocks):
        cols = pl.ds(block * rows, rows)
        one_hot, one_hot_mag, star_weight, means = [], [], [], []
        for band in range(bands):
            mags = data_ref[band, 0, :, cols]
            wts = data_ref[band, 1, :, cols]
            slots = places_ref[band, :, cols]
            scaled = wts * mags
            weight_sum = jnp.sum(wts, axis=0, keepdims=True)
            star_weight.append(weight_sum)
            means.append(jnp.sum(scaled, axis=0, keepdims=True) / weight_sum)
            hot = jnp.zeros((list_len, rows), jnp.float32)
            hot_mag = jnp.zeros((list_len, rows), jnp.float32)
            for k in range(obs):
                hit = slots[k : k + 1] == entry
                hot = hot + jnp.where(hit, wts[k : k + 1], 0.0)
                hot_mag = hot_mag + jnp.where(hit, scaled[k : k + 1], 0.0)
            one_hot.append(hot)
            one_hot_mag.append(hot_mag)
        rest = []
        shares = []
        for band in range(bands):
            predicted = mix_ref[band, 0] * means[0]
            for other in range(1, bands):
                predicted = predicted + mix_ref[band, other] * means[other]
            rest.append(one_hot_mag[band] - one_hot[band] * predicted)
            shares.append(one_hot[band] / star_weight[band])
        hot_all = jnp.concatenate(one_hot, axis=0)
        share_all = jnp.concatenate(shares, axis=0)
        rest_all = jnp.concatenate(rest, axis=0)
        coupling = contract_lanes(share_all, hot_all) * mix_grid_ref[...]
        ones = jnp.ones((8, rows), jnp.float32)
        rest_row = contract_lanes(ones, rest_all)
        weight_row = contract_lanes(ones, hot_all)
        first = lax.broadcasted_iota(jnp.int32, (EXTRA, LANES), 0) == 0
        full.append(jnp.concatenate([coupling, jnp.where(first, rest_row, weight_row)], axis=0))
    split = bands // 2
    for part in range(split):
        pieces = []
        for half in range(2):
            band = half * split + part
            for block in range(blocks):
                pieces.append(full[block][:, band * list_len : (band + 1) * list_len])
        out_ref[part] = jnp.concatenate(pieces, axis=1)


def sweep_kernel(
    bands, list_len, row_count,
    coupled_ref, pick_ref, color_ref,
    out_ref, kt, base, tot, rden, zp, move, stage, sems, window,
):
    groups = row_count // 8
    pack = LANES // list_len
    split = bands // 2
    levels, places = pick_ref.shape[:2]
    depth = stage.shape[0]
    lane = lax.broadcasted_iota(jnp.int32, (8, LANES), 1)
    lane_wide = lax.broadcasted_iota(jnp.int32, (LANES + EXTRA, LANES), 1)

    def fetch(row, slot):
        return pltpu.make_async_copy(
            coupled_ref.at[pl.ds(row * (2 * split), 2 * split)], stage.at[slot], sems.at[slot]
        )

    for row in range(depth - 1):
        fetch(row, row).start()

    def unpack(row, carry):
        slot = lax.rem(row, depth)
        ahead = row + depth - 1

        @pl.when(ahead < row_count)
        def _():
            fetch(ahead, lax.rem(ahead, depth)).start()

        fetch(row, slot).wait()
        group = lax.div(row, 8)
        place = lax.rem(row, 8)
        for part in range(split):
            left = stage[slot, part]
            right = stage[slot, split + part]
            low = jnp.where(lane_wide < LANES // 2, left, pltpu.roll(right, LANES // 2, 1))
            high = jnp.where(lane_wide < LANES // 2, pltpu.roll(left, LANES // 2, 1), right)
            for band, value in ((part, low), (split + part, high)):
                start = (group * bands + band) * (LANES * 8) + place
                kt[pl.ds(start, LANES, stride=8), :] = value[0:LANES]
                base[band, pl.ds(row, 1), :] = value[LANES : LANES + 1]
                tot[band, pl.ds(row + 8, 1), :] = value[LANES + 1 : LANES + 2]
        return carry

    lax.fori_loop(0, row_count, unpack, 0)

    def rows_of(group):
        return pl.ds(pl.multiple_of(group * 8, 8), 8)

    def wrap():
        for band in range(bands):
            tot[band, 0:8, :] = tot[band, row_count : row_count + 8, :]
            tot[band, row_count + 8 : row_count + 16, :] = tot[band, 8:16, :]

    def gather(group, first, count, sums):
        for place in range(places):
            start = group * 8 + (8 + place - places // 2)
            near = [tot[band, pl.ds(start, 8), :] for band in range(bands)]
            for level in range(count):
                pick = pick_ref[first + level, place, rows_of(group), :]
                mask = pick < LANES
                lanes = pick & (LANES - 1)
                for band in range(bands):
                    index = 2 * band + level % 2
                    sums[index] = sums[index] + jnp.where(mask, take(near[band], lanes), 0.0)
        return sums

    def gathered(group):
        sums = []
        for band in range(bands):
            sums += [tot[band, pl.ds(pl.multiple_of(group * 8 + 8, 8), 8), :], jnp.zeros((8, LANES), jnp.float32)]
        sums = gather(group, 0, 2, sums)
        sums = lax.fori_loop(2, window[2 * COLORS], lambda level, sums: gather(group, level, 1, sums), sums)
        return [sums[2 * band] + sums[2 * band + 1] for band in range(bands)]

    position = (lane & (list_len - 1)).astype(jnp.float32)
    for color_no in range(COLORS):
        low = jnp.full((8, LANES), float(list_len), jnp.float32)
        high = jnp.zeros((8, LANES), jnp.float32)
        for group in range(groups):
            now = color_ref[group * 8 : group * 8 + 8, :] == color_no
            low = jnp.minimum(low, jnp.where(now, position, float(list_len)))
            high = jnp.maximum(high, jnp.where(now, position + 1.0, 0.0))
        window[2 * color_no] = jnp.min(low).astype(jnp.int32)
        window[2 * color_no + 1] = jnp.max(high).astype(jnp.int32)
    deepest = jnp.int32(2)
    for level in range(2, levels):
        def least(index, value, level=level):
            place, group = lax.div(index, groups), lax.rem(index, groups)
            return jnp.minimum(value, pick_ref[level, place, rows_of(group), :])
        found = lax.fori_loop(0, places * groups, least, jnp.full((8, LANES), LANES, jnp.int32))
        some = jnp.min(found.astype(jnp.float32)) < LANES
        deepest = jnp.where(some, level + 1, deepest)
    window[2 * COLORS] = deepest

    def weigh(group, carry):
        for band, value in enumerate(gathered(group)):
            rden[band, rows_of(group), :] = 1.0 / (value + PRIOR_WEIGHT)
        return carry

    wrap()
    lax.fori_loop(0, groups, weigh, 0)
    zp[...] = jnp.zeros_like(zp)
    tot[:, 8 : row_count + 8, :] = base[...]
    wrap()

    def push(width, origin):
        def add(group, inner):
            here = [move[band, rows_of(group), :] for band in range(bands)]
            middle = pl.ds(pl.multiple_of(group * 8 + 8, 8), 8)
            sums = [tot[band, middle, :] for band in range(bands)]
            for entry in range(width):
                lanes = (lane & (LANES - list_len)) + (origin + entry)
                values = [take(here[band], lanes) for band in range(bands)]
                for band in range(bands):
                    for other in range(bands):
                        start = (group * bands + band) * (LANES * 8) + (other * list_len + origin + entry) * 8
                        rows = pl.ds(pl.multiple_of(start, 8), 8)
                        sums[band] = sums[band] + values[other] * kt[rows, :]
            for band in range(bands):
                tot[band, middle, :] = sums[band]
            return inner

        lax.fori_loop(0, groups, add, 0, unroll=2)

    def step(number, carry):
        color_no = lax.rem(number, COLORS)

        def update(group, inner):
            rows = rows_of(group)
            now = color_ref[rows, :] == color_no
            for band, value in enumerate(gathered(group)):
                old = zp[band, rows, :]
                new = jnp.where(now, value * rden[band, rows, :], old)
                zp[band, rows, :] = new
                move[band, rows, :] = new - old
            return inner

        lax.fori_loop(0, groups, update, 0, unroll=2)

        @pl.when(color_no == COLORS - 1)
        def _():
            out_ref[lax.div(number, COLORS)] = zp[...]

        low, high = window[2 * color_no], window[2 * color_no + 1]
        widths = (list_len // 4, list_len * 3 // 8, list_len // 2)
        for index, width in enumerate(widths):
            fits = high - low <= width
            if index:
                fits = fits & (high - low > widths[index - 1])

            @pl.when(fits)
            def _(width=width):
                push(width, jnp.minimum(low, list_len - width))

        @pl.when(high - low > widths[-1])
        def _():
            lax.fori_loop(0, 2, lambda part, inner: (push(widths[-1], part * widths[-1]), inner)[1], 0)

        wrap()
        return carry

    lax.fori_loop(0, SWEEPS * COLORS, step, 0)


def greet(axes):
    barrier = pltpu.get_barrier_semaphore()
    total = 0
    for axis, count in axes:
        for step in range(1, count):
            peer = lax.rem(lax.axis_index(axis) + step, count)
            pl.semaphore_signal(barrier, inc=1, device_id={axis: peer}, device_id_type=MESH)
            total += 1
    pl.semaphore_wait(barrier, total)


def send_all(axis, count, source, target, send_sems, recv_sems, first):
    me = lax.axis_index(axis)
    copies = []
    for step in range(1, count):
        peer = lax.rem(me + step, count)
        copy = pltpu.make_async_remote_copy(
            src_ref=source(peer),
            dst_ref=target.at[me],
            send_sem=send_sems.at[first + step - 1],
            recv_sem=recv_sems.at[first + step - 1],
            device_id={axis: peer},
            device_id_type=MESH,
        )
        copy.start()
        copies.append(copy)
    return copies


def take(value, picks):
    return jnp.take_along_axis(value, picks, axis=1, mode="promise_in_bounds")


def sort_entries(list_len, fields, listed, color_ref):
    lane = lax.broadcasted_iota(jnp.int32, (8, LANES), 1)
    segment = lane & (LANES - list_len)
    live = listed < fields
    row_no, lane_no = listed // LANES, listed % LANES
    color = jnp.full((8, LANES), -1, jnp.int32)
    for row in range(color_ref.shape[0]):
        table = jnp.broadcast_to(color_ref[row : row + 1, :], (8, LANES))
        color = jnp.where(row_no == row, take(table, lane_no), color)
    color = jnp.where(live, color, -1)
    masks = jnp.concatenate([(color == c).astype(jnp.float32) for c in range(COLORS)], axis=0)
    source = lax.broadcasted_iota(jnp.int32, (LANES, LANES), 0)
    target = lax.broadcasted_iota(jnp.int32, (LANES, LANES), 1)
    same = (source // list_len) == (target // list_len)
    dims = (((1,), (0,)), ((), ()))
    before = (same & (source < target)).astype(jnp.float32)
    ranks = lax.dot_general(masks, before, dims, preferred_element_type=jnp.float32)
    counts = lax.dot_general(masks, same.astype(jnp.float32), dims, preferred_element_type=jnp.float32)
    rest = jnp.zeros((8, LANES), jnp.float32)
    room = [None] * COLORS
    for c in reversed(range(COLORS)):
        rest = rest + counts[c * 8 : c * 8 + 8]
        room[c] = list_len - rest
    end = jnp.zeros((8, LANES), jnp.float32)
    place = jnp.full((8, LANES), -1.0, jnp.float32)
    for c in range(COLORS):
        start = jnp.minimum(jnp.maximum(end, float(list_len * c // COLORS)), room[c])
        end = start + counts[c * 8 : c * 8 + 8]
        place = jnp.where(color == c, start + ranks[c * 8 : c * 8 + 8], place)
    place = place.astype(jnp.int32)
    sorted_fields = jnp.full((8, LANES), fields, jnp.int32)
    sorted_colors = jnp.full((8, LANES), -1, jnp.int32)
    for entry in range(list_len):
        picks = segment + entry
        hit = take(place, picks) == lane - segment
        sorted_fields = jnp.where(hit, take(listed, picks), sorted_fields)
        sorted_colors = jnp.where(hit, take(color, picks), sorted_colors)
    return place, sorted_fields, sorted_colors


def exchange_kernel(
    tiles, bands, list_len, fields,
    lists_ref, color_ref, mags_ref, wts_ref, slots_ref,
    all_lists_ref, data_ref, places_ref, data_places_ref,
    listed_ref, sorted_ref, send_sems, recv_sems,
):
    blocks = lists_ref.shape[0]
    pack = LANES // list_len
    tile_rows = blocks // pack
    obs, stars = mags_ref.shape
    rows = stars // blocks
    mine = stars // bands
    my_tile, my_band = lax.axis_index("sky"), lax.axis_index("band")
    greet((("sky", tiles), ("band", bands)))

    def columns(band):
        return pl.ds(pl.multiple_of(band * mine, LANES), mine)

    count = [0]

    def send(source, target, device):
        copy = pltpu.make_async_remote_copy(
            src_ref=source,
            dst_ref=target,
            send_sem=send_sems.at[count[0]],
            recv_sem=recv_sems.at[count[0]],
            device_id=device,
            device_id_type=MESH,
        )
        count[0] += 1
        copy.start()
        return copy

    peers = [lax.rem(my_band + step, bands) for step in range(1, bands)]
    copies = []
    for peer in peers:
        copies.append(send(mags_ref.at[:, columns(peer)], data_ref.at[my_band, 0], {"band": peer}))
        copies.append(send(wts_ref.at[:, columns(peer)], data_ref.at[my_band, 1], {"band": peer}))
    listed_ref[...] = jnp.full((8, LANES), fields, jnp.int32)
    for row in range(tile_rows):
        pieces = [lists_ref[row * pack + part : row * pack + part + 1, :] for part in range(pack)]
        listed_ref[row : row + 1, :] = jnp.concatenate(pieces, axis=1)
    place, sorted_fields, sorted_colors = sort_entries(list_len, fields, listed_ref[...], color_ref)
    sorted_ref[0] = sorted_fields[0:tile_rows]
    sorted_ref[1] = sorted_colors[0:tile_rows]
    for block in range(blocks):
        table = jnp.broadcast_to(place[block // pack : block // pack + 1, :], (obs, LANES))
        for half in range(rows // LANES):
            cols = pl.ds(block * rows + half * LANES, LANES)
            places_ref[:, cols] = take(table, slots_ref[:, cols] + block % pack * list_len)
    for peer in peers:
        copies.append(send(places_ref.at[:, columns(peer)], data_places_ref.at[my_band], {"band": peer}))
    for step in range(1, tiles):
        peer = lax.rem(my_tile + step, tiles)
        copies.append(send(sorted_ref, all_lists_ref.at[my_tile], {"sky": peer}))
    all_lists_ref[my_tile] = sorted_ref[...]
    data_ref[my_band, 0] = mags_ref[:, columns(my_band)]
    data_ref[my_band, 1] = wts_ref[:, columns(my_band)]
    data_places_ref[my_band] = places_ref[:, columns(my_band)]
    for copy in copies:
        copy.wait()


def spread_kernel(high_count, matching, own_ref, rows_ref, all_ref, pick_ref, send_sems, recv_sems):
    sky, band = lax.axis_index("sky"), lax.axis_index("band")
    high, low = sky // 2, sky % 2
    side, core = band // 2, band % 2
    highs = [lax.rem(high + step, high_count) for step in range(1, high_count)]
    to_low = {"sky": high * 2 + (1 - low)}
    to_side = {"band": (1 - side) * 2 + core}
    to_core = {"band": side * 2 + (1 - core)}
    peers = [{"sky": peer * 2 + low} for peer in highs] + [to_low, to_side, to_core]
    barrier = pltpu.get_barrier_semaphore()
    for peer in peers:
        pl.semaphore_signal(barrier, inc=1, device_id=peer, device_id_type=MESH)
    pl.semaphore_wait(barrier, len(peers))
    count = [0]

    def send(source, target, peer):
        copy = pltpu.make_async_remote_copy(
            src_ref=source,
            dst_ref=target,
            send_sem=send_sems.at[count[0]],
            recv_sem=recv_sems.at[count[0]],
            device_id=peer,
            device_id_type=MESH,
        )
        count[0] += 1
        copy.start()
        return copy

    def wait(copies):
        for copy in copies:
            copy.wait()

    mine = all_ref.at[high, low, side, core]
    copies = [send(own_ref, mine, peer) for peer in peers[: high_count - 1]]
    all_ref[high, low, side, core] = own_ref[...]
    match_kernel(*matching, rows_ref, pick_ref)
    wait(copies)

    column = all_ref.at[:, low, side, core]
    first = all_ref.at[:, low, side, core, 0]
    second = all_ref.at[:, low, side, core, 1]
    copies = [send(first, first, to_low), send(second, second, to_side)]
    late = [send(column, column, to_core)]
    wait(copies)

    first = all_ref.at[:, :, side, core, 0]
    second = all_ref.at[:, low, :, core, 1]
    copies = [send(first, first, to_side), send(second, second, to_low)]
    for part in (all_ref.at[:, 1 - low, side, core, 0], all_ref.at[:, low, 1 - side, core, 1]):
        late.append(send(part, part, to_core))
    wait(copies)

    for part in (all_ref.at[:, :, 1 - side, core, 0], all_ref.at[:, 1 - low, :, core, 1]):
        late.append(send(part, part, to_core))
    wait(late)


def total_kernel(tiles, bands, part_ref, out_ref, by_band, held, by_tile, send_sems, recv_sems):
    greet((("sky", tiles), ("band", bands)))
    copies = send_all("band", bands, lambda peer: part_ref, by_band, send_sems, recv_sems, tiles - 1)
    by_band[lax.axis_index("band")] = part_ref[...]
    for copy in copies:
        copy.wait()
    total = by_band[0]
    for band in range(1, bands):
        total = total + by_band[band]
    held[...] = total
    copies = send_all("sky", tiles, lambda peer: held, by_tile, send_sems, recv_sems, 0)
    by_tile[lax.axis_index("sky")] = total
    for copy in copies:
        copy.wait()
    total = by_tile[0]
    for tile in range(1, tiles):
        total = total + by_tile[tile]
    out_ref[...] = total


def match_kernel(list_len, fields, places, rows_ref, pick_ref):
    pack = LANES // list_len
    lane = lax.broadcasted_iota(jnp.int32, (8, LANES), 1)

    def group_picks(group, carry):
        home = rows_ref[pl.ds(pl.multiple_of(group * 8 + 8, 8), 8), :]
        home = jnp.where(home < fields, home, -1)
        near = [rows_ref[pl.ds(group * 8 + 8 + place - places // 2, 8), :] for place in range(places)]
        found = [[] for _ in range(places)]
        for quarter in range(pack):
            picks = [jnp.full((8, LANES), LANES, jnp.int32) for _ in range(places)]
            for entry in range(list_len):
                source = quarter * list_len + entry
                for place in range(places):
                    other = jnp.broadcast_to(near[place][:, source : source + 1], (8, LANES))
                    picks[place] = jnp.where(other == home, source, picks[place])
            for place in range(places):
                found[place].append(picks[place])
        rows = pl.ds(pl.multiple_of(group * 8, 8), 8)
        for place in range(places):
            ranked = found[place]
            if place == places // 2:
                ranked = [jnp.where(pick == lane, LANES, pick) for pick in ranked]
            for turn in range(pack):
                for low in range(turn % 2, pack - 1, 2):
                    pair = ranked[low], ranked[low + 1]
                    ranked[low], ranked[low + 1] = jnp.minimum(*pair), jnp.maximum(*pair)
            for level in range(pack):
                pick_ref[level, place, rows, :] = ranked[level]
        return carry

    lax.fori_loop(0, pick_ref.shape[2] // 8, group_picks, 0)


def finish_kernel(
    bands, obs, list_len, rows,
    mix_ref, data_ref, data_places_ref, mags_ref, wts_ref, places_ref, zp_two_ref, zp_own_ref,
    means_ref, misfit_ref,
):
    halves = rows // LANES
    pack = LANES // list_len
    mine = data_ref.shape[3] // rows
    first = lax.rem(lax.axis_index("band") * mine, pack)

    def spread(row, picks):
        return take(jnp.broadcast_to(row, (obs, LANES)), picks)

    for block in range(zp_own_ref.shape[0] * pack):
        row = zp_own_ref[block // pack : block // pack + 1, :]
        for half in range(halves):
            cols = pl.ds(block * rows + half * LANES, LANES)
            wts = wts_ref[:, cols]
            picks = places_ref[:, cols] + block % pack * list_len
            left = wts * (mags_ref[:, cols] - spread(row, picks))
            means_ref[0:1, cols] = jnp.sum(left, axis=0, keepdims=True) / jnp.sum(wts, axis=0, keepdims=True)

    lines = []
    for sweep in range(SWEEPS):
        partial = [jnp.zeros((obs, LANES), jnp.float32) for _ in range(bands)]
        for block in range(mine):
            for half in range(halves):
                cols = pl.ds(block * rows + half * LANES, LANES)
                left, means = [], []
                for band in range(bands):
                    wts = data_ref[band, 1, :, cols]
                    picks = data_places_ref[band, :, cols] + (first + block) * list_len
                    row = zp_two_ref[sweep, band]
                    mags = data_ref[band, 0, :, cols] - spread(row, picks)
                    left.append(mags)
                    means.append(jnp.sum(wts * mags, axis=0, keepdims=True) / jnp.sum(wts, axis=0, keepdims=True))
                for band in range(bands):
                    predicted = mix_ref[band, 0] * means[0]
                    for other in range(1, bands):
                        predicted = predicted + mix_ref[band, other] * means[other]
                    wts = data_ref[band, 1, :, cols]
                    partial[band] = partial[band] + wts * (left[band] - predicted) ** 2
        lines += [jnp.sum(partial[band], axis=0, keepdims=True) for band in range(bands)]
    lines.append(jnp.zeros((LANES - len(lines), LANES), jnp.float32))
    block_sums = jnp.concatenate(lines, axis=0)
    misfit_ref[...] = contract_lanes(jnp.ones((8, LANES), jnp.float32), block_sums)


def body(magnitudes, weights, slots, block_fields, owner, colors, color_terms):
    bands = color_terms.shape[0]
    tiles = lax.axis_size("sky")
    my_tile = lax.axis_index("sky")
    my_band = lax.axis_index("band")
    _, obs, stars = magnitudes.shape
    blocks, list_len = block_fields.shape
    rows = stars // blocks
    fields = owner.shape[0]
    owned = fields // tiles
    mine = blocks // bands
    pack = LANES // list_len
    tile_rows = blocks // pack
    row_count = tiles * tile_rows
    mixing = (
        jnp.eye(bands, dtype=jnp.float32) + color_terms - jnp.diag(jnp.sum(color_terms, axis=1))
    )
    vmem = pl.BlockSpec(memory_space=pltpu.VMEM)
    smem = pl.BlockSpec(memory_space=pltpu.SMEM)
    hbm = pl.BlockSpec(memory_space=pl.ANY)

    field_no = jnp.arange(fields, dtype=jnp.int32)[:, None]
    copies = 3 * (bands - 1) + tiles - 1
    lists, data, places, data_places = pl.pallas_call(
        functools.partial(exchange_kernel, tiles, bands, list_len, fields),
        out_shape=(
            jax.ShapeDtypeStruct((tiles, 2, tile_rows, LANES), jnp.int32),
            jax.ShapeDtypeStruct((bands, 2, obs, mine * rows), jnp.float32),
            jax.ShapeDtypeStruct((obs, stars), jnp.int32),
            jax.ShapeDtypeStruct((bands, obs, mine * rows), jnp.int32),
        ),
        in_specs=[vmem] * 5,
        out_specs=(vmem,) * 4,
        scratch_shapes=[
            pltpu.VMEM((8, LANES), jnp.int32),
            pltpu.VMEM((2, tile_rows, LANES), jnp.int32),
            pltpu.SemaphoreType.DMA((copies,)),
            pltpu.SemaphoreType.DMA((copies,)),
        ],
        compiler_params=pltpu.CompilerParams(collective_id=0, has_side_effects=True),
        name="exchange",
    )(block_fields, colors.reshape(-1, LANES), magnitudes[0], weights[0], slots[0])
    all_fields = lists[:, 0].reshape(row_count, LANES)
    entry_colors = lists[:, 1].reshape(row_count, LANES)

    mix_grid = jnp.repeat(jnp.repeat(mixing.T, list_len, axis=0), list_len, axis=1)
    coupled = pl.pallas_call(
        functools.partial(couple_kernel, bands, obs, list_len, rows),
        out_shape=jax.ShapeDtypeStruct((bands // 2, LANES + EXTRA, LANES), jnp.float32),
        in_specs=[smem, vmem, vmem, vmem],
        out_specs=vmem,
        name="couple",
    )(mixing, mix_grid, data, data_places)
    reach_rows = REACH * tile_rows + tile_rows - 1
    padded = jnp.concatenate([all_fields[-8:], all_fields, all_fields[:8]], axis=0)
    reach = 2 * reach_rows + 1
    everyone = (tiles // 2, 2, bands // 2, 2) + coupled.shape
    copies = tiles // 2 - 1 + 9
    coupled, pick = pl.pallas_call(
        functools.partial(spread_kernel, tiles // 2, (list_len, fields, reach)),
        out_shape=(
            jax.ShapeDtypeStruct(everyone, jnp.float32),
            jax.ShapeDtypeStruct((pack, reach, row_count, LANES), jnp.int32),
        ),
        in_specs=[vmem, vmem],
        out_specs=(vmem, vmem),
        scratch_shapes=[pltpu.SemaphoreType.DMA((copies,)), pltpu.SemaphoreType.DMA((copies,))],
        compiler_params=pltpu.CompilerParams(
            collective_id=2, has_side_effects=True, vmem_limit_bytes=60 * 1024 * 1024
        ),
        name="spread",
    )(coupled, padded)
    coupled = coupled.reshape((-1,) + coupled.shape[-2:])

    big = (bands, row_count, LANES)
    snapshots = pl.pallas_call(
        functools.partial(sweep_kernel, bands, list_len, row_count),
        out_shape=jax.ShapeDtypeStruct((SWEEPS,) + big, jnp.float32),
        in_specs=[hbm, vmem, vmem],
        out_specs=vmem,
        scratch_shapes=[
            pltpu.VMEM((row_count * bands * LANES, LANES), jnp.float32),
            pltpu.VMEM(big, jnp.float32),
            pltpu.VMEM((bands, row_count + 16, LANES), jnp.float32),
            pltpu.VMEM(big, jnp.float32),
            pltpu.VMEM(big, jnp.float32),
            pltpu.VMEM(big, jnp.float32),
            pltpu.VMEM((4, bands, LANES + EXTRA, LANES), jnp.float32),
            pltpu.SemaphoreType.DMA((4,)),
            pltpu.SMEM((2 * COLORS + 1,), jnp.int32),
        ],
        compiler_params=pltpu.CompilerParams(vmem_limit_bytes=60 * 1024 * 1024),
        name="sweeps",
    )(coupled, pick, entry_colors)

    final = lax.dynamic_index_in_dim(snapshots[SWEEPS - 1], my_band, 0, keepdims=False)
    zp_tile = lax.dynamic_slice_in_dim(final, my_tile * tile_rows, tile_rows, axis=0)
    my_row = (my_tile * blocks + my_band * mine) // pack
    zp_two = lax.dynamic_slice_in_dim(snapshots, my_row, 1, axis=2)
    star_means, partial = pl.pallas_call(
        functools.partial(finish_kernel, bands, obs, list_len, rows),
        out_shape=(
            jax.ShapeDtypeStruct((1, stars), jnp.float32),
            jax.ShapeDtypeStruct((8, LANES), jnp.float32),
        ),
        in_specs=[smem] + [vmem] * 7,
        out_specs=(vmem, vmem),
        name="finish",
    )(mixing, data, data_places, magnitudes[0], weights[0], places, zp_two, zp_tile)
    slab = (8, LANES)
    peers = tiles + bands - 2
    total = pl.pallas_call(
        functools.partial(total_kernel, tiles, bands),
        out_shape=jax.ShapeDtypeStruct(slab, jnp.float32),
        in_specs=[vmem],
        out_specs=vmem,
        scratch_shapes=[
            pltpu.VMEM((bands,) + slab, jnp.float32),
            pltpu.VMEM(slab, jnp.float32),
            pltpu.VMEM((tiles,) + slab, jnp.float32),
            pltpu.SemaphoreType.DMA((peers,)),
            pltpu.SemaphoreType.DMA((peers,)),
        ],
        compiler_params=pltpu.CompilerParams(collective_id=1, has_side_effects=True),
        name="total",
    )(partial)
    misfit = total[0, : SWEEPS * bands].reshape(SWEEPS, bands) / (obs * stars * tiles)
    misfit = lax.dynamic_slice_in_dim(misfit, my_band, 1, axis=1)

    tile_ids = jnp.mod(my_tile + jnp.arange(3, dtype=jnp.int32) - 1, tiles)

    def close(table):
        by_tile = table.reshape(tiles, tile_rows * LANES)
        parts = [lax.dynamic_index_in_dim(by_tile, tile_ids[n], 0, keepdims=False) for n in range(3)]
        return jnp.concatenate(parts)

    close_fields = close(all_fields)
    is_mine = (owner == my_tile)[:, None]
    rank = jnp.sum((is_mine & (field_no < close_fields[None])).astype(jnp.int32), axis=0)
    has = jnp.sum((is_mine & (field_no == close_fields[None])).astype(jnp.int32), axis=0) > 0
    rank = jnp.where(has, rank, owned)
    entry_no = jnp.arange(close_fields.shape[0], dtype=jnp.int32)[:, None]
    hit = rank[:, None] == jnp.arange(owned, dtype=jnp.int32)[None]
    chosen = jnp.max(jnp.where(hit, entry_no, -1), axis=0)
    own_zp = jnp.sum(jnp.where(chosen[None] == entry_no, close(final)[:, None], 0.0), axis=0)
    return own_zp[None], star_means, misfit


def solution(mesh):
    in_specs = (
        P("band", None, "sky"),
        P("band", None, "sky"),
        P("band", None, "sky"),
        P("sky", None),
        P(),
        P(),
        P(),
    )
    out_specs = (P("band", "sky"), P("band", "sky"), P(None, "band"))
    return jax.shard_map(body, mesh=mesh, in_specs=in_specs, out_specs=out_specs, check_vma=False)
```

```python
import functools

import jax
import jax.numpy as jnp
from jax import lax
from jax.experimental import pallas as pl
from jax.experimental.pallas import tpu as pltpu
from jax.sharding import PartitionSpec as P

COLORS = 8
SWEEPS = 4
PRIOR_WEIGHT = 1.0
REACH = 2
HIGHEST = lax.Precision.HIGHEST
LANES = 128
EXTRA = 8
MESH = pl.DeviceIdType.MESH


def contract_lanes(left, right):
    dims = (((1,), (1,)), ((), ()))
    return lax.dot_general(left, right, dims, precision=HIGHEST, preferred_element_type=jnp.float32)


def mixing_of(terms_ref, bands):
    mixing = []
    for band in range(bands):
        total = terms_ref[band, 0]
        for other in range(1, bands):
            total = total + terms_ref[band, other]
        row = [terms_ref[band, other] for other in range(bands)]
        row[band] = (1.0 + row[band]) - total
        mixing.append(row)
    return mixing


def mixed(mixing, band, means):
    predicted = mixing[band][0] * means[0]
    for other in range(1, len(means)):
        predicted = predicted + mixing[band][other] * means[other]
    return predicted


def couple(bands, obs, list_len, rows, terms_ref, data_ref, places_ref, out_ref):
    blocks = data_ref.shape[3] // rows
    mixing = mixing_of(terms_ref, bands)
    row_band = lax.broadcasted_iota(jnp.int32, (LANES, LANES), 0) // list_len
    lane_band = lax.broadcasted_iota(jnp.int32, (LANES, LANES), 1) // list_len
    mix_grid = jnp.zeros((LANES, LANES), jnp.float32)
    for band in range(bands):
        for other in range(bands):
            here = (row_band == other) & (lane_band == band)
            mix_grid = jnp.where(here, mixing[band][other], mix_grid)
    full = []
    entry = lax.broadcasted_iota(jnp.int32, (list_len, rows), 0)
    for block in range(blocks):
        cols = pl.ds(block * rows, rows)
        one_hot, one_hot_mag, star_weight, means = [], [], [], []
        for band in range(bands):
            mags = data_ref[band, 0, :, cols]
            wts = data_ref[band, 1, :, cols]
            slots = places_ref[band, :, cols]
            scaled = wts * mags
            weight_sum = jnp.sum(wts, axis=0, keepdims=True)
            star_weight.append(weight_sum)
            means.append(jnp.sum(scaled, axis=0, keepdims=True) / weight_sum)
            hot = jnp.zeros((list_len, rows), jnp.float32)
            hot_mag = jnp.zeros((list_len, rows), jnp.float32)
            for k in range(obs):
                hit = slots[k : k + 1] == entry
                hot = hot + jnp.where(hit, wts[k : k + 1], 0.0)
                hot_mag = hot_mag + jnp.where(hit, scaled[k : k + 1], 0.0)
            one_hot.append(hot)
            one_hot_mag.append(hot_mag)
        rest = []
        shares = []
        for band in range(bands):
            rest.append(one_hot_mag[band] - one_hot[band] * mixed(mixing, band, means))
            shares.append(one_hot[band] / star_weight[band])
        hot_all = jnp.concatenate(one_hot, axis=0)
        share_all = jnp.concatenate(shares, axis=0)
        rest_all = jnp.concatenate(rest, axis=0)
        coupling = contract_lanes(share_all, hot_all) * mix_grid
        ones = jnp.ones((8, rows), jnp.float32)
        rest_row = contract_lanes(ones, rest_all)
        weight_row = contract_lanes(ones, hot_all)
        first = lax.broadcasted_iota(jnp.int32, (EXTRA, LANES), 0) == 0
        full.append(jnp.concatenate([coupling, jnp.where(first, rest_row, weight_row)], axis=0))
    split = bands // 2
    for part in range(split):
        pieces = []
        for half in range(2):
            band = half * split + part
            for block in range(blocks):
                pieces.append(full[block][:, band * list_len : (band + 1) * list_len])
        out_ref[part] = jnp.concatenate(pieces, axis=1)


def sweep_kernel(
    bands, list_len, row_count,
    window_ref, coupled_ref, pick_ref, color_ref,
    out_ref, kt, base, tot, rden, zp, move, stage, sems,
):
    groups = row_count // 8
    pack = LANES // list_len
    split = bands // 2
    levels, places = pick_ref.shape[:2]
    depth = stage.shape[0]
    lane = lax.broadcasted_iota(jnp.int32, (8, LANES), 1)
    lane_wide = lax.broadcasted_iota(jnp.int32, (LANES + EXTRA, LANES), 1)

    def fetch(row, slot):
        return pltpu.make_async_copy(
            coupled_ref.at[pl.ds(row * (2 * split), 2 * split)], stage.at[slot], sems.at[slot]
        )

    for row in range(depth - 1):
        fetch(row, row).start()

    def unpack(row, carry):
        slot = lax.rem(row, depth)
        ahead = row + depth - 1

        @pl.when(ahead < row_count)
        def _():
            fetch(ahead, lax.rem(ahead, depth)).start()

        fetch(row, slot).wait()
        group = lax.div(row, 8)
        place = lax.rem(row, 8)
        for part in range(split):
            left = stage[slot, part]
            right = stage[slot, split + part]
            low = jnp.where(lane_wide < LANES // 2, left, pltpu.roll(right, LANES // 2, 1))
            high = jnp.where(lane_wide < LANES // 2, pltpu.roll(left, LANES // 2, 1), right)
            for band, value in ((part, low), (split + part, high)):
                start = (group * bands + band) * (LANES * 8) + place
                kt[pl.ds(start, LANES, stride=8), :] = value[0:LANES]
                base[band, pl.ds(row, 1), :] = value[LANES : LANES + 1]
                tot[band, pl.ds(row + 8, 1), :] = value[LANES + 1 : LANES + 2]
        return carry

    lax.fori_loop(0, row_count, unpack, 0)

    def rows_of(group):
        return pl.ds(pl.multiple_of(group * 8, 8), 8)

    def wrap():
        for band in range(bands):
            tot[band, 0:8, :] = tot[band, row_count : row_count + 8, :]
            tot[band, row_count + 8 : row_count + 16, :] = tot[band, 8:16, :]

    def gather(group, first, count, sums):
        for place in range(places):
            start = group * 8 + (8 + place - places // 2)
            near = [tot[band, pl.ds(start, 8), :] for band in range(bands)]
            for level in range(count):
                pick = pick_ref[first + level, place, rows_of(group), :]
                mask = pick < LANES
                lanes = pick & (LANES - 1)
                for band in range(bands):
                    index = 2 * band + level % 2
                    sums[index] = sums[index] + jnp.where(mask, take(near[band], lanes), 0.0)
        return sums

    def gathered(group):
        sums = []
        for band in range(bands):
            sums += [tot[band, pl.ds(pl.multiple_of(group * 8 + 8, 8), 8), :], jnp.zeros((8, LANES), jnp.float32)]
        sums = gather(group, 0, 2, sums)
        sums = lax.fori_loop(2, window_ref[0, 2], lambda level, sums: gather(group, level, 1, sums), sums)
        return [sums[2 * band] + sums[2 * band + 1] for band in range(bands)]

    def weigh(group, carry):
        for band, value in enumerate(gathered(group)):
            rden[band, rows_of(group), :] = 1.0 / (value + PRIOR_WEIGHT)
        return carry

    wrap()
    lax.fori_loop(0, groups, weigh, 0)
    zp[...] = jnp.zeros_like(zp)
    tot[:, 8 : row_count + 8, :] = base[...]
    wrap()

    def push(width, origin):
        def add(group, inner):
            here = [move[band, rows_of(group), :] for band in range(bands)]
            middle = pl.ds(pl.multiple_of(group * 8 + 8, 8), 8)
            sums = [tot[band, middle, :] for band in range(bands)]
            for entry in range(width):
                lanes = (lane & (LANES - list_len)) + (origin + entry)
                values = [take(here[band], lanes) for band in range(bands)]
                for band in range(bands):
                    for other in range(bands):
                        start = (group * bands + band) * (LANES * 8) + (other * list_len + origin + entry) * 8
                        rows = pl.ds(pl.multiple_of(start, 8), 8)
                        sums[band] = sums[band] + values[other] * kt[rows, :]
            for band in range(bands):
                tot[band, middle, :] = sums[band]
            return inner

        lax.fori_loop(0, groups, add, 0, unroll=2)

    def step(number, carry):
        color_no = lax.rem(number, COLORS)

        def update(group, inner):
            rows = rows_of(group)
            now = color_ref[rows, :] == color_no
            for band, value in enumerate(gathered(group)):
                old = zp[band, rows, :]
                new = jnp.where(now, value * rden[band, rows, :], old)
                zp[band, rows, :] = new
                move[band, rows, :] = new - old
            return inner

        lax.fori_loop(0, groups, update, 0, unroll=2)

        @pl.when(color_no == COLORS - 1)
        def _():
            out_ref[lax.div(number, COLORS)] = zp[...]

        low, high = window_ref[color_no, 0], window_ref[color_no, 1]
        widths = (list_len // 4, list_len * 3 // 8, list_len // 2)
        for index, width in enumerate(widths):
            fits = high - low <= width
            if index:
                fits = fits & (high - low > widths[index - 1])

            @pl.when(fits)
            def _(width=width):
                push(width, jnp.minimum(low, list_len - width))

        @pl.when(high - low > widths[-1])
        def _():
            lax.fori_loop(0, 2, lambda part, inner: (push(widths[-1], part * widths[-1]), inner)[1], 0)

        wrap()
        return carry

    lax.fori_loop(0, SWEEPS * COLORS, step, 0)


def greet(axes):
    barrier = pltpu.get_barrier_semaphore()
    total = 0
    for axis, count in axes:
        for step in range(1, count):
            peer = lax.rem(lax.axis_index(axis) + step, count)
            pl.semaphore_signal(barrier, inc=1, device_id={axis: peer}, device_id_type=MESH)
            total += 1
    pl.semaphore_wait(barrier, total)


def take(value, picks):
    return jnp.take_along_axis(value, picks, axis=1, mode="promise_in_bounds")


def sort_entries(list_len, fields, listed, color_ref):
    lane = lax.broadcasted_iota(jnp.int32, (8, LANES), 1)
    segment = lane & (LANES - list_len)
    live = listed < fields
    row_no, lane_no = listed // LANES, listed % LANES
    color = jnp.full((8, LANES), -1, jnp.int32)
    for row in range(color_ref.shape[0]):
        table = jnp.broadcast_to(color_ref[row : row + 1, :], (8, LANES))
        color = jnp.where(row_no == row, take(table, lane_no), color)
    color = jnp.where(live, color, -1)
    masks = jnp.concatenate([(color == c).astype(jnp.float32) for c in range(COLORS)], axis=0)
    source = lax.broadcasted_iota(jnp.int32, (LANES, LANES), 0)
    target = lax.broadcasted_iota(jnp.int32, (LANES, LANES), 1)
    same = (source // list_len) == (target // list_len)
    dims = (((1,), (0,)), ((), ()))
    before = (same & (source < target)).astype(jnp.float32)
    ranks = lax.dot_general(masks, before, dims, preferred_element_type=jnp.float32)
    counts = lax.dot_general(masks, same.astype(jnp.float32), dims, preferred_element_type=jnp.float32)
    rest = jnp.zeros((8, LANES), jnp.float32)
    room = [None] * COLORS
    for c in reversed(range(COLORS)):
        rest = rest + counts[c * 8 : c * 8 + 8]
        room[c] = list_len - rest
    end = jnp.zeros((8, LANES), jnp.float32)
    place = jnp.full((8, LANES), -1.0, jnp.float32)
    for c in range(COLORS):
        start = jnp.minimum(jnp.maximum(end, float(list_len * c // COLORS)), room[c])
        end = start + counts[c * 8 : c * 8 + 8]
        place = jnp.where(color == c, start + ranks[c * 8 : c * 8 + 8], place)
    place = place.astype(jnp.int32)
    sorted_fields = jnp.full((8, LANES), fields, jnp.int32)
    sorted_colors = jnp.full((8, LANES), -1, jnp.int32)
    for entry in range(list_len):
        picks = segment + entry
        hit = take(place, picks) == lane - segment
        sorted_fields = jnp.where(hit, take(listed, picks), sorted_fields)
        sorted_colors = jnp.where(hit, take(color, picks), sorted_colors)
    return place, sorted_fields, sorted_colors


def exchange_kernel(
    tiles, bands, list_len, fields,
    lists_ref, color_ref, mags_ref, wts_ref, slots_ref,
    all_lists_ref, data_ref, places_ref, data_places_ref,
    listed_ref, sorted_ref, send_sems, recv_sems,
):
    blocks = lists_ref.shape[0]
    pack = LANES // list_len
    tile_rows = blocks // pack
    obs, stars = mags_ref.shape
    rows = stars // blocks
    mine = stars // bands
    my_tile, my_band = lax.axis_index("sky"), lax.axis_index("band")
    greet((("sky", tiles), ("band", bands)))

    def columns(band):
        return pl.ds(pl.multiple_of(band * mine, LANES), mine)

    count = [0]

    def send(source, target, device):
        copy = pltpu.make_async_remote_copy(
            src_ref=source,
            dst_ref=target,
            send_sem=send_sems.at[count[0]],
            recv_sem=recv_sems.at[count[0]],
            device_id=device,
            device_id_type=MESH,
        )
        count[0] += 1
        copy.start()
        return copy

    peers = [lax.rem(my_band + step, bands) for step in range(1, bands)]
    copies = []
    for peer in peers:
        copies.append(send(mags_ref.at[:, columns(peer)], data_ref.at[my_band, 0], {"band": peer}))
        copies.append(send(wts_ref.at[:, columns(peer)], data_ref.at[my_band, 1], {"band": peer}))
    listed_ref[...] = jnp.full((8, LANES), fields, jnp.int32)
    for row in range(tile_rows):
        pieces = [lists_ref[row * pack + part : row * pack + part + 1, :] for part in range(pack)]
        listed_ref[row : row + 1, :] = jnp.concatenate(pieces, axis=1)
    place, sorted_fields, sorted_colors = sort_entries(list_len, fields, listed_ref[...], color_ref)
    sorted_ref[0] = sorted_fields[0:tile_rows]
    sorted_ref[1] = sorted_colors[0:tile_rows]
    for block in range(blocks):
        table = jnp.broadcast_to(place[block // pack : block // pack + 1, :], (obs, LANES))
        for half in range(rows // LANES):
            cols = pl.ds(block * rows + half * LANES, LANES)
            places_ref[:, cols] = take(table, slots_ref[:, cols] + block % pack * list_len)
    for peer in peers:
        copies.append(send(places_ref.at[:, columns(peer)], data_places_ref.at[my_band], {"band": peer}))
    for step in range(1, tiles):
        peer = lax.rem(my_tile + step, tiles)
        copies.append(send(sorted_ref, all_lists_ref.at[my_tile], {"sky": peer}))
    all_lists_ref[my_tile] = sorted_ref[...]
    data_ref[my_band, 0] = mags_ref[:, columns(my_band)]
    data_ref[my_band, 1] = wts_ref[:, columns(my_band)]
    data_places_ref[my_band] = places_ref[:, columns(my_band)]
    for copy in copies:
        copy.wait()


def match(list_len, fields, lists_ref, rows_ref, pick_ref, color_ref):
    tiles, _, tile_rows, _ = lists_ref.shape
    pack = LANES // list_len
    levels, places, row_count, _ = pick_ref.shape
    lane = lax.broadcasted_iota(jnp.int32, (8, LANES), 1)
    for tile in range(tiles):
        start = tile * tile_rows
        rows_ref[8 + start : 8 + start + tile_rows, :] = lists_ref[tile, 0]
        color_ref[start : start + tile_rows, :] = lists_ref[tile, 1]
    rows_ref[0:8, :] = rows_ref[row_count : row_count + 8, :]
    rows_ref[row_count + 8 : row_count + 16, :] = rows_ref[8:16, :]

    def group_picks(group, carry):
        home = rows_ref[pl.ds(pl.multiple_of(group * 8 + 8, 8), 8), :]
        home = jnp.where(home < fields, home, -1)
        near = [rows_ref[pl.ds(group * 8 + 8 + place - places // 2, 8), :] for place in range(places)]
        found = [[] for _ in range(places)]
        for quarter in range(pack):
            picks = [jnp.full((8, LANES), LANES, jnp.int32) for _ in range(places)]
            for entry in range(list_len):
                source = quarter * list_len + entry
                for place in range(places):
                    other = jnp.broadcast_to(near[place][:, source : source + 1], (8, LANES))
                    picks[place] = jnp.where(other == home, source, picks[place])
            for place in range(places):
                found[place].append(picks[place])
        rows = pl.ds(pl.multiple_of(group * 8, 8), 8)
        for place in range(places):
            ranked = found[place]
            if place == places // 2:
                ranked = [jnp.where(pick == lane, LANES, pick) for pick in ranked]
            for turn in range(pack):
                for low in range(turn % 2, pack - 1, 2):
                    pair = ranked[low], ranked[low + 1]
                    ranked[low], ranked[low + 1] = jnp.minimum(*pair), jnp.maximum(*pair)
            for level in range(pack):
                pick_ref[level, place, rows, :] = ranked[level]
        return carry

    lax.fori_loop(0, row_count // 8, group_picks, 0)


def windows(list_len, pick_ref, color_ref, window_ref):
    levels, places, row_count, _ = pick_ref.shape
    lane = lax.broadcasted_iota(jnp.int32, (8, LANES), 1)
    position = (lane & (list_len - 1)).astype(jnp.float32)

    def rows_of(group):
        return pl.ds(pl.multiple_of(group * 8, 8), 8)

    def bounds(group, carry):
        lows, highs = carry
        color = color_ref[rows_of(group), :]
        new_lows, new_highs = [], []
        for c in range(COLORS):
            new_lows.append(jnp.minimum(lows[c], jnp.where(color == c, position, float(list_len))))
            new_highs.append(jnp.maximum(highs[c], jnp.where(color == c, position + 1.0, 0.0)))
        return new_lows, new_highs

    start = [jnp.full((8, LANES), float(list_len), jnp.float32)] * COLORS, [jnp.zeros((8, LANES), jnp.float32)] * COLORS
    lows, highs = lax.fori_loop(0, row_count // 8, bounds, start)
    lows = jnp.concatenate([jnp.min(value, axis=0, keepdims=True) for value in lows], axis=0)
    highs = jnp.concatenate([jnp.max(value, axis=0, keepdims=True) for value in highs], axis=0)
    lows = jnp.min(lows, axis=1, keepdims=True)
    highs = jnp.max(highs, axis=1, keepdims=True)
    deepest = jnp.full((8, LANES), 2.0, jnp.float32)
    for level in range(2, levels):
        def least(group, value, level=level):
            for place in range(places):
                value = jnp.minimum(value, pick_ref[level, place, rows_of(group), :])
            return value

        found = lax.fori_loop(0, row_count // 8, least, jnp.full((8, LANES), LANES, jnp.int32))
        deepest = jnp.where(found < LANES, level + 1.0, deepest)
    deepest = jnp.max(jnp.max(deepest, axis=0, keepdims=True), axis=1, keepdims=True)
    table = jnp.where(lane == 0, lows, jnp.where(lane == 1, highs, deepest))
    window_ref[...] = table.astype(jnp.int32)


def choose(tiles, fields, owner_ref, rows_ref, chosen_ref):
    field_rows = owner_ref.shape[0]
    tile_rows = (rows_ref.shape[0] - 16) // tiles
    my_tile = lax.axis_index("sky")
    lane = lax.broadcasted_iota(jnp.int32, (8, LANES), 1)
    below = lax.broadcasted_iota(jnp.int32, (8, LANES), 0)
    owned = owner_ref[...] == my_tile
    ones = owned.astype(jnp.float32)
    source = lax.broadcasted_iota(jnp.int32, (LANES, LANES), 0)
    target = lax.broadcasted_iota(jnp.int32, (LANES, LANES), 1)
    dims = (((1,), (0,)), ((), ()))
    inside = lax.dot_general(ones, (source < target).astype(jnp.float32), dims, preferred_element_type=jnp.float32)
    counts = lax.dot_general(ones, jnp.ones((LANES, LANES), jnp.float32), dims, preferred_element_type=jnp.float32)
    upper = lax.broadcasted_iota(jnp.int32, (field_rows, field_rows), 1)
    lower = lax.broadcasted_iota(jnp.int32, (field_rows, field_rows), 0)
    above = lax.dot_general((upper < lower).astype(jnp.float32), counts, dims, preferred_element_type=jnp.float32)
    rank = jnp.where(owned, (inside + above).astype(jnp.int32), -1)
    close = jnp.full((8, LANES), fields, jnp.int32)
    for offset in range(3):
        tile = lax.rem(my_tile + offset + tiles - 1, tiles)
        for row in range(tile_rows):
            value = rows_ref[pl.ds(8 + tile * tile_rows + row, 1), :]
            close = jnp.where(below == offset * tile_rows + row, jnp.broadcast_to(value, (8, LANES)), close)
    row_no, lane_no = close // LANES, close % LANES
    order = jnp.full((8, LANES), -1, jnp.int32)
    for row in range(field_rows):
        table = jnp.broadcast_to(rank[row : row + 1, :], (8, LANES))
        order = jnp.where(row_no == row, take(table, lane_no), order)
    own_rows = chosen_ref.shape[0]
    codes = [jnp.full((8, LANES), -1, jnp.int32) for _ in range(own_rows)]
    for entry in range(LANES):
        value = jnp.broadcast_to(order[:, entry : entry + 1], (8, LANES))
        for row in range(own_rows):
            codes[row] = jnp.where(value == row * LANES + lane, entry, codes[row])
    for row in range(own_rows):
        ranked = jnp.where(codes[row] >= 0, (below + 1).astype(jnp.float32), 0.0)
        last = jnp.max(ranked, axis=0, keepdims=True)
        keep = (ranked > 0.0) & (ranked == last)
        chosen_ref[row] = jnp.where(keep, codes[row], LANES)


def spread_kernel(
    tiles, bands, obs, list_len, rows, fields,
    terms_ref, data_ref, data_places_ref, lists_ref, owner_ref,
    all_ref, pick_ref, color_ref, window_ref, chosen_ref,
    rows_ref, own_ref, send_sems, recv_sems,
):
    high_count = tiles // 2
    sky, band = lax.axis_index("sky"), lax.axis_index("band")
    high, low = sky // 2, sky % 2
    side, core = band // 2, band % 2
    to_low = {"sky": high * 2 + (1 - low)}
    to_side = {"band": (1 - side) * 2 + core}
    to_core = {"band": side * 2 + (1 - core)}
    barrier = pltpu.get_barrier_semaphore()

    def greet_peers(peers):
        for peer in peers:
            pl.semaphore_signal(barrier, inc=1, device_id=peer, device_id_type=MESH)

    def tables():
        match(list_len, fields, lists_ref, rows_ref, pick_ref, color_ref)

    def more_tables():
        windows(list_len, pick_ref, color_ref, window_ref)
        choose(tiles, fields, owner_ref, rows_ref, chosen_ref)

    if high_count > 4:
        highs = [lax.rem(high + step, high_count) for step in range(1, high_count)]
        peers = [{"sky": peer * 2 + low} for peer in highs] + [to_low, to_side, to_core]
        greet_peers(peers)
        couple(bands, obs, list_len, rows, terms_ref, data_ref, data_places_ref, own_ref)
        pl.semaphore_wait(barrier, len(peers))
        count = [0]

        def send(source, target, peer):
            copy = pltpu.make_async_remote_copy(
                src_ref=source,
                dst_ref=target,
                send_sem=send_sems.at[count[0]],
                recv_sem=recv_sems.at[count[0]],
                device_id=peer,
                device_id_type=MESH,
            )
            count[0] += 1
            copy.start()
            return copy

        def wait(copies):
            for copy in copies:
                copy.wait()

        mine = all_ref.at[high, low, side, core]
        copies = [send(own_ref, mine, peer) for peer in peers[: high_count - 1]]
        all_ref[high, low, side, core] = own_ref[...]
        tables()
        more_tables()
        wait(copies)

        column = all_ref.at[:, low, side, core]
        first = all_ref.at[:, low, side, core, 0]
        second = all_ref.at[:, low, side, core, 1]
        copies = [send(first, first, to_low), send(second, second, to_side)]
        late = [send(column, column, to_core)]
        wait(copies)

        first = all_ref.at[:, :, side, core, 0]
        second = all_ref.at[:, low, :, core, 1]
        copies = [send(first, first, to_side), send(second, second, to_low)]
        for part in (all_ref.at[:, 1 - low, side, core, 0], all_ref.at[:, low, 1 - side, core, 1]):
            late.append(send(part, part, to_core))
        wait(copies)

        for part in (all_ref.at[:, :, 1 - side, core, 0], all_ref.at[:, 1 - low, :, core, 1]):
            late.append(send(part, part, to_core))
        wait(late)
        return

    chunks = high_count * 8
    lower, upper = high > 0, high < high_count - 1
    greet_peers([to_low, to_side, to_core])
    for there, step in ((lower, -1), (upper, 1)):
        @pl.when(there)
        def _(step=step):
            greet_peers([{"sky": (high + step) * 2 + low}])

    mine = all_ref.at[high, low, side, core]
    couple(bands, obs, list_len, rows, terms_ref, data_ref, data_places_ref, mine)
    pl.semaphore_wait(barrier, 3 + lower.astype(jnp.int32) + upper.astype(jnp.int32))

    def copy_of(kind, z, y, x, part, peer, landing):
        chunk = all_ref.at[z, y, x, core, part]
        number = ((z * 2 + y) * 2 + x) * 2 + part
        return pltpu.make_async_remote_copy(
            src_ref=chunk,
            dst_ref=chunk,
            send_sem=send_sems.at[kind * chunks + number],
            recv_sem=recv_sems.at[landing * chunks + number],
            device_id=peer,
            device_id_type=MESH,
        )

    def along(z, part, step):
        return copy_of((step + 1) // 2, z, low, side, part, {"sky": (high + step) * 2 + low}, 0)

    def across_x(z, y, part):
        return copy_of(2, z, y, side, part, to_side, 0)

    def across_y(z, x, part):
        return copy_of(3, z, low, x, part, to_low, 0)

    def over(z, y, x, part):
        return copy_of(4, z, y, x, part, to_core, 1)

    def arrived(z, y, x, part):
        copy_of(4, z, y, x, part, to_core, 0).wait_recv()

    ends = {-1: lower, 1: upper}

    def along_if(z, part, step):
        @pl.when(ends[step])
        def _():
            along(z, part, step).start()

    def first_hop(z, part):
        if part == 0:
            across_x(z, low, part).start()
        else:
            across_y(z, side, part).start()

    def second_hop(z, part):
        if part == 0:
            across_y(z, side, part).start()
        else:
            across_x(z, low, part).start()

    for part in range(2):
        along_if(high, part, 1)
        along_if(high, part, -1)
        first_hop(high, part)
    for part in range(2):
        second_hop(high, part)
        over(high, low, side, part).start()
    tables()

    def column_arrival(distance, part):
        for step in (-1, 1):
            z = high - step * distance
            here = z >= 0 if step == 1 else z < high_count

            @pl.when(here)
            def _(z=z, step=step):
                arrived(z, low, side, part)
                along_if(z, part, step)
                first_hop(z, part)
                second_hop(z, part)
                over(z, low, side, part).start()

    def at_distance(distance, action):
        if distance == 0:
            action(high)
            return
        for step in (-1, 1):
            z = high - step * distance

            @pl.when(z >= 0 if step == 1 else z < high_count)
            def _(z=z):
                action(z)

    def turn(z):
        arrived(z, low, 1 - side, 0)
        across_y(z, 1 - side, 0).start()
        over(z, low, 1 - side, 0).start()
        arrived(z, 1 - low, side, 1)
        across_x(z, 1 - low, 1).start()
        over(z, 1 - low, side, 1).start()

    def last(z):
        for y, x, part in ((1 - low, side, 0), (low, 1 - side, 1), (1 - low, 1 - side, 0), (1 - low, 1 - side, 1)):
            arrived(z, y, x, part)
            over(z, y, x, part).start()

    for distance in range(1, high_count):
        column_arrival(distance, 0)
        at_distance(distance - 1, turn)
        column_arrival(distance, 1)
        if distance > 1:
            at_distance(distance - 2, last)
        if distance == 1:
            more_tables()
    at_distance(high_count - 1, turn)
    for distance in range(max(high_count - 2, 0), high_count):
        at_distance(distance, last)

    for z in range(high_count):
        for y in range(2):
            for x in range(2):
                for part in range(2):
                    copy_of(4, z, y, x, part, to_core, 1).wait()
    for z in range(high_count):
        for part in range(2):
            for step in (-1, 1):
                passing = (z >= high) if step == -1 else (z <= high)

                @pl.when(ends[step] & passing)
                def _(z=z, part=part, step=step):
                    along(z, part, step).wait_send()

            for other in range(2):
                if part == 0:
                    across_y(z, other, part).wait_send()
                else:
                    across_x(z, other, part).wait_send()
            first = across_x(z, low, part) if part == 0 else across_y(z, side, part)
            first.wait_send()


def finish_kernel(
    tiles, bands, obs, list_len, rows,
    terms_ref, data_ref, data_places_ref, mags_ref, wts_ref, places_ref, zp_ref, chosen_ref,
    own_zp_ref, means_ref, misfit_ref,
    part_ref, all_parts, send_sems, recv_sems,
):
    halves = rows // LANES
    pack = LANES // list_len
    stars = mags_ref.shape[1]
    blocks = stars // rows
    tile_rows = blocks // pack
    mine = data_ref.shape[3] // rows
    my_tile, my_band = lax.axis_index("sky"), lax.axis_index("band")
    me = my_tile * bands + my_band
    first = lax.rem(my_band * mine, pack)
    mixing = mixing_of(terms_ref, bands)
    peers = []
    for sky_step in range(tiles):
        for band_step in range(bands):
            if sky_step or band_step:
                peers.append({"sky": lax.rem(my_tile + sky_step, tiles), "band": lax.rem(my_band + band_step, bands)})
    barrier = pltpu.get_barrier_semaphore()
    for peer in peers:
        pl.semaphore_signal(barrier, inc=1, device_id=peer, device_id_type=MESH)

    def spread(row, picks):
        return take(jnp.broadcast_to(row, (obs, LANES)), picks)

    my_row = my_tile * tile_rows + lax.div(my_band * mine, pack)
    lines = []
    for sweep in range(SWEEPS):
        partial = [jnp.zeros((obs, LANES), jnp.float32) for _ in range(bands)]
        for block in range(mine):
            for half in range(halves):
                cols = pl.ds(block * rows + half * LANES, LANES)
                left, means = [], []
                for band in range(bands):
                    wts = data_ref[band, 1, :, cols]
                    picks = data_places_ref[band, :, cols] + (first + block) * list_len
                    row = zp_ref[sweep, band, pl.ds(my_row, 1), :]
                    mags = data_ref[band, 0, :, cols] - spread(row, picks)
                    left.append(mags)
                    means.append(jnp.sum(wts * mags, axis=0, keepdims=True) / jnp.sum(wts, axis=0, keepdims=True))
                for band in range(bands):
                    wts = data_ref[band, 1, :, cols]
                    partial[band] = partial[band] + wts * (left[band] - mixed(mixing, band, means)) ** 2
        lines += [jnp.sum(partial[band], axis=0, keepdims=True) for band in range(bands)]
    lines.append(jnp.zeros((LANES - len(lines), LANES), jnp.float32))
    block_sums = jnp.concatenate(lines, axis=0)
    sums = contract_lanes(jnp.ones((8, LANES), jnp.float32), block_sums)
    part_ref[...] = sums
    all_parts[pl.ds(me, 1), :] = sums[0:1, :]
    pl.semaphore_wait(barrier, len(peers))
    copies = []
    for number, peer in enumerate(peers):
        copy = pltpu.make_async_remote_copy(
            src_ref=part_ref.at[0:1],
            dst_ref=all_parts.at[pl.ds(me, 1)],
            send_sem=send_sems.at[number],
            recv_sem=recv_sems.at[number],
            device_id=peer,
            device_id_type=MESH,
        )
        copy.start()
        copies.append(copy)

    for block in range(blocks):
        row = zp_ref[SWEEPS - 1, my_band, pl.ds(my_tile * tile_rows + block // pack, 1), :]
        for half in range(halves):
            cols = pl.ds(block * rows + half * LANES, LANES)
            wts = wts_ref[:, cols]
            picks = places_ref[:, cols] + block % pack * list_len
            left = wts * (mags_ref[:, cols] - spread(row, picks))
            means_ref[0:1, cols] = jnp.sum(left, axis=0, keepdims=True) / jnp.sum(wts, axis=0, keepdims=True)

    below = lax.broadcasted_iota(jnp.int32, (8, LANES), 0)
    close = jnp.zeros((8, LANES), jnp.float32)
    for offset in range(3):
        tile = lax.rem(my_tile + offset + tiles - 1, tiles)
        for row in range(tile_rows):
            value = zp_ref[SWEEPS - 1, my_band, pl.ds(tile * tile_rows + row, 1), :]
            close = jnp.where(below == offset * tile_rows + row, jnp.broadcast_to(value, (8, LANES)), close)
    owned = own_zp_ref.shape[1]
    for row in range(chosen_ref.shape[0]):
        pick = chosen_ref[row]
        value = jnp.where(pick < LANES, take(close, pick & (LANES - 1)), 0.0)
        value = jnp.sum(value, axis=0, keepdims=True)
        width = min(LANES, owned - row * LANES)
        own_zp_ref[0:1, row * LANES : row * LANES + width] = value[:, 0:width]

    for copy in copies:
        copy.wait()
    total = jnp.sum(all_parts[...], axis=0, keepdims=True) / (obs * stars * tiles)
    picks = below * bands + my_band
    column = take(jnp.broadcast_to(total, (8, LANES)), picks)
    misfit_ref[...] = column[0:SWEEPS, 0:1]


def body(magnitudes, weights, slots, block_fields, owner, colors, color_terms):
    bands = color_terms.shape[0]
    tiles = lax.axis_size("sky")
    _, obs, stars = magnitudes.shape
    blocks, list_len = block_fields.shape
    rows = stars // blocks
    fields = owner.shape[0]
    owned = fields // tiles
    mine = blocks // bands
    pack = LANES // list_len
    tile_rows = blocks // pack
    row_count = tiles * tile_rows
    vmem = pl.BlockSpec(memory_space=pltpu.VMEM)
    smem = pl.BlockSpec(memory_space=pltpu.SMEM)
    hbm = pl.BlockSpec(memory_space=pl.ANY)
    magnitudes, weights, slots = magnitudes[0], weights[0], slots[0]

    copies = 3 * (bands - 1) + tiles - 1
    lists, data, places, data_places = pl.pallas_call(
        functools.partial(exchange_kernel, tiles, bands, list_len, fields),
        out_shape=(
            jax.ShapeDtypeStruct((tiles, 2, tile_rows, LANES), jnp.int32),
            jax.ShapeDtypeStruct((bands, 2, obs, mine * rows), jnp.float32),
            jax.ShapeDtypeStruct((obs, stars), jnp.int32),
            jax.ShapeDtypeStruct((bands, obs, mine * rows), jnp.int32),
        ),
        in_specs=[vmem] * 5,
        out_specs=(vmem,) * 4,
        scratch_shapes=[
            pltpu.VMEM((8, LANES), jnp.int32),
            pltpu.VMEM((2, tile_rows, LANES), jnp.int32),
            pltpu.SemaphoreType.DMA((copies,)),
            pltpu.SemaphoreType.DMA((copies,)),
        ],
        compiler_params=pltpu.CompilerParams(collective_id=0, has_side_effects=True),
        name="exchange",
    )(block_fields, colors.reshape(-1, LANES), magnitudes, weights, slots)

    reach = 2 * (REACH * tile_rows + tile_rows - 1) + 1
    own_rows = -(-owned // LANES)
    part = (bands // 2, LANES + EXTRA, LANES)
    everyone = (tiles // 2, 2, bands // 2, 2) + part
    if tiles > 8:
        sends = landings = tiles // 2 - 1 + 9
    else:
        sends, landings = 5 * tiles * 4, 2 * tiles * 4
    coupled, pick, entry_colors, window, chosen = pl.pallas_call(
        functools.partial(spread_kernel, tiles, bands, obs, list_len, rows, fields),
        out_shape=(
            jax.ShapeDtypeStruct(everyone, jnp.float32),
            jax.ShapeDtypeStruct((pack, reach, row_count, LANES), jnp.int32),
            jax.ShapeDtypeStruct((row_count, LANES), jnp.int32),
            jax.ShapeDtypeStruct((8, LANES), jnp.int32),
            jax.ShapeDtypeStruct((own_rows, 8, LANES), jnp.int32),
        ),
        in_specs=[smem] + [vmem] * 4,
        out_specs=(vmem,) * 5,
        scratch_shapes=[
            pltpu.VMEM((row_count + 16, LANES), jnp.int32),
            pltpu.VMEM(part, jnp.float32),
            pltpu.SemaphoreType.DMA((sends,)),
            pltpu.SemaphoreType.DMA((landings,)),
        ],
        compiler_params=pltpu.CompilerParams(
            collective_id=2, has_side_effects=True, vmem_limit_bytes=60 * 1024 * 1024
        ),
        name="spread",
    )(color_terms, data, data_places, lists, owner.reshape(-1, LANES))
    coupled = coupled.reshape((-1,) + coupled.shape[-2:])

    big = (bands, row_count, LANES)
    snapshots = pl.pallas_call(
        functools.partial(sweep_kernel, bands, list_len, row_count),
        out_shape=jax.ShapeDtypeStruct((SWEEPS,) + big, jnp.float32),
        in_specs=[smem, hbm, vmem, vmem],
        out_specs=vmem,
        scratch_shapes=[
            pltpu.VMEM((row_count * bands * LANES, LANES), jnp.float32),
            pltpu.VMEM(big, jnp.float32),
            pltpu.VMEM((bands, row_count + 16, LANES), jnp.float32),
            pltpu.VMEM(big, jnp.float32),
            pltpu.VMEM(big, jnp.float32),
            pltpu.VMEM(big, jnp.float32),
            pltpu.VMEM((4, bands, LANES + EXTRA, LANES), jnp.float32),
            pltpu.SemaphoreType.DMA((4,)),
        ],
        compiler_params=pltpu.CompilerParams(vmem_limit_bytes=60 * 1024 * 1024),
        name="sweeps",
    )(window, coupled, pick, entry_colors)

    devices = tiles * bands
    own_zp, star_means, misfit = pl.pallas_call(
        functools.partial(finish_kernel, tiles, bands, obs, list_len, rows),
        out_shape=(
            jax.ShapeDtypeStruct((1, owned), jnp.float32),
            jax.ShapeDtypeStruct((1, stars), jnp.float32),
            jax.ShapeDtypeStruct((SWEEPS, 1), jnp.float32),
        ),
        in_specs=[smem] + [vmem] * 7,
        out_specs=(vmem,) * 3,
        scratch_shapes=[
            pltpu.VMEM((8, LANES), jnp.float32),
            pltpu.VMEM((devices, LANES), jnp.float32),
            pltpu.SemaphoreType.DMA((devices - 1,)),
            pltpu.SemaphoreType.DMA((devices - 1,)),
        ],
        compiler_params=pltpu.CompilerParams(collective_id=1, has_side_effects=True),
        name="finish",
    )(color_terms, data, data_places, magnitudes, weights, places, snapshots, chosen)
    return own_zp, star_means, misfit


def solution(mesh):
    in_specs = (
        P("band", None, "sky"),
        P("band", None, "sky"),
        P("band", None, "sky"),
        P("sky", None),
        P(),
        P(),
        P(),
    )
    out_specs = (P("band", "sky"), P("band", "sky"), P(None, "band"))
    return jax.shard_map(body, mesh=mesh, in_specs=in_specs, out_specs=out_specs, check_vma=False)
```

```python
import functools

import jax
import jax.numpy as jnp
from jax import lax
from jax.experimental import pallas as pl
from jax.experimental.pallas import tpu as pltpu
from jax.sharding import PartitionSpec as P

COLORS = 8
SWEEPS = 4
PRIOR_WEIGHT = 1.0
REACH = 2
HIGHEST = lax.Precision.HIGHEST
LANES = 128
EXTRA = 8
MESH = pl.DeviceIdType.MESH


def contract_lanes(left, right):
    dims = (((1,), (1,)), ((), ()))
    return lax.dot_general(left, right, dims, precision=HIGHEST, preferred_element_type=jnp.float32)


def mixing_of(terms_ref, bands):
    mixing = []
    for band in range(bands):
        total = terms_ref[band, 0]
        for other in range(1, bands):
            total = total + terms_ref[band, other]
        row = [terms_ref[band, other] for other in range(bands)]
        row[band] = (1.0 + row[band]) - total
        mixing.append(row)
    return mixing


def mixed(mixing, band, means):
    predicted = mixing[band][0] * means[0]
    for other in range(1, len(means)):
        predicted = predicted + mixing[band][other] * means[other]
    return predicted


def couple(bands, obs, list_len, rows, terms_ref, data_ref, places_ref, out_ref):
    blocks = data_ref.shape[3] // rows
    mixing = mixing_of(terms_ref, bands)
    row_band = lax.broadcasted_iota(jnp.int32, (LANES, LANES), 0) // list_len
    lane_band = lax.broadcasted_iota(jnp.int32, (LANES, LANES), 1) // list_len
    mix_grid = jnp.zeros((LANES, LANES), jnp.float32)
    for band in range(bands):
        for other in range(bands):
            here = (row_band == other) & (lane_band == band)
            mix_grid = jnp.where(here, mixing[band][other], mix_grid)
    full = []
    entry = lax.broadcasted_iota(jnp.int32, (list_len, rows), 0)
    for block in range(blocks):
        cols = pl.ds(block * rows, rows)
        one_hot, one_hot_mag, star_weight, means = [], [], [], []
        for band in range(bands):
            mags = data_ref[band, 0, :, cols]
            wts = data_ref[band, 1, :, cols]
            slots = places_ref[band, :, cols]
            scaled = wts * mags
            weight_sum = jnp.sum(wts, axis=0, keepdims=True)
            star_weight.append(weight_sum)
            means.append(jnp.sum(scaled, axis=0, keepdims=True) / weight_sum)
            hot = jnp.zeros((list_len, rows), jnp.float32)
            hot_mag = jnp.zeros((list_len, rows), jnp.float32)
            for k in range(obs):
                hit = slots[k : k + 1] == entry
                hot = hot + jnp.where(hit, wts[k : k + 1], 0.0)
                hot_mag = hot_mag + jnp.where(hit, scaled[k : k + 1], 0.0)
            one_hot.append(hot)
            one_hot_mag.append(hot_mag)
        rest = []
        shares = []
        for band in range(bands):
            rest.append(one_hot_mag[band] - one_hot[band] * mixed(mixing, band, means))
            shares.append(one_hot[band] / star_weight[band])
        hot_all = jnp.concatenate(one_hot, axis=0)
        share_all = jnp.concatenate(shares, axis=0)
        rest_all = jnp.concatenate(rest, axis=0)
        coupling = contract_lanes(share_all, hot_all) * mix_grid
        ones = jnp.ones((8, rows), jnp.float32)
        rest_row = contract_lanes(ones, rest_all)
        weight_row = contract_lanes(ones, hot_all)
        first = lax.broadcasted_iota(jnp.int32, (EXTRA, LANES), 0) == 0
        full.append(jnp.concatenate([coupling, jnp.where(first, rest_row, weight_row)], axis=0))
    split = bands // 2
    for part in range(split):
        pieces = []
        for half in range(2):
            band = half * split + part
            for block in range(blocks):
                pieces.append(full[block][:, band * list_len : (band + 1) * list_len])
        out_ref[part] = jnp.concatenate(pieces, axis=1)


def sweep_kernel(
    tiles, bands, obs, list_len, rows, row_count,
    window_ref, terms_ref, coupled_ref, pick_ref, color_ref,
    data_ref, data_places_ref, mags_ref, wts_ref, places_ref, chosen_ref,
    own_zp_ref, means_ref, sums_ref,
    kt, base, tot, rden, zp, move, lines, stage, sems,
):
    groups = row_count // 8
    pack = LANES // list_len
    split = bands // 2
    levels, places = pick_ref.shape[:2]
    depth = stage.shape[0]
    lane = lax.broadcasted_iota(jnp.int32, (8, LANES), 1)
    lane_wide = lax.broadcasted_iota(jnp.int32, (LANES + EXTRA, LANES), 1)

    def fetch(row, slot):
        return pltpu.make_async_copy(
            coupled_ref.at[pl.ds(row * (2 * split), 2 * split)], stage.at[slot], sems.at[slot]
        )

    for row in range(depth - 1):
        fetch(row, row).start()

    def unpack(row, carry):
        slot = lax.rem(row, depth)
        ahead = row + depth - 1

        @pl.when(ahead < row_count)
        def _():
            fetch(ahead, lax.rem(ahead, depth)).start()

        fetch(row, slot).wait()
        group = lax.div(row, 8)
        place = lax.rem(row, 8)
        for part in range(split):
            left = stage[slot, part]
            right = stage[slot, split + part]
            low = jnp.where(lane_wide < LANES // 2, left, pltpu.roll(right, LANES // 2, 1))
            high = jnp.where(lane_wide < LANES // 2, pltpu.roll(left, LANES // 2, 1), right)
            for band, value in ((part, low), (split + part, high)):
                start = (group * bands + band) * (LANES * 8) + place
                kt[pl.ds(start, LANES, stride=8), :] = value[0:LANES]
                base[band, pl.ds(row, 1), :] = value[LANES : LANES + 1]
                tot[band, pl.ds(row + 8, 1), :] = value[LANES + 1 : LANES + 2]
        return carry

    lax.fori_loop(0, row_count, unpack, 0)

    def rows_of(group):
        return pl.ds(pl.multiple_of(group * 8, 8), 8)

    def wrap():
        for band in range(bands):
            tot[band, 0:8, :] = tot[band, row_count : row_count + 8, :]
            tot[band, row_count + 8 : row_count + 16, :] = tot[band, 8:16, :]

    def gather(group, first, count, sums):
        for place in range(places):
            start = group * 8 + (8 + place - places // 2)
            near = [tot[band, pl.ds(start, 8), :] for band in range(bands)]
            for level in range(count):
                pick = pick_ref[first + level, place, rows_of(group), :]
                mask = pick < LANES
                lanes = pick & (LANES - 1)
                for band in range(bands):
                    index = 2 * band + level % 2
                    sums[index] = sums[index] + jnp.where(mask, take(near[band], lanes), 0.0)
        return sums

    def gathered(group):
        sums = []
        for band in range(bands):
            sums += [tot[band, pl.ds(pl.multiple_of(group * 8 + 8, 8), 8), :], jnp.zeros((8, LANES), jnp.float32)]
        sums = gather(group, 0, 2, sums)
        sums = lax.fori_loop(2, window_ref[0, 2], lambda level, sums: gather(group, level, 1, sums), sums)
        return [sums[2 * band] + sums[2 * band + 1] for band in range(bands)]

    def weigh(group, carry):
        for band, value in enumerate(gathered(group)):
            rden[band, rows_of(group), :] = 1.0 / (value + PRIOR_WEIGHT)
        return carry

    wrap()
    lax.fori_loop(0, groups, weigh, 0)
    zp[...] = jnp.zeros_like(zp)
    tot[:, 8 : row_count + 8, :] = base[...]
    wrap()

    def push(width, origin):
        def add(group, inner):
            here = [move[band, rows_of(group), :] for band in range(bands)]
            middle = pl.ds(pl.multiple_of(group * 8 + 8, 8), 8)
            sums = [tot[band, middle, :] for band in range(bands)]
            for entry in range(width):
                lanes = (lane & (LANES - list_len)) + (origin + entry)
                values = [take(here[band], lanes) for band in range(bands)]
                for band in range(bands):
                    for other in range(bands):
                        start = (group * bands + band) * (LANES * 8) + (other * list_len + origin + entry) * 8
                        rows = pl.ds(pl.multiple_of(start, 8), 8)
                        sums[band] = sums[band] + values[other] * kt[rows, :]
            for band in range(bands):
                tot[band, middle, :] = sums[band]
            return inner

        lax.fori_loop(0, groups, add, 0, unroll=2)

    halves = rows // LANES
    stars = mags_ref.shape[1]
    blocks = stars // rows
    tile_rows = blocks // pack
    mine = data_ref.shape[3] // rows
    my_tile, my_band = lax.axis_index("sky"), lax.axis_index("band")
    first = lax.rem(my_band * mine, pack)
    my_row = my_tile * tile_rows + lax.div(my_band * mine, pack)
    mixing = mixing_of(terms_ref, bands)
    lines[...] = jnp.zeros_like(lines)

    def spread(row, picks):
        return take(jnp.broadcast_to(row, (obs, LANES)), picks)

    def misfit_lines(sweep):
        partial = [jnp.zeros((obs, LANES), jnp.float32) for _ in range(bands)]
        for block in range(mine):
            for half in range(halves):
                cols = pl.ds(block * rows + half * LANES, LANES)
                left, means = [], []
                for band in range(bands):
                    wts = data_ref[band, 1, :, cols]
                    picks = data_places_ref[band, :, cols] + (first + block) * list_len
                    mags = data_ref[band, 0, :, cols] - spread(zp[band, pl.ds(my_row, 1), :], picks)
                    left.append(mags)
                    means.append(jnp.sum(wts * mags, axis=0, keepdims=True) / jnp.sum(wts, axis=0, keepdims=True))
                for band in range(bands):
                    wts = data_ref[band, 1, :, cols]
                    partial[band] = partial[band] + wts * (left[band] - mixed(mixing, band, means)) ** 2
        for band in range(bands):
            lines[pl.ds(sweep * bands + band, 1), :] = jnp.sum(partial[band], axis=0, keepdims=True)

    def step(number, carry):
        color_no = lax.rem(number, COLORS)

        def update(group, inner):
            rows = rows_of(group)
            now = color_ref[rows, :] == color_no
            for band, value in enumerate(gathered(group)):
                old = zp[band, rows, :]
                new = jnp.where(now, value * rden[band, rows, :], old)
                zp[band, rows, :] = new
                move[band, rows, :] = new - old
            return inner

        lax.fori_loop(0, groups, update, 0, unroll=2)

        @pl.when(color_no == COLORS - 1)
        def _():
            misfit_lines(lax.div(number, COLORS))

        low, high = window_ref[color_no, 0], window_ref[color_no, 1]
        widths = (list_len // 4, list_len * 3 // 8, list_len // 2)
        for index, width in enumerate(widths):
            fits = high - low <= width
            if index:
                fits = fits & (high - low > widths[index - 1])

            @pl.when(fits)
            def _(width=width):
                push(width, jnp.minimum(low, list_len - width))

        @pl.when(high - low > widths[-1])
        def _():
            lax.fori_loop(0, 2, lambda part, inner: (push(widths[-1], part * widths[-1]), inner)[1], 0)

        wrap()
        return carry

    lax.fori_loop(0, SWEEPS * COLORS, step, 0)
    sums_ref[...] = contract_lanes(jnp.ones((8, LANES), jnp.float32), lines[...])
    for block in range(blocks):
        row = zp[my_band, pl.ds(my_tile * tile_rows + block // pack, 1), :]
        for half in range(halves):
            cols = pl.ds(block * rows + half * LANES, LANES)
            wts = wts_ref[:, cols]
            picks = places_ref[:, cols] + block % pack * list_len
            left = wts * (mags_ref[:, cols] - spread(row, picks))
            means_ref[0:1, cols] = jnp.sum(left, axis=0, keepdims=True) / jnp.sum(wts, axis=0, keepdims=True)
    below = lax.broadcasted_iota(jnp.int32, (8, LANES), 0)
    close = jnp.zeros((8, LANES), jnp.float32)
    for offset in range(3):
        tile = lax.rem(my_tile + offset + tiles - 1, tiles)
        for row in range(tile_rows):
            value = zp[my_band, pl.ds(tile * tile_rows + row, 1), :]
            close = jnp.where(below == offset * tile_rows + row, jnp.broadcast_to(value, (8, LANES)), close)
    owned = own_zp_ref.shape[1]
    for row in range(chosen_ref.shape[0]):
        pick = chosen_ref[row]
        value = jnp.where(pick < LANES, take(close, pick & (LANES - 1)), 0.0)
        value = jnp.sum(value, axis=0, keepdims=True)
        width = min(LANES, owned - row * LANES)
        own_zp_ref[0:1, row * LANES : row * LANES + width] = value[:, 0:width]


def take(value, picks):
    return jnp.take_along_axis(value, picks, axis=1, mode="promise_in_bounds")


def sort_entries(list_len, fields, listed, color_ref):
    lane = lax.broadcasted_iota(jnp.int32, (8, LANES), 1)
    segment = lane & (LANES - list_len)
    live = listed < fields
    row_no, lane_no = listed // LANES, listed % LANES
    color = jnp.full((8, LANES), -1, jnp.int32)
    for row in range(color_ref.shape[0]):
        table = jnp.broadcast_to(color_ref[row : row + 1, :], (8, LANES))
        color = jnp.where(row_no == row, take(table, lane_no), color)
    color = jnp.where(live, color, -1)
    masks = jnp.concatenate([(color == c).astype(jnp.float32) for c in range(COLORS)], axis=0)
    source = lax.broadcasted_iota(jnp.int32, (LANES, LANES), 0)
    target = lax.broadcasted_iota(jnp.int32, (LANES, LANES), 1)
    same = (source // list_len) == (target // list_len)
    dims = (((1,), (0,)), ((), ()))
    before = (same & (source < target)).astype(jnp.float32)
    ranks = lax.dot_general(masks, before, dims, preferred_element_type=jnp.float32)
    counts = lax.dot_general(masks, same.astype(jnp.float32), dims, preferred_element_type=jnp.float32)
    rest = jnp.zeros((8, LANES), jnp.float32)
    room = [None] * COLORS
    for c in reversed(range(COLORS)):
        rest = rest + counts[c * 8 : c * 8 + 8]
        room[c] = list_len - rest
    end = jnp.zeros((8, LANES), jnp.float32)
    place = jnp.full((8, LANES), -1.0, jnp.float32)
    for c in range(COLORS):
        start = jnp.minimum(jnp.maximum(end, float(list_len * c // COLORS)), room[c])
        end = start + counts[c * 8 : c * 8 + 8]
        place = jnp.where(color == c, start + ranks[c * 8 : c * 8 + 8], place)
    place = place.astype(jnp.int32)
    sorted_fields = jnp.full((8, LANES), fields, jnp.int32)
    sorted_colors = jnp.full((8, LANES), -1, jnp.int32)
    for entry in range(list_len):
        picks = segment + entry
        hit = take(place, picks) == lane - segment
        sorted_fields = jnp.where(hit, take(listed, picks), sorted_fields)
        sorted_colors = jnp.where(hit, take(color, picks), sorted_colors)
    return place, sorted_fields, sorted_colors


def match(list_len, fields, lists_ref, rows_ref, pick_ref, color_ref):
    tiles, _, tile_rows, _ = lists_ref.shape
    pack = LANES // list_len
    levels, places, row_count, _ = pick_ref.shape
    lane = lax.broadcasted_iota(jnp.int32, (8, LANES), 1)
    for tile in range(tiles):
        start = tile * tile_rows
        rows_ref[8 + start : 8 + start + tile_rows, :] = lists_ref[tile, 0]
        color_ref[start : start + tile_rows, :] = lists_ref[tile, 1]
    rows_ref[0:8, :] = rows_ref[row_count : row_count + 8, :]
    rows_ref[row_count + 8 : row_count + 16, :] = rows_ref[8:16, :]

    def group_picks(group, carry):
        home = rows_ref[pl.ds(pl.multiple_of(group * 8 + 8, 8), 8), :]
        home = jnp.where(home < fields, home, -1)
        near = [rows_ref[pl.ds(group * 8 + 8 + place - places // 2, 8), :] for place in range(places)]
        found = [[] for _ in range(places)]
        for quarter in range(pack):
            picks = [jnp.full((8, LANES), LANES, jnp.int32) for _ in range(places)]
            for entry in range(list_len):
                source = quarter * list_len + entry
                for place in range(places):
                    other = jnp.broadcast_to(near[place][:, source : source + 1], (8, LANES))
                    picks[place] = jnp.where(other == home, source, picks[place])
            for place in range(places):
                found[place].append(picks[place])
        rows = pl.ds(pl.multiple_of(group * 8, 8), 8)
        for place in range(places):
            ranked = found[place]
            if place == places // 2:
                ranked = [jnp.where(pick == lane, LANES, pick) for pick in ranked]
            for turn in range(pack):
                for low in range(turn % 2, pack - 1, 2):
                    pair = ranked[low], ranked[low + 1]
                    ranked[low], ranked[low + 1] = jnp.minimum(*pair), jnp.maximum(*pair)
            for level in range(pack):
                pick_ref[level, place, rows, :] = ranked[level]
        return carry

    lax.fori_loop(0, row_count // 8, group_picks, 0)


def windows(list_len, pick_ref, color_ref, window_ref):
    levels, places, row_count, _ = pick_ref.shape
    lane = lax.broadcasted_iota(jnp.int32, (8, LANES), 1)
    position = (lane & (list_len - 1)).astype(jnp.float32)

    def rows_of(group):
        return pl.ds(pl.multiple_of(group * 8, 8), 8)

    def bounds(group, carry):
        lows, highs = carry
        color = color_ref[rows_of(group), :]
        new_lows, new_highs = [], []
        for c in range(COLORS):
            new_lows.append(jnp.minimum(lows[c], jnp.where(color == c, position, float(list_len))))
            new_highs.append(jnp.maximum(highs[c], jnp.where(color == c, position + 1.0, 0.0)))
        return new_lows, new_highs

    start = [jnp.full((8, LANES), float(list_len), jnp.float32)] * COLORS, [jnp.zeros((8, LANES), jnp.float32)] * COLORS
    lows, highs = lax.fori_loop(0, row_count // 8, bounds, start)
    lows = jnp.concatenate([jnp.min(value, axis=0, keepdims=True) for value in lows], axis=0)
    highs = jnp.concatenate([jnp.max(value, axis=0, keepdims=True) for value in highs], axis=0)
    lows = jnp.min(lows, axis=1, keepdims=True)
    highs = jnp.max(highs, axis=1, keepdims=True)
    deepest = jnp.full((8, LANES), 2.0, jnp.float32)
    for level in range(2, levels):
        def least(group, value, level=level):
            for place in range(places):
                value = jnp.minimum(value, pick_ref[level, place, rows_of(group), :])
            return value

        found = lax.fori_loop(0, row_count // 8, least, jnp.full((8, LANES), LANES, jnp.int32))
        deepest = jnp.where(found < LANES, level + 1.0, deepest)
    deepest = jnp.max(jnp.max(deepest, axis=0, keepdims=True), axis=1, keepdims=True)
    table = jnp.where(lane == 0, lows, jnp.where(lane == 1, highs, deepest))
    window_ref[...] = table.astype(jnp.int32)


def choose(tiles, fields, owner_ref, rows_ref, chosen_ref):
    field_rows = owner_ref.shape[0]
    tile_rows = (rows_ref.shape[0] - 16) // tiles
    my_tile = lax.axis_index("sky")
    lane = lax.broadcasted_iota(jnp.int32, (8, LANES), 1)
    below = lax.broadcasted_iota(jnp.int32, (8, LANES), 0)
    owned = owner_ref[...] == my_tile
    ones = owned.astype(jnp.float32)
    source = lax.broadcasted_iota(jnp.int32, (LANES, LANES), 0)
    target = lax.broadcasted_iota(jnp.int32, (LANES, LANES), 1)
    dims = (((1,), (0,)), ((), ()))
    inside = lax.dot_general(ones, (source < target).astype(jnp.float32), dims, preferred_element_type=jnp.float32)
    counts = lax.dot_general(ones, jnp.ones((LANES, LANES), jnp.float32), dims, preferred_element_type=jnp.float32)
    upper = lax.broadcasted_iota(jnp.int32, (field_rows, field_rows), 1)
    lower = lax.broadcasted_iota(jnp.int32, (field_rows, field_rows), 0)
    above = lax.dot_general((upper < lower).astype(jnp.float32), counts, dims, preferred_element_type=jnp.float32)
    rank = jnp.where(owned, (inside + above).astype(jnp.int32), -1)
    close = jnp.full((8, LANES), fields, jnp.int32)
    for offset in range(3):
        tile = lax.rem(my_tile + offset + tiles - 1, tiles)
        for row in range(tile_rows):
            value = rows_ref[pl.ds(8 + tile * tile_rows + row, 1), :]
            close = jnp.where(below == offset * tile_rows + row, jnp.broadcast_to(value, (8, LANES)), close)
    row_no, lane_no = close // LANES, close % LANES
    order = jnp.full((8, LANES), -1, jnp.int32)
    for row in range(field_rows):
        table = jnp.broadcast_to(rank[row : row + 1, :], (8, LANES))
        order = jnp.where(row_no == row, take(table, lane_no), order)
    own_rows = chosen_ref.shape[0]
    codes = [jnp.full((8, LANES), -1, jnp.int32) for _ in range(own_rows)]
    for entry in range(LANES):
        value = jnp.broadcast_to(order[:, entry : entry + 1], (8, LANES))
        for row in range(own_rows):
            codes[row] = jnp.where(value == row * LANES + lane, entry, codes[row])
    for row in range(own_rows):
        ranked = jnp.where(codes[row] >= 0, (below + 1).astype(jnp.float32), 0.0)
        last = jnp.max(ranked, axis=0, keepdims=True)
        keep = (ranked > 0.0) & (ranked == last)
        chosen_ref[row] = jnp.where(keep, codes[row], LANES)


def relabel(list_len, rows, block, offset, place_ref, slots_ref, out_ref):
    pack = LANES // list_len
    table = jnp.broadcast_to(place_ref[pl.ds(block // pack, 1), :], (slots_ref.shape[0], LANES))
    for half in range(rows // LANES):
        cols = pl.ds(offset + half * LANES, LANES)
        out_ref[:, cols] = take(table, slots_ref[:, cols] + block % pack * list_len)


def gather_kernel(
    tiles, bands, obs, list_len, rows, fields,
    terms_ref, tile_lists_ref, field_colors_ref, mags_ref, wts_ref, slots_ref, owner_ref,
    all_ref, pick_ref, color_ref, window_ref, chosen_ref, data_ref, data_places_ref, places_ref,
    rows_ref, own_ref, listed_ref, place_ref, sorted_ref, lists_ref, data_slots_ref,
    send_sems, recv_sems, early_send_sems, early_recv_sems,
):
    high_count = tiles // 2
    blocks = tile_lists_ref.shape[0]
    pack = LANES // list_len
    tile_rows = blocks // pack
    mine = blocks // bands
    width = mine * rows
    sky, band = lax.axis_index("sky"), lax.axis_index("band")
    high, low = sky // 2, sky % 2
    side, core = band // 2, band % 2
    to_low = {"sky": high * 2 + (1 - low)}
    to_side = {"band": (1 - side) * 2 + core}
    to_core = {"band": side * 2 + (1 - core)}
    barrier = pltpu.get_barrier_semaphore()
    tile_peers = [lax.rem(sky + step, tiles) for step in range(1, tiles)]
    band_peers = [lax.rem(band + step, bands) for step in range(1, bands)]
    for peer in tile_peers:
        pl.semaphore_signal(barrier, inc=1, device_id={"sky": peer}, device_id_type=MESH)
    for peer in band_peers:
        pl.semaphore_signal(barrier, inc=1, device_id={"band": peer}, device_id_type=MESH)

    listed_ref[...] = jnp.full((8, LANES), fields, jnp.int32)
    for row in range(tile_rows):
        pieces = [tile_lists_ref[row * pack + part : row * pack + part + 1, :] for part in range(pack)]
        listed_ref[row : row + 1, :] = jnp.concatenate(pieces, axis=1)
    place, sorted_fields, sorted_colors = sort_entries(list_len, fields, listed_ref[...], field_colors_ref)
    place_ref[...] = place
    sorted_ref[0] = sorted_fields[0:tile_rows]
    sorted_ref[1] = sorted_colors[0:tile_rows]
    lists_ref[sky] = sorted_ref[...]
    pl.semaphore_wait(barrier, tiles + bands - 2)

    def early(number, source, target, device):
        copy = pltpu.make_async_remote_copy(
            src_ref=source,
            dst_ref=target,
            send_sem=early_send_sems.at[number],
            recv_sem=early_recv_sems.at[number],
            device_id=device,
            device_id_type=MESH,
        )
        copy.start()
        return copy

    def columns(peer):
        return pl.ds(pl.multiple_of(peer * width, LANES), width)

    data_copies, list_copies = [], []
    for step, peer in enumerate(band_peers):
        cols = columns(peer)
        for kind, (source, target) in enumerate((
            (slots_ref, data_slots_ref.at[band]),
            (wts_ref, data_ref.at[band, 1]),
            (mags_ref, data_ref.at[band, 0]),
        )):
            data_copies.append(early(3 * step + kind, source.at[:, cols], target, {"band": peer}))
    for step, peer in enumerate(tile_peers):
        list_copies.append(early(3 * (bands - 1) + step, sorted_ref, lists_ref.at[sky], {"sky": peer}))
    data_ref[band, 0] = mags_ref[:, columns(band)]
    data_ref[band, 1] = wts_ref[:, columns(band)]
    data_slots_ref[band] = slots_ref[:, columns(band)]
    for block in range(blocks):
        relabel(list_len, rows, block, block * rows, place_ref, slots_ref, places_ref)
    for copy in data_copies:
        copy.wait_recv()
    for other in range(bands):
        for block in range(mine):
            source, target = data_slots_ref.at[other], data_places_ref.at[other]
            relabel(list_len, rows, band * mine + block, block * rows, place_ref, source, target)

    def tables():
        for copy in list_copies:
            copy.wait_recv()
        match(list_len, fields, lists_ref, rows_ref, pick_ref, color_ref)

    def more_tables():
        windows(list_len, pick_ref, color_ref, window_ref)
        choose(tiles, fields, owner_ref, rows_ref, chosen_ref)
        for copy in data_copies + list_copies:
            copy.wait_send()

    if high_count > 4:
        highs = [lax.rem(high + step, high_count) for step in range(1, high_count)]
        peers = [{"sky": peer * 2 + low} for peer in highs]
        couple(bands, obs, list_len, rows, terms_ref, data_ref, data_places_ref, own_ref)
        count = [0]

        def send(source, target, peer):
            copy = pltpu.make_async_remote_copy(
                src_ref=source,
                dst_ref=target,
                send_sem=send_sems.at[count[0]],
                recv_sem=recv_sems.at[count[0]],
                device_id=peer,
                device_id_type=MESH,
            )
            count[0] += 1
            copy.start()
            return copy

        def wait(copies):
            for copy in copies:
                copy.wait()

        mine = all_ref.at[high, low, side, core]
        copies = [send(own_ref, mine, peer) for peer in peers]
        all_ref[high, low, side, core] = own_ref[...]
        tables()
        more_tables()
        wait(copies)

        column = all_ref.at[:, low, side, core]
        first = all_ref.at[:, low, side, core, 0]
        second = all_ref.at[:, low, side, core, 1]
        copies = [send(first, first, to_low), send(second, second, to_side)]
        late = [send(column, column, to_core)]
        wait(copies)

        first = all_ref.at[:, :, side, core, 0]
        second = all_ref.at[:, low, :, core, 1]
        copies = [send(first, first, to_side), send(second, second, to_low)]
        for part in (all_ref.at[:, 1 - low, side, core, 0], all_ref.at[:, low, 1 - side, core, 1]):
            late.append(send(part, part, to_core))
        wait(copies)

        for part in (all_ref.at[:, :, 1 - side, core, 0], all_ref.at[:, 1 - low, :, core, 1]):
            late.append(send(part, part, to_core))
        wait(late)
        return

    chunks = high_count * 8
    lower, upper = high > 0, high < high_count - 1
    own_chunk = all_ref.at[high, low, side, core]
    couple(bands, obs, list_len, rows, terms_ref, data_ref, data_places_ref, own_chunk)
    def copy_of(kind, z, y, x, part, peer, landing):
        chunk = all_ref.at[z, y, x, core, part]
        number = ((z * 2 + y) * 2 + x) * 2 + part
        return pltpu.make_async_remote_copy(
            src_ref=chunk,
            dst_ref=chunk,
            send_sem=send_sems.at[kind * chunks + number],
            recv_sem=recv_sems.at[landing * chunks + number],
            device_id=peer,
            device_id_type=MESH,
        )

    def along(z, part, step):
        return copy_of((step + 1) // 2, z, low, side, part, {"sky": (high + step) * 2 + low}, 0)

    def across_x(z, y, part):
        return copy_of(2, z, y, side, part, to_side, 0)

    def across_y(z, x, part):
        return copy_of(3, z, low, x, part, to_low, 0)

    def over(z, y, x, part):
        return copy_of(4, z, y, x, part, to_core, 1)

    def arrived(z, y, x, part):
        copy_of(4, z, y, x, part, to_core, 0).wait_recv()

    ends = {-1: lower, 1: upper}

    def along_if(z, part, step):
        @pl.when(ends[step])
        def _():
            along(z, part, step).start()

    def first_hop(z, part):
        if part == 0:
            across_x(z, low, part).start()
        else:
            across_y(z, side, part).start()

    def second_hop(z, part):
        if part == 0:
            across_y(z, side, part).start()
        else:
            across_x(z, low, part).start()

    for part in range(2):
        along_if(high, part, 1)
        along_if(high, part, -1)
        first_hop(high, part)
    for part in range(2):
        second_hop(high, part)
        over(high, low, side, part).start()
    tables()

    def column_arrival(distance, part):
        for step in (-1, 1):
            z = high - step * distance
            here = z >= 0 if step == 1 else z < high_count

            @pl.when(here)
            def _(z=z, step=step):
                arrived(z, low, side, part)
                along_if(z, part, step)
                first_hop(z, part)
                second_hop(z, part)
                over(z, low, side, part).start()

    def at_distance(distance, action):
        if distance == 0:
            action(high)
            return
        for step in (-1, 1):
            z = high - step * distance

            @pl.when(z >= 0 if step == 1 else z < high_count)
            def _(z=z):
                action(z)

    def turn(z):
        arrived(z, low, 1 - side, 0)
        across_y(z, 1 - side, 0).start()
        over(z, low, 1 - side, 0).start()
        arrived(z, 1 - low, side, 1)
        across_x(z, 1 - low, 1).start()
        over(z, 1 - low, side, 1).start()

    def last(z):
        for y, x, part in ((1 - low, side, 0), (low, 1 - side, 1), (1 - low, 1 - side, 0), (1 - low, 1 - side, 1)):
            arrived(z, y, x, part)
            over(z, y, x, part).start()

    for distance in range(1, high_count):
        column_arrival(distance, 0)
        at_distance(distance - 1, turn)
        column_arrival(distance, 1)
        if distance > 1:
            at_distance(distance - 2, last)
        if distance == 1:
            more_tables()
    at_distance(high_count - 1, turn)
    for distance in range(max(high_count - 2, 0), high_count):
        at_distance(distance, last)

    for z in range(high_count):
        for y in range(2):
            for x in range(2):
                for part in range(2):
                    copy_of(4, z, y, x, part, to_core, 1).wait()
    for z in range(high_count):
        for part in range(2):
            for step in (-1, 1):
                passing = (z >= high) if step == -1 else (z <= high)

                @pl.when(ends[step] & passing)
                def _(z=z, part=part, step=step):
                    along(z, part, step).wait_send()

            for other in range(2):
                if part == 0:
                    across_y(z, other, part).wait_send()
                else:
                    across_x(z, other, part).wait_send()
            first = across_x(z, low, part) if part == 0 else across_y(z, side, part)
            first.wait_send()


def total_kernel(tiles, bands, scale, sums_ref, misfit_ref, all_sums, send_sems, recv_sems):
    my_tile, my_band = lax.axis_index("sky"), lax.axis_index("band")
    me = my_tile * bands + my_band
    peers = []
    for sky_step in range(tiles):
        for band_step in range(bands):
            if sky_step or band_step:
                peers.append({"sky": lax.rem(my_tile + sky_step, tiles), "band": lax.rem(my_band + band_step, bands)})
    barrier = pltpu.get_barrier_semaphore()
    for peer in peers:
        pl.semaphore_signal(barrier, inc=1, device_id=peer, device_id_type=MESH)
    all_sums[pl.ds(me, 1), :] = sums_ref[0:1, :]
    pl.semaphore_wait(barrier, len(peers))
    copies = []
    for number, peer in enumerate(peers):
        copy = pltpu.make_async_remote_copy(
            src_ref=sums_ref.at[0:1],
            dst_ref=all_sums.at[pl.ds(me, 1)],
            send_sem=send_sems.at[number],
            recv_sem=recv_sems.at[number],
            device_id=peer,
            device_id_type=MESH,
        )
        copy.start()
        copies.append(copy)
    for copy in copies:
        copy.wait()
    total = jnp.sum(all_sums[...], axis=0, keepdims=True) / scale
    lane = lax.broadcasted_iota(jnp.int32, (8, LANES), 1)
    picks = (lane * bands + my_band) & (LANES - 1)
    misfit_ref[...] = take(jnp.broadcast_to(total, (8, LANES)), picks)[0:1, 0:SWEEPS]


def body(magnitudes, weights, slots, block_fields, owner, colors, color_terms):
    bands = color_terms.shape[0]
    tiles = lax.axis_size("sky")
    _, obs, stars = magnitudes.shape
    blocks, list_len = block_fields.shape
    rows = stars // blocks
    fields = owner.shape[0]
    owned = fields // tiles
    mine = blocks // bands
    pack = LANES // list_len
    tile_rows = blocks // pack
    row_count = tiles * tile_rows
    vmem = pl.BlockSpec(memory_space=pltpu.VMEM)
    smem = pl.BlockSpec(memory_space=pltpu.SMEM)
    hbm = pl.BlockSpec(memory_space=pl.ANY)
    magnitudes, weights, slots = magnitudes[0], weights[0], slots[0]

    earlier = 3 * (bands - 1) + tiles - 1
    reach = 2 * (REACH * tile_rows + tile_rows - 1) + 1
    own_rows = -(-owned // LANES)
    part = (bands // 2, LANES + EXTRA, LANES)
    everyone = (tiles // 2, 2, bands // 2, 2) + part
    listed = (tiles, 2, tile_rows, LANES)
    if tiles > 8:
        sends = landings = tiles // 2 - 1 + 9
    else:
        sends, landings = 5 * tiles * 4, 2 * tiles * 4
    coupled, pick, entry_colors, window, chosen, data, data_places, places = pl.pallas_call(
        functools.partial(gather_kernel, tiles, bands, obs, list_len, rows, fields),
        out_shape=(
            jax.ShapeDtypeStruct(everyone, jnp.float32),
            jax.ShapeDtypeStruct((pack, reach, row_count, LANES), jnp.int32),
            jax.ShapeDtypeStruct((row_count, LANES), jnp.int32),
            jax.ShapeDtypeStruct((8, LANES), jnp.int32),
            jax.ShapeDtypeStruct((own_rows, 8, LANES), jnp.int32),
            jax.ShapeDtypeStruct((bands, 2, obs, mine * rows), jnp.float32),
            jax.ShapeDtypeStruct((bands, obs, mine * rows), jnp.int32),
            jax.ShapeDtypeStruct((obs, stars), jnp.int32),
        ),
        in_specs=[smem] + [vmem] * 6,
        out_specs=(vmem,) * 8,
        scratch_shapes=[
            pltpu.VMEM((row_count + 16, LANES), jnp.int32),
            pltpu.VMEM(part, jnp.float32),
            pltpu.VMEM((8, LANES), jnp.int32),
            pltpu.VMEM((8, LANES), jnp.int32),
            pltpu.VMEM(listed[1:], jnp.int32),
            pltpu.VMEM(listed, jnp.int32),
            pltpu.VMEM((bands, obs, mine * rows), jnp.int32),
            pltpu.SemaphoreType.DMA((sends,)),
            pltpu.SemaphoreType.DMA((landings,)),
            pltpu.SemaphoreType.DMA((earlier,)),
            pltpu.SemaphoreType.DMA((earlier,)),
        ],
        compiler_params=pltpu.CompilerParams(
            collective_id=0, has_side_effects=True, vmem_limit_bytes=60 * 1024 * 1024
        ),
        name="gather",
    )(color_terms, block_fields, colors.reshape(-1, LANES), magnitudes, weights, slots, owner.reshape(-1, LANES))
    coupled = coupled.reshape((-1,) + coupled.shape[-2:])

    big = (bands, row_count, LANES)
    depth = min(row_count, 16)
    own_zp, star_means, sums = pl.pallas_call(
        functools.partial(sweep_kernel, tiles, bands, obs, list_len, rows, row_count),
        out_shape=(
            jax.ShapeDtypeStruct((1, owned), jnp.float32),
            jax.ShapeDtypeStruct((1, stars), jnp.float32),
            jax.ShapeDtypeStruct((8, LANES), jnp.float32),
        ),
        in_specs=[smem, smem, hbm] + [vmem] * 8,
        out_specs=(vmem,) * 3,
        scratch_shapes=[
            pltpu.VMEM((row_count * bands * LANES, LANES), jnp.float32),
            pltpu.VMEM(big, jnp.float32),
            pltpu.VMEM((bands, row_count + 16, LANES), jnp.float32),
            pltpu.VMEM(big, jnp.float32),
            pltpu.VMEM(big, jnp.float32),
            pltpu.VMEM(big, jnp.float32),
            pltpu.VMEM((LANES, LANES), jnp.float32),
            pltpu.VMEM((depth, bands, LANES + EXTRA, LANES), jnp.float32),
            pltpu.SemaphoreType.DMA((depth,)),
        ],
        compiler_params=pltpu.CompilerParams(vmem_limit_bytes=60 * 1024 * 1024),
        name="sweeps",
    )(window, color_terms, coupled, pick, entry_colors, data, data_places, magnitudes, weights, places, chosen)

    devices = tiles * bands
    misfit = pl.pallas_call(
        functools.partial(total_kernel, tiles, bands, float(obs * stars * tiles)),
        out_shape=jax.ShapeDtypeStruct((1, SWEEPS), jnp.float32),
        in_specs=[vmem],
        out_specs=vmem,
        scratch_shapes=[
            pltpu.VMEM((devices, LANES), jnp.float32),
            pltpu.SemaphoreType.DMA((devices - 1,)),
            pltpu.SemaphoreType.DMA((devices - 1,)),
        ],
        compiler_params=pltpu.CompilerParams(collective_id=1, has_side_effects=True),
        name="total",
    )(sums)
    return own_zp, star_means, misfit.reshape(SWEEPS, 1)


def solution(mesh):
    in_specs = (
        P("band", None, "sky"),
        P("band", None, "sky"),
        P("band", None, "sky"),
        P("sky", None),
        P(),
        P(),
        P(),
    )
    out_specs = (P("band", "sky"), P("band", "sky"), P(None, "band"))
    return jax.shard_map(body, mesh=mesh, in_specs=in_specs, out_specs=out_specs, check_vma=False)
```

```python
import functools

import jax
import jax.numpy as jnp
from jax import lax
from jax.experimental import pallas as pl
from jax.experimental.pallas import tpu as pltpu
from jax.sharding import PartitionSpec as P

COLORS = 8
SWEEPS = 4
PRIOR_WEIGHT = 1.0
REACH = 2
HIGHEST = lax.Precision.HIGHEST
LANES = 128
EXTRA = 8
MESH = pl.DeviceIdType.MESH


def contract_lanes(left, right):
    dims = (((1,), (1,)), ((), ()))
    return lax.dot_general(left, right, dims, precision=HIGHEST, preferred_element_type=jnp.float32)


def mixing_of(terms_ref, bands):
    mixing = []
    for band in range(bands):
        total = terms_ref[band, 0]
        for other in range(1, bands):
            total = total + terms_ref[band, other]
        row = [terms_ref[band, other] for other in range(bands)]
        row[band] = (1.0 + row[band]) - total
        mixing.append(row)
    return mixing


def mixed(mixing, band, means):
    predicted = mixing[band][0] * means[0]
    for other in range(1, len(means)):
        predicted = predicted + mixing[band][other] * means[other]
    return predicted


def couple(bands, obs, list_len, rows, terms_ref, data_ref, places_ref, out_ref):
    blocks = data_ref.shape[3] // rows
    mixing = mixing_of(terms_ref, bands)
    row_band = lax.broadcasted_iota(jnp.int32, (LANES, LANES), 0) // list_len
    lane_band = lax.broadcasted_iota(jnp.int32, (LANES, LANES), 1) // list_len
    mix_grid = jnp.zeros((LANES, LANES), jnp.float32)
    for band in range(bands):
        for other in range(bands):
            here = (row_band == other) & (lane_band == band)
            mix_grid = jnp.where(here, mixing[band][other], mix_grid)
    full = []
    entry = lax.broadcasted_iota(jnp.int32, (list_len, rows), 0)
    for block in range(blocks):
        cols = pl.ds(block * rows, rows)
        one_hot, one_hot_mag, star_weight, means = [], [], [], []
        for band in range(bands):
            mags = data_ref[band, 0, :, cols]
            wts = data_ref[band, 1, :, cols]
            slots = places_ref[band, :, cols]
            scaled = wts * mags
            weight_sum = jnp.sum(wts, axis=0, keepdims=True)
            star_weight.append(weight_sum)
            means.append(jnp.sum(scaled, axis=0, keepdims=True) / weight_sum)
            hot = jnp.zeros((list_len, rows), jnp.float32)
            hot_mag = jnp.zeros((list_len, rows), jnp.float32)
            for k in range(obs):
                hit = slots[k : k + 1] == entry
                hot = hot + jnp.where(hit, wts[k : k + 1], 0.0)
                hot_mag = hot_mag + jnp.where(hit, scaled[k : k + 1], 0.0)
            one_hot.append(hot)
            one_hot_mag.append(hot_mag)
        rest = []
        shares = []
        for band in range(bands):
            rest.append(one_hot_mag[band] - one_hot[band] * mixed(mixing, band, means))
            shares.append(one_hot[band] / star_weight[band])
        hot_all = jnp.concatenate(one_hot, axis=0)
        share_all = jnp.concatenate(shares, axis=0)
        rest_all = jnp.concatenate(rest, axis=0)
        coupling = contract_lanes(share_all, hot_all) * mix_grid
        ones = jnp.ones((8, rows), jnp.float32)
        rest_row = contract_lanes(ones, rest_all)
        weight_row = contract_lanes(ones, hot_all)
        first = lax.broadcasted_iota(jnp.int32, (EXTRA, LANES), 0) == 0
        full.append(jnp.concatenate([coupling, jnp.where(first, rest_row, weight_row)], axis=0))
    split = bands // 2
    for part in range(split):
        pieces = []
        for half in range(2):
            band = half * split + part
            for block in range(blocks):
                pieces.append(full[block][:, band * list_len : (band + 1) * list_len])
        out_ref[part] = jnp.concatenate(pieces, axis=1)


def sweep_kernel(
    tiles, bands, obs, list_len, rows, row_count,
    window_ref, terms_ref, coupled_ref, pick_hbm_ref, color_ref,
    data_ref, data_places_ref, mags_ref, wts_ref, places_ref, chosen_ref, homes_ref, ranked_ref,
    own_zp_ref, means_ref, sums_ref,
    kt, base, tot, rden, zp, move, lines, pick_ref, pick_sem, wide, twice, ctot, crden, stage, sems,
):
    groups = row_count // 8
    pack = LANES // list_len
    split = bands // 2
    levels, places = pick_ref.shape[:2]
    depth = stage.shape[0]
    lane = lax.broadcasted_iota(jnp.int32, (8, LANES), 1)
    lane_wide = lax.broadcasted_iota(jnp.int32, (LANES + EXTRA, LANES), 1)

    def fetch(row, slot):
        return pltpu.make_async_copy(
            coupled_ref.at[pl.ds(row * (2 * split), 2 * split)], stage.at[slot], sems.at[slot]
        )

    for row in range(depth - 1):
        fetch(row, row).start()

    def unpack(row, carry):
        slot = lax.rem(row, depth)
        ahead = row + depth - 1

        @pl.when(ahead < row_count)
        def _():
            fetch(ahead, lax.rem(ahead, depth)).start()

        fetch(row, slot).wait()
        group = lax.div(row, 8)
        place = lax.rem(row, 8)
        for part in range(split):
            left = stage[slot, part]
            right = stage[slot, split + part]
            low = jnp.where(lane_wide < LANES // 2, left, pltpu.roll(right, LANES // 2, 1))
            high = jnp.where(lane_wide < LANES // 2, pltpu.roll(left, LANES // 2, 1), right)
            for band, value in ((part, low), (split + part, high)):
                start = (group * bands + band) * (LANES * 8) + place
                kt[pl.ds(start, LANES, stride=8), :] = value[0:LANES]
                base[band, pl.ds(row, 1), :] = value[LANES : LANES + 1]
                tot[band, pl.ds(row + 8, 1), :] = value[LANES + 1 : LANES + 2]
        return carry

    lax.fori_loop(0, row_count, unpack, 0)

    def rows_of(group):
        return pl.ds(pl.multiple_of(group * 8, 8), 8)

    def wrap():
        for band in range(bands):
            tot[band, 0:8, :] = tot[band, row_count : row_count + 8, :]
            tot[band, row_count + 8 : row_count + 16, :] = tot[band, 8:16, :]

    def gather(group, first, count, sums):
        for place in range(places):
            start = group * 8 + (8 + place - places // 2)
            near = [tot[band, pl.ds(start, 8), :] for band in range(bands)]
            for level in range(count):
                pick = pick_ref[first + level, place, rows_of(group), :]
                mask = pick < LANES
                lanes = pick & (LANES - 1)
                for band in range(bands):
                    index = 2 * band + level % 2
                    sums[index] = sums[index] + jnp.where(mask, take(near[band], lanes), 0.0)
        return sums

    def gathered(group):
        sums = []
        for band in range(bands):
            sums += [tot[band, pl.ds(pl.multiple_of(group * 8 + 8, 8), 8), :], jnp.zeros((8, LANES), jnp.float32)]
        sums = gather(group, 0, 2, sums)
        sums = lax.fori_loop(2, window_ref[0, 2], lambda level, sums: gather(group, level, 1, sums), sums)
        return [sums[2 * band] + sums[2 * band + 1] for band in range(bands)]

    def weigh(group, carry):
        for band, value in enumerate(gathered(group)):
            rden[band, rows_of(group), :] = 1.0 / (value + PRIOR_WEIGHT)
        return carry

    zp[...] = jnp.zeros_like(zp)

    def push(width, origin, first_lane):
        def add(group, inner):
            here = [move[band, rows_of(group), :] for band in range(bands)]
            middle = pl.ds(pl.multiple_of(group * 8 + 8, 8), 8)
            sums = [tot[band, middle, :] for band in range(bands)]
            for entry in range(width):
                lanes = first_lane + entry
                values = [take(here[band], lanes) for band in range(bands)]
                for band in range(bands):
                    for other in range(bands):
                        start = (group * bands + band) * (LANES * 8) + (other * list_len + origin + entry) * 8
                        rows = pl.ds(pl.multiple_of(start, 8), 8)
                        sums[band] = sums[band] + values[other] * kt[rows, :]
            for band in range(bands):
                tot[band, middle, :] = sums[band]
            return inner

        lax.fori_loop(0, groups, add, 0, unroll=2)

    def push_window(color_no, first_lane):
        low, high = window_ref[color_no, 0], window_ref[color_no, 1]
        widths = (list_len // 4, list_len * 3 // 8, list_len // 2)
        for index, width in enumerate(widths):
            fits = high - low <= width
            if index:
                fits = fits & (high - low > widths[index - 1])

            @pl.when(fits)
            def _(width=width):
                origin = jnp.minimum(low, list_len - width)
                push(width, origin, first_lane(origin))

    halves = rows // LANES
    stars = mags_ref.shape[1]
    blocks = stars // rows
    tile_rows = blocks // pack
    mine = data_ref.shape[3] // rows
    my_tile, my_band = lax.axis_index("sky"), lax.axis_index("band")
    first = lax.rem(my_band * mine, pack)
    my_row = my_tile * tile_rows + lax.div(my_band * mine, pack)
    mixing = mixing_of(terms_ref, bands)
    lines[...] = jnp.zeros_like(lines)

    def spread(row, picks):
        return take(jnp.broadcast_to(row, (obs, LANES)), picks)

    def misfit_lines(sweep):
        partial = [jnp.zeros((obs, LANES), jnp.float32) for _ in range(bands)]
        for block in range(mine):
            for half in range(halves):
                cols = pl.ds(block * rows + half * LANES, LANES)
                left, means = [], []
                for band in range(bands):
                    wts = data_ref[band, 1, :, cols]
                    picks = data_places_ref[band, :, cols] + (first + block) * list_len
                    mags = data_ref[band, 0, :, cols] - spread(zp[band, pl.ds(my_row, 1), :], picks)
                    left.append(mags)
                    means.append(jnp.sum(wts * mags, axis=0, keepdims=True) / jnp.sum(wts, axis=0, keepdims=True))
                for band in range(bands):
                    wts = data_ref[band, 1, :, cols]
                    partial[band] = partial[band] + wts * (left[band] - mixed(mixing, band, means)) ** 2
        for band in range(bands):
            lines[pl.ds(sweep * bands + band, 1), :] = jnp.sum(partial[band], axis=0, keepdims=True)

    def step(number, carry):
        color_no = lax.rem(number, COLORS)

        def update(group, inner):
            rows = rows_of(group)
            now = color_ref[rows, :] == color_no
            for band, value in enumerate(gathered(group)):
                old = zp[band, rows, :]
                new = jnp.where(now, value * rden[band, rows, :], old)
                zp[band, rows, :] = new
                move[band, rows, :] = new - old
            return inner

        lax.fori_loop(0, groups, update, 0, unroll=2)

        @pl.when(color_no == COLORS - 1)
        def _():
            misfit_lines(lax.div(number, COLORS))

        segment = lane & (LANES - list_len)
        push_window(color_no, lambda origin: segment + origin)

        @pl.when(window_ref[color_no, 1] - window_ref[color_no, 0] > list_len // 2)
        def _():
            def half(part, inner):
                push(list_len // 2, part * (list_len // 2), segment + part * (list_len // 2))
                return inner

            lax.fori_loop(0, 2, half, 0)

        wrap()
        return carry

    def all_steps():
        copy = pltpu.make_async_copy(pick_hbm_ref, pick_ref, pick_sem)
        copy.start()
        copy.wait()
        wrap()
        lax.fori_loop(0, groups, weigh, 0)
        tot[:, 8 : row_count + 8, :] = base[...]
        wrap()
        lax.fori_loop(0, SWEEPS * COLORS, step, 0)

    def compact(color_no):
        picks = (lane // SLOTS) % pack * list_len + lane % SLOTS
        picks = picks + jnp.minimum(window_ref[color_no, 0], list_len - SLOTS)
        for group in range(2):
            for band in range(bands):
                wide[band, group * 8 : group * 8 + 8, :] = take(tot[band, group * 8 + 8 : group * 8 + 16, :], picks)
        sums = []
        for band in range(bands):
            even = wide[band, pl.ds(0, 8, stride=2), :]
            odd = wide[band, pl.ds(1, 8, stride=2), :]
            value = jnp.where(lane < LANES // 2, even, odd)
            twice[band, 0:8, :] = value
            twice[band, 8:16, :] = value
            sums += [value, jnp.zeros((8, LANES), jnp.float32)]

        def add(first, count, sums):
            for index in range(2 * AROUND + 1):
                start = (index - AROUND) % 8
                near = [twice[band, start : start + 8, :] for band in range(bands)]
                for level in range(count):
                    pick = ranked_ref[color_no, first + level, index]
                    mask = pick < LANES
                    lanes = pick & (LANES - 1)
                    for band in range(bands):
                        at = 2 * band + level % 2
                        sums[at] = sums[at] + jnp.where(mask, take(near[band], lanes), 0.0)
            return sums

        sums = add(0, DEPTH - 1, sums)
        sums = lax.fori_loop(DEPTH - 1, window_ref[0, 3], lambda level, sums: add(level, 1, sums), sums)
        return [sums[2 * band] + sums[2 * band + 1] for band in range(bands)]

    def compact_weigh(color_no, carry):
        live = homes_ref[color_no] >= 0
        for band, value in enumerate(compact(color_no)):
            crden[color_no, band] = jnp.where(live, 1.0 / (value + PRIOR_WEIGHT), 0.0)
        return carry

    def compact_step(number, carry):
        color_no = lax.rem(number, COLORS)
        for band, value in enumerate(compact(color_no)):
            new = value * crden[color_no, band]
            change = new - ctot[color_no, band]
            ctot[color_no, band] = new
            wide[band, pl.ds(0, 8, stride=2), :] = change
            wide[band, pl.ds(1, 8, stride=2), :] = change
        below = lax.broadcasted_iota(jnp.int32, (8, LANES), 0)
        origin = jnp.minimum(window_ref[color_no, 0], list_len - SLOTS)
        first_lane = (below & 1) * (LANES // 2) + (lane // list_len) * SLOTS
        own_lane = (first_lane + (lane & (list_len - 1)) - origin) & (LANES - 1)
        for group in range(2):
            now = color_ref[group * 8 : group * 8 + 8, :] == color_no
            for band in range(bands):
                change = wide[band, group * 8 : group * 8 + 8, :]
                move[band, group * 8 : group * 8 + 8, :] = change
                old = zp[band, group * 8 : group * 8 + 8, :]
                zp[band, group * 8 : group * 8 + 8, :] = old + jnp.where(now, take(change, own_lane), 0.0)

        @pl.when(color_no == COLORS - 1)
        def _():
            misfit_lines(lax.div(number, COLORS))

        push_window(color_no, lambda start: first_lane + (start - origin))
        return carry

    if row_count == 16:
        fast = window_ref[0, 3] <= DEPTH
        for color_no in range(COLORS):
            fast = fast & (window_ref[color_no, 1] - window_ref[color_no, 0] <= SLOTS)

        @pl.when(fast)
        def _():
            lax.fori_loop(0, COLORS, compact_weigh, 0)
            ctot[...] = jnp.zeros_like(ctot)
            tot[:, 8 : row_count + 8, :] = base[...]
            lax.fori_loop(0, SWEEPS * COLORS, compact_step, 0)

        pl.when(jnp.logical_not(fast))(all_steps)
    else:
        all_steps()
    sums_ref[...] = contract_lanes(jnp.ones((8, LANES), jnp.float32), lines[...])
    for block in range(blocks):
        row = zp[my_band, pl.ds(my_tile * tile_rows + block // pack, 1), :]
        for half in range(halves):
            cols = pl.ds(block * rows + half * LANES, LANES)
            wts = wts_ref[:, cols]
            picks = places_ref[:, cols] + block % pack * list_len
            left = wts * (mags_ref[:, cols] - spread(row, picks))
            means_ref[0:1, cols] = jnp.sum(left, axis=0, keepdims=True) / jnp.sum(wts, axis=0, keepdims=True)
    below = lax.broadcasted_iota(jnp.int32, (8, LANES), 0)
    close = jnp.zeros((8, LANES), jnp.float32)
    for offset in range(3):
        tile = lax.rem(my_tile + offset + tiles - 1, tiles)
        for row in range(tile_rows):
            value = zp[my_band, pl.ds(tile * tile_rows + row, 1), :]
            close = jnp.where(below == offset * tile_rows + row, jnp.broadcast_to(value, (8, LANES)), close)
    owned = own_zp_ref.shape[1]
    for row in range(chosen_ref.shape[0]):
        pick = chosen_ref[row]
        value = jnp.where(pick < LANES, take(close, pick & (LANES - 1)), 0.0)
        value = jnp.sum(value, axis=0, keepdims=True)
        width = min(LANES, owned - row * LANES)
        own_zp_ref[0:1, row * LANES : row * LANES + width] = value[:, 0:width]


def take(value, picks):
    return jnp.take_along_axis(value, picks, axis=1, mode="promise_in_bounds")


def sort_entries(list_len, fields, listed, color_ref):
    lane = lax.broadcasted_iota(jnp.int32, (8, LANES), 1)
    segment = lane & (LANES - list_len)
    live = listed < fields
    row_no, lane_no = listed // LANES, listed % LANES
    color = jnp.full((8, LANES), -1, jnp.int32)
    for row in range(color_ref.shape[0]):
        table = jnp.broadcast_to(color_ref[row : row + 1, :], (8, LANES))
        color = jnp.where(row_no == row, take(table, lane_no), color)
    color = jnp.where(live, color, -1)
    masks = jnp.concatenate([(color == c).astype(jnp.float32) for c in range(COLORS)], axis=0)
    source = lax.broadcasted_iota(jnp.int32, (LANES, LANES), 0)
    target = lax.broadcasted_iota(jnp.int32, (LANES, LANES), 1)
    same = (source // list_len) == (target // list_len)
    dims = (((1,), (0,)), ((), ()))
    before = (same & (source < target)).astype(jnp.float32)
    ranks = lax.dot_general(masks, before, dims, preferred_element_type=jnp.float32)
    counts = lax.dot_general(masks, same.astype(jnp.float32), dims, preferred_element_type=jnp.float32)
    rest = jnp.zeros((8, LANES), jnp.float32)
    room = [None] * COLORS
    for c in reversed(range(COLORS)):
        rest = rest + counts[c * 8 : c * 8 + 8]
        room[c] = list_len - rest
    end = jnp.zeros((8, LANES), jnp.float32)
    place = jnp.full((8, LANES), -1.0, jnp.float32)
    for c in range(COLORS):
        start = jnp.minimum(jnp.maximum(end, float(list_len * c // COLORS)), room[c])
        end = start + counts[c * 8 : c * 8 + 8]
        place = jnp.where(color == c, start + ranks[c * 8 : c * 8 + 8], place)
    place = place.astype(jnp.int32)
    sorted_fields = jnp.full((8, LANES), fields, jnp.int32)
    sorted_colors = jnp.full((8, LANES), -1, jnp.int32)
    for entry in range(list_len):
        picks = segment + entry
        hit = take(place, picks) == lane - segment
        sorted_fields = jnp.where(hit, take(listed, picks), sorted_fields)
        sorted_colors = jnp.where(hit, take(color, picks), sorted_colors)
    return place, sorted_fields, sorted_colors


def match(list_len, fields, lists_ref, rows_ref, pick_ref, color_ref):
    tiles, _, tile_rows, _ = lists_ref.shape
    pack = LANES // list_len
    levels, places, row_count, _ = pick_ref.shape
    lane = lax.broadcasted_iota(jnp.int32, (8, LANES), 1)
    for tile in range(tiles):
        start = tile * tile_rows
        rows_ref[8 + start : 8 + start + tile_rows, :] = lists_ref[tile, 0]
        color_ref[start : start + tile_rows, :] = lists_ref[tile, 1]
    rows_ref[0:8, :] = rows_ref[row_count : row_count + 8, :]
    rows_ref[row_count + 8 : row_count + 16, :] = rows_ref[8:16, :]

    def group_picks(group, carry):
        home = rows_ref[pl.ds(pl.multiple_of(group * 8 + 8, 8), 8), :]
        home = jnp.where(home < fields, home, -1)
        near = [rows_ref[pl.ds(group * 8 + 8 + place - places // 2, 8), :] for place in range(places)]
        found = [[] for _ in range(places)]
        for quarter in range(pack):
            picks = [jnp.full((8, LANES), LANES, jnp.int32) for _ in range(places)]
            for entry in range(list_len):
                source = quarter * list_len + entry
                for place in range(places):
                    other = jnp.broadcast_to(near[place][:, source : source + 1], (8, LANES))
                    picks[place] = jnp.where(other == home, source, picks[place])
            for place in range(places):
                found[place].append(picks[place])
        rows = pl.ds(pl.multiple_of(group * 8, 8), 8)
        for place in range(places):
            ranked = found[place]
            if place == places // 2:
                ranked = [jnp.where(pick == lane, LANES, pick) for pick in ranked]
            for turn in range(pack):
                for low in range(turn % 2, pack - 1, 2):
                    pair = ranked[low], ranked[low + 1]
                    ranked[low], ranked[low + 1] = jnp.minimum(*pair), jnp.maximum(*pair)
            for level in range(pack):
                pick_ref[level, place, rows, :] = ranked[level]
        return carry

    lax.fori_loop(0, row_count // 8, group_picks, 0)


def windows(list_len, pick_ref, color_ref, window_ref):
    levels, places, row_count, _ = pick_ref.shape
    lane = lax.broadcasted_iota(jnp.int32, (8, LANES), 1)
    position = (lane & (list_len - 1)).astype(jnp.float32)

    def rows_of(group):
        return pl.ds(pl.multiple_of(group * 8, 8), 8)

    def bounds(group, carry):
        lows, highs = carry
        color = color_ref[rows_of(group), :]
        new_lows, new_highs = [], []
        for c in range(COLORS):
            new_lows.append(jnp.minimum(lows[c], jnp.where(color == c, position, float(list_len))))
            new_highs.append(jnp.maximum(highs[c], jnp.where(color == c, position + 1.0, 0.0)))
        return new_lows, new_highs

    start = [jnp.full((8, LANES), float(list_len), jnp.float32)] * COLORS, [jnp.zeros((8, LANES), jnp.float32)] * COLORS
    lows, highs = lax.fori_loop(0, row_count // 8, bounds, start)
    lows = jnp.concatenate([jnp.min(value, axis=0, keepdims=True) for value in lows], axis=0)
    highs = jnp.concatenate([jnp.max(value, axis=0, keepdims=True) for value in highs], axis=0)
    lows = jnp.min(lows, axis=1, keepdims=True)
    highs = jnp.max(highs, axis=1, keepdims=True)
    deepest = jnp.full((8, LANES), 2.0, jnp.float32)
    for level in range(2, levels):
        def least(group, value, level=level):
            for place in range(places):
                value = jnp.minimum(value, pick_ref[level, place, rows_of(group), :])
            return value

        found = lax.fori_loop(0, row_count // 8, least, jnp.full((8, LANES), LANES, jnp.int32))
        deepest = jnp.where(found < LANES, level + 1.0, deepest)
    deepest = jnp.max(jnp.max(deepest, axis=0, keepdims=True), axis=1, keepdims=True)
    table = jnp.where(lane == 0, lows, jnp.where(lane == 1, highs, deepest))
    window_ref[...] = table.astype(jnp.int32)


SLOTS = 16
DEPTH = 3
AROUND = 3


def compact_tables(list_len, colors, rows_ref, color_ref, window_ref, homes_ref, ranked_ref, stage_ref, flags_ref):
    lane = lax.broadcasted_iota(jnp.int32, (8, LANES), 1)
    offsets = range(-AROUND, AROUND + 1)

    def one_color(c, carry):
        low = jnp.broadcast_to(window_ref[pl.ds(c, 1), :][:, 0:1], (8, LANES))
        picks = (lane // SLOTS) % (LANES // list_len) * list_len + lane % SLOTS
        picks = picks + jnp.minimum(low, list_len - SLOTS)
        for group in range(2):
            listed = rows_ref[8 + group * 8 : 16 + group * 8, :]
            color = color_ref[group * 8 : group * 8 + 8, :]
            stage_ref[group * 8 : group * 8 + 8, :] = take(jnp.where(color == c, listed, -1), picks)
        even = stage_ref[pl.ds(0, 8, stride=2), :]
        odd = stage_ref[pl.ds(1, 8, stride=2), :]
        home = jnp.where(lane < LANES // 2, even, odd)
        homes_ref[c] = home
        stage_ref[0:8, :] = home
        stage_ref[8:16, :] = home
        near = [stage_ref[offset % 8 : offset % 8 + 8, :] for offset in offsets]
        target = jnp.where(home >= 0, home, -2)
        ranked = [[jnp.full((8, LANES), LANES, jnp.int32)] * (DEPTH + 1) for _ in offsets]
        for block in range(LANES // SLOTS):
            found = [jnp.full((8, LANES), LANES, jnp.int32) for _ in offsets]
            for source in range(block * SLOTS, (block + 1) * SLOTS):
                for index in range(len(offsets)):
                    other = jnp.broadcast_to(near[index][:, source : source + 1], (8, LANES))
                    found[index] = jnp.where(other == target, source, found[index])
            found[AROUND] = jnp.where(found[AROUND] == lane, LANES, found[AROUND])
            for index in range(len(offsets)):
                rest = found[index]
                for level in range(DEPTH + 1):
                    kept = ranked[index][level]
                    ranked[index][level] = jnp.minimum(kept, rest)
                    rest = jnp.maximum(kept, rest)
        flags = flags_ref[...]
        for index in range(len(offsets)):
            for level in range(DEPTH):
                ranked_ref[c, level, index] = ranked[index][level]
            flags = jnp.where(ranked[index][DEPTH - 1] < LANES, jnp.maximum(flags, float(DEPTH)), flags)
            flags = jnp.where(ranked[index][DEPTH] < LANES, DEPTH + 1.0, flags)
        flags_ref[...] = flags
        return carry

    lax.fori_loop(*colors, one_color, 0)


def note_depth(window_ref, flags_ref):
    lane = lax.broadcasted_iota(jnp.int32, (8, LANES), 1)
    deepest = jnp.max(jnp.max(flags_ref[...], axis=0, keepdims=True), axis=1, keepdims=True)
    window_ref[...] = jnp.where(lane == 3, deepest.astype(jnp.int32), window_ref[...])


def choose(tiles, fields, owner_ref, rows_ref, chosen_ref):
    field_rows = owner_ref.shape[0]
    tile_rows = (rows_ref.shape[0] - 16) // tiles
    my_tile = lax.axis_index("sky")
    lane = lax.broadcasted_iota(jnp.int32, (8, LANES), 1)
    below = lax.broadcasted_iota(jnp.int32, (8, LANES), 0)
    owned = owner_ref[...] == my_tile
    ones = owned.astype(jnp.float32)
    source = lax.broadcasted_iota(jnp.int32, (LANES, LANES), 0)
    target = lax.broadcasted_iota(jnp.int32, (LANES, LANES), 1)
    dims = (((1,), (0,)), ((), ()))
    inside = lax.dot_general(ones, (source < target).astype(jnp.float32), dims, preferred_element_type=jnp.float32)
    counts = lax.dot_general(ones, jnp.ones((LANES, LANES), jnp.float32), dims, preferred_element_type=jnp.float32)
    upper = lax.broadcasted_iota(jnp.int32, (field_rows, field_rows), 1)
    lower = lax.broadcasted_iota(jnp.int32, (field_rows, field_rows), 0)
    above = lax.dot_general((upper < lower).astype(jnp.float32), counts, dims, preferred_element_type=jnp.float32)
    rank = jnp.where(owned, (inside + above).astype(jnp.int32), -1)
    close = jnp.full((8, LANES), fields, jnp.int32)
    for offset in range(3):
        tile = lax.rem(my_tile + offset + tiles - 1, tiles)
        for row in range(tile_rows):
            value = rows_ref[pl.ds(8 + tile * tile_rows + row, 1), :]
            close = jnp.where(below == offset * tile_rows + row, jnp.broadcast_to(value, (8, LANES)), close)
    row_no, lane_no = close // LANES, close % LANES
    order = jnp.full((8, LANES), -1, jnp.int32)
    for row in range(field_rows):
        table = jnp.broadcast_to(rank[row : row + 1, :], (8, LANES))
        order = jnp.where(row_no == row, take(table, lane_no), order)
    own_rows = chosen_ref.shape[0]
    codes = [jnp.full((8, LANES), -1, jnp.int32) for _ in range(own_rows)]
    for entry in range(LANES):
        value = jnp.broadcast_to(order[:, entry : entry + 1], (8, LANES))
        for row in range(own_rows):
            codes[row] = jnp.where(value == row * LANES + lane, entry, codes[row])
    for row in range(own_rows):
        ranked = jnp.where(codes[row] >= 0, (below + 1).astype(jnp.float32), 0.0)
        last = jnp.max(ranked, axis=0, keepdims=True)
        keep = (ranked > 0.0) & (ranked == last)
        chosen_ref[row] = jnp.where(keep, codes[row], LANES)


def relabel(list_len, rows, block, offset, place_ref, slots_ref, out_ref):
    pack = LANES // list_len
    table = jnp.broadcast_to(place_ref[pl.ds(block // pack, 1), :], (slots_ref.shape[0], LANES))
    for half in range(rows // LANES):
        cols = pl.ds(offset + half * LANES, LANES)
        out_ref[:, cols] = take(table, slots_ref[:, cols] + block % pack * list_len)


def gather_kernel(
    tiles, bands, obs, list_len, rows, fields,
    terms_ref, tile_lists_ref, field_colors_ref, mags_ref, wts_ref, slots_ref, owner_ref,
    all_ref, pick_ref, color_ref, window_ref, chosen_ref, data_ref, data_places_ref, places_ref,
    homes_ref, ranked_ref,
    pair_ref, flags_ref, rows_ref, own_ref, listed_ref, place_ref, sorted_ref, lists_ref, data_slots_ref,
    send_sems, recv_sems, early_send_sems, early_recv_sems,
):
    high_count = tiles // 2
    blocks = tile_lists_ref.shape[0]
    pack = LANES // list_len
    tile_rows = blocks // pack
    mine = blocks // bands
    width = mine * rows
    sky, band = lax.axis_index("sky"), lax.axis_index("band")
    high, low = sky // 2, sky % 2
    side, core = band // 2, band % 2
    to_low = {"sky": high * 2 + (1 - low)}
    to_side = {"band": (1 - side) * 2 + core}
    to_core = {"band": side * 2 + (1 - core)}
    barrier = pltpu.get_barrier_semaphore()
    tile_peers = [lax.rem(sky + step, tiles) for step in range(1, tiles)]
    band_peers = [lax.rem(band + step, bands) for step in range(1, bands)]
    for peer in tile_peers:
        pl.semaphore_signal(barrier, inc=1, device_id={"sky": peer}, device_id_type=MESH)
    for peer in band_peers:
        pl.semaphore_signal(barrier, inc=1, device_id={"band": peer}, device_id_type=MESH)

    listed_ref[...] = jnp.full((8, LANES), fields, jnp.int32)
    for row in range(tile_rows):
        pieces = [tile_lists_ref[row * pack + part : row * pack + part + 1, :] for part in range(pack)]
        listed_ref[row : row + 1, :] = jnp.concatenate(pieces, axis=1)
    place, sorted_fields, sorted_colors = sort_entries(list_len, fields, listed_ref[...], field_colors_ref)
    place_ref[...] = place
    sorted_ref[0] = sorted_fields[0:tile_rows]
    sorted_ref[1] = sorted_colors[0:tile_rows]
    lists_ref[sky] = sorted_ref[...]
    pl.semaphore_wait(barrier, tiles + bands - 2)

    def early(number, source, target, device):
        copy = pltpu.make_async_remote_copy(
            src_ref=source,
            dst_ref=target,
            send_sem=early_send_sems.at[number],
            recv_sem=early_recv_sems.at[number],
            device_id=device,
            device_id_type=MESH,
        )
        copy.start()
        return copy

    def columns(peer):
        return pl.ds(pl.multiple_of(peer * width, LANES), width)

    data_copies, list_copies = [], []
    for step, peer in enumerate(band_peers):
        cols = columns(peer)
        for kind, (source, target) in enumerate((
            (slots_ref, data_slots_ref.at[band]),
            (wts_ref, data_ref.at[band, 1]),
            (mags_ref, data_ref.at[band, 0]),
        )):
            data_copies.append(early(3 * step + kind, source.at[:, cols], target, {"band": peer}))
    for step, peer in enumerate(tile_peers):
        list_copies.append(early(3 * (bands - 1) + step, sorted_ref, lists_ref.at[sky], {"sky": peer}))
    data_ref[band, 0] = mags_ref[:, columns(band)]
    data_ref[band, 1] = wts_ref[:, columns(band)]
    data_slots_ref[band] = slots_ref[:, columns(band)]
    for block in range(blocks):
        relabel(list_len, rows, block, block * rows, place_ref, slots_ref, places_ref)
    for copy in data_copies:
        copy.wait_recv()
    for other in range(bands):
        for block in range(mine):
            source, target = data_slots_ref.at[other], data_places_ref.at[other]
            relabel(list_len, rows, band * mine + block, block * rows, place_ref, source, target)

    def tables():
        for copy in list_copies:
            copy.wait_recv()
        match(list_len, fields, lists_ref, rows_ref, pick_ref, color_ref)

    def more_tables():
        windows(list_len, pick_ref, color_ref, window_ref)
        flags_ref[...] = jnp.full((8, LANES), DEPTH - 1.0, jnp.float32)
        choose(tiles, fields, owner_ref, rows_ref, chosen_ref)
        for copy in data_copies + list_copies:
            copy.wait_send()

    def color_tables(start, stop):
        args = rows_ref, color_ref, window_ref, homes_ref, ranked_ref, pair_ref, flags_ref
        compact_tables(list_len, (start, stop), *args)
        if stop == COLORS:
            note_depth(window_ref, flags_ref)

    if high_count > 4:
        highs = [lax.rem(high + step, high_count) for step in range(1, high_count)]
        peers = [{"sky": peer * 2 + low} for peer in highs]
        couple(bands, obs, list_len, rows, terms_ref, data_ref, data_places_ref, own_ref)
        count = [0]

        def send(source, target, peer):
            copy = pltpu.make_async_remote_copy(
                src_ref=source,
                dst_ref=target,
                send_sem=send_sems.at[count[0]],
                recv_sem=recv_sems.at[count[0]],
                device_id=peer,
                device_id_type=MESH,
            )
            count[0] += 1
            copy.start()
            return copy

        def wait(copies):
            for copy in copies:
                copy.wait()

        mine = all_ref.at[high, low, side, core]
        copies = [send(own_ref, mine, peer) for peer in peers]
        all_ref[high, low, side, core] = own_ref[...]
        tables()
        more_tables()
        homes_ref[...] = jnp.zeros_like(homes_ref)
        ranked_ref[...] = jnp.zeros_like(ranked_ref)
        wait(copies)

        column = all_ref.at[:, low, side, core]
        first = all_ref.at[:, low, side, core, 0]
        second = all_ref.at[:, low, side, core, 1]
        copies = [send(first, first, to_low), send(second, second, to_side)]
        late = [send(column, column, to_core)]
        wait(copies)

        first = all_ref.at[:, :, side, core, 0]
        second = all_ref.at[:, low, :, core, 1]
        copies = [send(first, first, to_side), send(second, second, to_low)]
        for part in (all_ref.at[:, 1 - low, side, core, 0], all_ref.at[:, low, 1 - side, core, 1]):
            late.append(send(part, part, to_core))
        wait(copies)

        for part in (all_ref.at[:, :, 1 - side, core, 0], all_ref.at[:, 1 - low, :, core, 1]):
            late.append(send(part, part, to_core))
        wait(late)
        return

    chunks = high_count * 8
    lower, upper = high > 0, high < high_count - 1
    own_chunk = all_ref.at[high, low, side, core]
    couple(bands, obs, list_len, rows, terms_ref, data_ref, data_places_ref, own_chunk)
    def copy_of(kind, z, y, x, part, peer, landing):
        chunk = all_ref.at[z, y, x, core, part]
        number = ((z * 2 + y) * 2 + x) * 2 + part
        return pltpu.make_async_remote_copy(
            src_ref=chunk,
            dst_ref=chunk,
            send_sem=send_sems.at[kind * chunks + number],
            recv_sem=recv_sems.at[landing * chunks + number],
            device_id=peer,
            device_id_type=MESH,
        )

    def along(z, part, step):
        return copy_of((step + 1) // 2, z, low, side, part, {"sky": (high + step) * 2 + low}, 0)

    def across_x(z, y, part):
        return copy_of(2, z, y, side, part, to_side, 0)

    def across_y(z, x, part):
        return copy_of(3, z, low, x, part, to_low, 0)

    def over(z, y, x, part):
        return copy_of(4, z, y, x, part, to_core, 1)

    def arrived(z, y, x, part):
        copy_of(4, z, y, x, part, to_core, 0).wait_recv()

    ends = {-1: lower, 1: upper}

    def along_if(z, part, step):
        @pl.when(ends[step])
        def _():
            along(z, part, step).start()

    def first_hop(z, part):
        if part == 0:
            across_x(z, low, part).start()
        else:
            across_y(z, side, part).start()

    def second_hop(z, part):
        if part == 0:
            across_y(z, side, part).start()
        else:
            across_x(z, low, part).start()

    for part in range(2):
        along_if(high, part, 1)
        along_if(high, part, -1)
        first_hop(high, part)
    for part in range(2):
        second_hop(high, part)
        over(high, low, side, part).start()
    tables()

    def column_arrival(distance, part):
        for step in (-1, 1):
            z = high - step * distance
            here = z >= 0 if step == 1 else z < high_count

            @pl.when(here)
            def _(z=z, step=step):
                arrived(z, low, side, part)
                along_if(z, part, step)
                first_hop(z, part)
                second_hop(z, part)
                over(z, low, side, part).start()

    def at_distance(distance, action):
        if distance == 0:
            action(high)
            return
        for step in (-1, 1):
            z = high - step * distance

            @pl.when(z >= 0 if step == 1 else z < high_count)
            def _(z=z):
                action(z)

    def turn(z):
        arrived(z, low, 1 - side, 0)
        across_y(z, 1 - side, 0).start()
        over(z, low, 1 - side, 0).start()
        arrived(z, 1 - low, side, 1)
        across_x(z, 1 - low, 1).start()
        over(z, 1 - low, side, 1).start()

    def last(z):
        for y, x, part in ((1 - low, side, 0), (low, 1 - side, 1), (1 - low, 1 - side, 0), (1 - low, 1 - side, 1)):
            arrived(z, y, x, part)
            over(z, y, x, part).start()

    for distance in range(1, high_count):
        column_arrival(distance, 0)
        at_distance(distance - 1, turn)
        column_arrival(distance, 1)
        if distance > 1:
            at_distance(distance - 2, last)
        if distance == 1:
            more_tables()
        else:
            color_tables(COLORS * (distance - 2) // (high_count - 1), COLORS * (distance - 1) // (high_count - 1))
    at_distance(high_count - 1, turn)
    color_tables(COLORS * (high_count - 2) // (high_count - 1), COLORS)
    for distance in range(max(high_count - 2, 0), high_count):
        at_distance(distance, last)

    for z in range(high_count):
        for y in range(2):
            for x in range(2):
                for part in range(2):
                    copy_of(4, z, y, x, part, to_core, 1).wait()
    for z in range(high_count):
        for part in range(2):
            for step in (-1, 1):
                passing = (z >= high) if step == -1 else (z <= high)

                @pl.when(ends[step] & passing)
                def _(z=z, part=part, step=step):
                    along(z, part, step).wait_send()

            for other in range(2):
                if part == 0:
                    across_y(z, other, part).wait_send()
                else:
                    across_x(z, other, part).wait_send()
            first = across_x(z, low, part) if part == 0 else across_y(z, side, part)
            first.wait_send()


def total_kernel(tiles, bands, scale, sums_ref, misfit_ref, all_sums, send_sems, recv_sems):
    my_tile, my_band = lax.axis_index("sky"), lax.axis_index("band")
    me = my_tile * bands + my_band
    peers = []
    for sky_step in range(tiles):
        for band_step in range(bands):
            if sky_step or band_step:
                peers.append({"sky": lax.rem(my_tile + sky_step, tiles), "band": lax.rem(my_band + band_step, bands)})
    barrier = pltpu.get_barrier_semaphore()
    for peer in peers:
        pl.semaphore_signal(barrier, inc=1, device_id=peer, device_id_type=MESH)
    all_sums[pl.ds(me, 1), :] = sums_ref[0:1, :]
    pl.semaphore_wait(barrier, len(peers))
    copies = []
    for number, peer in enumerate(peers):
        copy = pltpu.make_async_remote_copy(
            src_ref=sums_ref.at[0:1],
            dst_ref=all_sums.at[pl.ds(me, 1)],
            send_sem=send_sems.at[number],
            recv_sem=recv_sems.at[number],
            device_id=peer,
            device_id_type=MESH,
        )
        copy.start()
        copies.append(copy)
    for copy in copies:
        copy.wait()
    total = jnp.sum(all_sums[...], axis=0, keepdims=True) / scale
    lane = lax.broadcasted_iota(jnp.int32, (8, LANES), 1)
    picks = (lane * bands + my_band) & (LANES - 1)
    misfit_ref[...] = take(jnp.broadcast_to(total, (8, LANES)), picks)[0:1, 0:SWEEPS]


def body(magnitudes, weights, slots, block_fields, owner, colors, color_terms):
    bands = color_terms.shape[0]
    tiles = lax.axis_size("sky")
    _, obs, stars = magnitudes.shape
    blocks, list_len = block_fields.shape
    rows = stars // blocks
    fields = owner.shape[0]
    owned = fields // tiles
    mine = blocks // bands
    pack = LANES // list_len
    tile_rows = blocks // pack
    row_count = tiles * tile_rows
    vmem = pl.BlockSpec(memory_space=pltpu.VMEM)
    smem = pl.BlockSpec(memory_space=pltpu.SMEM)
    hbm = pl.BlockSpec(memory_space=pl.ANY)
    magnitudes, weights, slots = magnitudes[0], weights[0], slots[0]

    earlier = 3 * (bands - 1) + tiles - 1
    reach = 2 * (REACH * tile_rows + tile_rows - 1) + 1
    own_rows = -(-owned // LANES)
    part = (bands // 2, LANES + EXTRA, LANES)
    everyone = (tiles // 2, 2, bands // 2, 2) + part
    listed = (tiles, 2, tile_rows, LANES)
    if tiles > 8:
        sends = landings = tiles // 2 - 1 + 9
    else:
        sends, landings = 5 * tiles * 4, 2 * tiles * 4
    coupled, pick, entry_colors, window, chosen, data, data_places, places, homes, ranked = pl.pallas_call(
        functools.partial(gather_kernel, tiles, bands, obs, list_len, rows, fields),
        out_shape=(
            jax.ShapeDtypeStruct(everyone, jnp.float32),
            jax.ShapeDtypeStruct((pack, reach, row_count, LANES), jnp.int32),
            jax.ShapeDtypeStruct((row_count, LANES), jnp.int32),
            jax.ShapeDtypeStruct((8, LANES), jnp.int32),
            jax.ShapeDtypeStruct((own_rows, 8, LANES), jnp.int32),
            jax.ShapeDtypeStruct((bands, 2, obs, mine * rows), jnp.float32),
            jax.ShapeDtypeStruct((bands, obs, mine * rows), jnp.int32),
            jax.ShapeDtypeStruct((obs, stars), jnp.int32),
            jax.ShapeDtypeStruct((COLORS, 8, LANES), jnp.int32),
            jax.ShapeDtypeStruct((COLORS, DEPTH, 2 * AROUND + 1, 8, LANES), jnp.int32),
        ),
        in_specs=[smem] + [vmem] * 6,
        out_specs=(vmem,) * 10,
        scratch_shapes=[
            pltpu.VMEM((16, LANES), jnp.int32),
            pltpu.VMEM((8, LANES), jnp.float32),
            pltpu.VMEM((row_count + 16, LANES), jnp.int32),
            pltpu.VMEM(part, jnp.float32),
            pltpu.VMEM((8, LANES), jnp.int32),
            pltpu.VMEM((8, LANES), jnp.int32),
            pltpu.VMEM(listed[1:], jnp.int32),
            pltpu.VMEM(listed, jnp.int32),
            pltpu.VMEM((bands, obs, mine * rows), jnp.int32),
            pltpu.SemaphoreType.DMA((sends,)),
            pltpu.SemaphoreType.DMA((landings,)),
            pltpu.SemaphoreType.DMA((earlier,)),
            pltpu.SemaphoreType.DMA((earlier,)),
        ],
        compiler_params=pltpu.CompilerParams(
            collective_id=0, has_side_effects=True, vmem_limit_bytes=60 * 1024 * 1024
        ),
        name="gather",
    )(color_terms, block_fields, colors.reshape(-1, LANES), magnitudes, weights, slots, owner.reshape(-1, LANES))
    coupled = coupled.reshape((-1,) + coupled.shape[-2:])

    big = (bands, row_count, LANES)
    depth = min(row_count, 16)
    own_zp, star_means, sums = pl.pallas_call(
        functools.partial(sweep_kernel, tiles, bands, obs, list_len, rows, row_count),
        out_shape=(
            jax.ShapeDtypeStruct((1, owned), jnp.float32),
            jax.ShapeDtypeStruct((1, stars), jnp.float32),
            jax.ShapeDtypeStruct((8, LANES), jnp.float32),
        ),
        in_specs=[smem, smem, hbm, hbm] + [vmem] * 9,
        out_specs=(vmem,) * 3,
        scratch_shapes=[
            pltpu.VMEM((row_count * bands * LANES, LANES), jnp.float32),
            pltpu.VMEM(big, jnp.float32),
            pltpu.VMEM((bands, row_count + 16, LANES), jnp.float32),
            pltpu.VMEM(big, jnp.float32),
            pltpu.VMEM(big, jnp.float32),
            pltpu.VMEM(big, jnp.float32),
            pltpu.VMEM((LANES, LANES), jnp.float32),
            pltpu.VMEM(pick.shape, jnp.int32),
            pltpu.SemaphoreType.DMA,
            pltpu.VMEM((bands, 16, LANES), jnp.float32),
            pltpu.VMEM((bands, 16, LANES), jnp.float32),
            pltpu.VMEM((COLORS, bands, 8, LANES), jnp.float32),
            pltpu.VMEM((COLORS, bands, 8, LANES), jnp.float32),
            pltpu.VMEM((depth, bands, LANES + EXTRA, LANES), jnp.float32),
            pltpu.SemaphoreType.DMA((depth,)),
        ],
        compiler_params=pltpu.CompilerParams(vmem_limit_bytes=60 * 1024 * 1024),
        name="sweeps",
    )(window, color_terms, coupled, pick, entry_colors, data, data_places, magnitudes, weights, places, chosen, homes, ranked)

    devices = tiles * bands
    misfit = pl.pallas_call(
        functools.partial(total_kernel, tiles, bands, float(obs * stars * tiles)),
        out_shape=jax.ShapeDtypeStruct((1, SWEEPS), jnp.float32),
        in_specs=[vmem],
        out_specs=vmem,
        scratch_shapes=[
            pltpu.VMEM((devices, LANES), jnp.float32),
            pltpu.SemaphoreType.DMA((devices - 1,)),
            pltpu.SemaphoreType.DMA((devices - 1,)),
        ],
        compiler_params=pltpu.CompilerParams(collective_id=1, has_side_effects=True),
        name="total",
    )(sums)
    return own_zp, star_means, misfit.reshape(SWEEPS, 1)


def solution(mesh):
    in_specs = (
        P("band", None, "sky"),
        P("band", None, "sky"),
        P("band", None, "sky"),
        P("sky", None),
        P(),
        P(),
        P(),
    )
    out_specs = (P("band", "sky"), P("band", "sky"), P(None, "band"))
    return jax.shard_map(body, mesh=mesh, in_specs=in_specs, out_specs=out_specs, check_vma=False)
```

```python
import functools

import jax
import jax.numpy as jnp
from jax import lax
from jax.experimental import pallas as pl
from jax.experimental.pallas import tpu as pltpu
from jax.sharding import PartitionSpec as P

COLORS = 8
SWEEPS = 4
PRIOR_WEIGHT = 1.0
REACH = 2
HIGHEST = lax.Precision.HIGHEST
LANES = 128
EXTRA = 8
MESH = pl.DeviceIdType.MESH


def contract_lanes(left, right):
    dims = (((1,), (1,)), ((), ()))
    return lax.dot_general(left, right, dims, precision=HIGHEST, preferred_element_type=jnp.float32)


def mixing_of(terms_ref, bands):
    mixing = []
    for band in range(bands):
        total = terms_ref[band, 0]
        for other in range(1, bands):
            total = total + terms_ref[band, other]
        row = [terms_ref[band, other] for other in range(bands)]
        row[band] = (1.0 + row[band]) - total
        mixing.append(row)
    return mixing


def mixed(mixing, band, means):
    predicted = mixing[band][0] * means[0]
    for other in range(1, len(means)):
        predicted = predicted + mixing[band][other] * means[other]
    return predicted


def couple(bands, obs, list_len, rows, terms_ref, data_ref, places_ref, out_ref):
    blocks = data_ref.shape[3] // rows
    mixing = mixing_of(terms_ref, bands)
    row_band = lax.broadcasted_iota(jnp.int32, (LANES, LANES), 0) // list_len
    lane_band = lax.broadcasted_iota(jnp.int32, (LANES, LANES), 1) // list_len
    mix_grid = jnp.zeros((LANES, LANES), jnp.float32)
    for band in range(bands):
        for other in range(bands):
            here = (row_band == other) & (lane_band == band)
            mix_grid = jnp.where(here, mixing[band][other], mix_grid)
    full = []
    entry = lax.broadcasted_iota(jnp.int32, (list_len, rows), 0)
    for block in range(blocks):
        cols = pl.ds(block * rows, rows)
        one_hot, one_hot_mag, star_weight, means = [], [], [], []
        for band in range(bands):
            mags = data_ref[band, 0, :, cols]
            wts = data_ref[band, 1, :, cols]
            slots = places_ref[band, :, cols]
            scaled = wts * mags
            weight_sum = jnp.sum(wts, axis=0, keepdims=True)
            star_weight.append(weight_sum)
            means.append(jnp.sum(scaled, axis=0, keepdims=True) / weight_sum)
            hot = jnp.zeros((list_len, rows), jnp.float32)
            hot_mag = jnp.zeros((list_len, rows), jnp.float32)
            for k in range(obs):
                hit = slots[k : k + 1] == entry
                hot = hot + jnp.where(hit, wts[k : k + 1], 0.0)
                hot_mag = hot_mag + jnp.where(hit, scaled[k : k + 1], 0.0)
            one_hot.append(hot)
            one_hot_mag.append(hot_mag)
        rest = []
        shares = []
        for band in range(bands):
            rest.append(one_hot_mag[band] - one_hot[band] * mixed(mixing, band, means))
            shares.append(one_hot[band] / star_weight[band])
        hot_all = jnp.concatenate(one_hot, axis=0)
        share_all = jnp.concatenate(shares, axis=0)
        rest_all = jnp.concatenate(rest, axis=0)
        coupling = contract_lanes(share_all, hot_all) * mix_grid
        ones = jnp.ones((8, rows), jnp.float32)
        rest_row = contract_lanes(ones, rest_all)
        weight_row = contract_lanes(ones, hot_all)
        first = lax.broadcasted_iota(jnp.int32, (EXTRA, LANES), 0) == 0
        full.append(jnp.concatenate([coupling, jnp.where(first, rest_row, weight_row)], axis=0))
    split = bands // 2
    for part in range(split):
        pieces = []
        for half in range(2):
            band = half * split + part
            for block in range(blocks):
                pieces.append(full[block][:, band * list_len : (band + 1) * list_len])
        out_ref[part] = jnp.concatenate(pieces, axis=1)


def sweep_kernel(
    tiles, bands, obs, list_len, rows, row_count,
    window_ref, terms_ref, coupled_ref, pick_ref, color_ref,
    data_ref, data_places_ref, mags_ref, wts_ref, places_ref, chosen_ref,
    own_zp_ref, means_ref, sums_ref,
    kt, base, tot, rden, zp, move, lines, stage, sems,
):
    groups = row_count // 8
    pack = LANES // list_len
    split = bands // 2
    levels, places = pick_ref.shape[:2]
    depth = stage.shape[0]
    lane = lax.broadcasted_iota(jnp.int32, (8, LANES), 1)
    lane_wide = lax.broadcasted_iota(jnp.int32, (LANES + EXTRA, LANES), 1)

    def fetch(row, slot):
        return pltpu.make_async_copy(
            coupled_ref.at[pl.ds(row * (2 * split), 2 * split)], stage.at[slot], sems.at[slot]
        )

    for row in range(depth - 1):
        fetch(row, row).start()

    def unpack(row, carry):
        slot = lax.rem(row, depth)
        ahead = row + depth - 1

        @pl.when(ahead < row_count)
        def _():
            fetch(ahead, lax.rem(ahead, depth)).start()

        fetch(row, slot).wait()
        group = lax.div(row, 8)
        place = lax.rem(row, 8)
        for part in range(split):
            left = stage[slot, part]
            right = stage[slot, split + part]
            low = jnp.where(lane_wide < LANES // 2, left, pltpu.roll(right, LANES // 2, 1))
            high = jnp.where(lane_wide < LANES // 2, pltpu.roll(left, LANES // 2, 1), right)
            for band, value in ((part, low), (split + part, high)):
                start = (group * bands + band) * (LANES * 8) + place
                kt[pl.ds(start, LANES, stride=8), :] = value[0:LANES]
                base[band, pl.ds(row, 1), :] = value[LANES : LANES + 1]
                tot[band, pl.ds(row + 8, 1), :] = value[LANES + 1 : LANES + 2]
        return carry

    lax.fori_loop(0, row_count, unpack, 0)

    def rows_of(group):
        return pl.ds(pl.multiple_of(group * 8, 8), 8)

    def wrap():
        for band in range(bands):
            tot[band, 0:8, :] = tot[band, row_count : row_count + 8, :]
            tot[band, row_count + 8 : row_count + 16, :] = tot[band, 8:16, :]

    def gather(group, first, count, sums):
        for place in range(places):
            start = group * 8 + (8 + place - places // 2)
            near = [tot[band, pl.ds(start, 8), :] for band in range(bands)]
            for level in range(count):
                pick = pick_ref[first + level, place, rows_of(group), :]
                mask = pick < LANES
                lanes = pick & (LANES - 1)
                for band in range(bands):
                    index = 2 * band + level % 2
                    sums[index] = sums[index] + jnp.where(mask, take(near[band], lanes), 0.0)
        return sums

    def gathered(group):
        sums = []
        for band in range(bands):
            sums += [tot[band, pl.ds(pl.multiple_of(group * 8 + 8, 8), 8), :], jnp.zeros((8, LANES), jnp.float32)]
        sums = gather(group, 0, 2, sums)
        sums = lax.fori_loop(2, window_ref[0, 2], lambda level, sums: gather(group, level, 1, sums), sums)
        return [sums[2 * band] + sums[2 * band + 1] for band in range(bands)]

    def weigh(group, carry):
        for band, value in enumerate(gathered(group)):
            rden[band, rows_of(group), :] = 1.0 / (value + PRIOR_WEIGHT)
        return carry

    wrap()
    lax.fori_loop(0, groups, weigh, 0)
    zp[...] = jnp.zeros_like(zp)
    tot[:, 8 : row_count + 8, :] = base[...]
    wrap()

    def push(width, origin):
        def add(group, inner):
            here = [move[band, rows_of(group), :] for band in range(bands)]
            middle = pl.ds(pl.multiple_of(group * 8 + 8, 8), 8)
            sums = [tot[band, middle, :] for band in range(bands)]
            for entry in range(width):
                lanes = (lane & (LANES - list_len)) + (origin + entry)
                values = [take(here[band], lanes) for band in range(bands)]
                for band in range(bands):
                    for other in range(bands):
                        start = (group * bands + band) * (LANES * 8) + (other * list_len + origin + entry) * 8
                        rows = pl.ds(pl.multiple_of(start, 8), 8)
                        sums[band] = sums[band] + values[other] * kt[rows, :]
            for band in range(bands):
                tot[band, middle, :] = sums[band]
            return inner

        lax.fori_loop(0, groups, add, 0, unroll=2)

    halves = rows // LANES
    stars = mags_ref.shape[1]
    blocks = stars // rows
    tile_rows = blocks // pack
    mine = data_ref.shape[3] // rows
    my_tile, my_band = lax.axis_index("sky"), lax.axis_index("band")
    first = lax.rem(my_band * mine, pack)
    my_row = my_tile * tile_rows + lax.div(my_band * mine, pack)
    mixing = mixing_of(terms_ref, bands)
    lines[...] = jnp.zeros_like(lines)

    def spread(row, picks):
        return take(jnp.broadcast_to(row, (obs, LANES)), picks)

    def misfit_lines(sweep):
        partial = [jnp.zeros((obs, LANES), jnp.float32) for _ in range(bands)]
        for block in range(mine):
            for half in range(halves):
                cols = pl.ds(block * rows + half * LANES, LANES)
                left, means = [], []
                for band in range(bands):
                    wts = data_ref[band, 1, :, cols]
                    picks = data_places_ref[band, :, cols] + (first + block) * list_len
                    mags = data_ref[band, 0, :, cols] - spread(zp[band, pl.ds(my_row, 1), :], picks)
                    left.append(mags)
                    means.append(jnp.sum(wts * mags, axis=0, keepdims=True) / jnp.sum(wts, axis=0, keepdims=True))
                for band in range(bands):
                    wts = data_ref[band, 1, :, cols]
                    partial[band] = partial[band] + wts * (left[band] - mixed(mixing, band, means)) ** 2
        for band in range(bands):
            lines[pl.ds(sweep * bands + band, 1), :] = jnp.sum(partial[band], axis=0, keepdims=True)

    def step(number, carry):
        color_no = lax.rem(number, COLORS)

        def update(group, inner):
            rows = rows_of(group)
            now = color_ref[rows, :] == color_no
            for band, value in enumerate(gathered(group)):
                old = zp[band, rows, :]
                new = jnp.where(now, value * rden[band, rows, :], old)
                zp[band, rows, :] = new
                move[band, rows, :] = new - old
            return inner

        lax.fori_loop(0, groups, update, 0, unroll=2)

        @pl.when(color_no == COLORS - 1)
        def _():
            misfit_lines(lax.div(number, COLORS))

        low, high = window_ref[color_no, 0], window_ref[color_no, 1]
        widths = (list_len // 4, list_len * 3 // 8, list_len // 2)
        for index, width in enumerate(widths):
            fits = high - low <= width
            if index:
                fits = fits & (high - low > widths[index - 1])

            @pl.when(fits)
            def _(width=width):
                push(width, jnp.minimum(low, list_len - width))

        @pl.when(high - low > widths[-1])
        def _():
            lax.fori_loop(0, 2, lambda part, inner: (push(widths[-1], part * widths[-1]), inner)[1], 0)

        wrap()
        return carry

    lax.fori_loop(0, SWEEPS * COLORS, step, 0)
    sums_ref[...] = contract_lanes(jnp.ones((8, LANES), jnp.float32), lines[...])
    for block in range(blocks):
        row = zp[my_band, pl.ds(my_tile * tile_rows + block // pack, 1), :]
        for half in range(halves):
            cols = pl.ds(block * rows + half * LANES, LANES)
            wts = wts_ref[:, cols]
            picks = places_ref[:, cols] + block % pack * list_len
            left = wts * (mags_ref[:, cols] - spread(row, picks))
            means_ref[0:1, cols] = jnp.sum(left, axis=0, keepdims=True) / jnp.sum(wts, axis=0, keepdims=True)
    below = lax.broadcasted_iota(jnp.int32, (8, LANES), 0)
    close = jnp.zeros((8, LANES), jnp.float32)
    for offset in range(3):
        tile = lax.rem(my_tile + offset + tiles - 1, tiles)
        for row in range(tile_rows):
            value = zp[my_band, pl.ds(tile * tile_rows + row, 1), :]
            close = jnp.where(below == offset * tile_rows + row, jnp.broadcast_to(value, (8, LANES)), close)
    owned = own_zp_ref.shape[1]
    for row in range(chosen_ref.shape[0]):
        pick = chosen_ref[row]
        value = jnp.where(pick < LANES, take(close, pick & (LANES - 1)), 0.0)
        value = jnp.sum(value, axis=0, keepdims=True)
        width = min(LANES, owned - row * LANES)
        own_zp_ref[0:1, row * LANES : row * LANES + width] = value[:, 0:width]


def take(value, picks):
    return jnp.take_along_axis(value, picks, axis=1, mode="promise_in_bounds")


def sort_entries(list_len, fields, listed, color_ref):
    lane = lax.broadcasted_iota(jnp.int32, (8, LANES), 1)
    segment = lane & (LANES - list_len)
    live = listed < fields
    row_no, lane_no = listed // LANES, listed % LANES
    color = jnp.full((8, LANES), -1, jnp.int32)
    for row in range(color_ref.shape[0]):
        table = jnp.broadcast_to(color_ref[row : row + 1, :], (8, LANES))
        color = jnp.where(row_no == row, take(table, lane_no), color)
    color = jnp.where(live, color, -1)
    masks = jnp.concatenate([(color == c).astype(jnp.float32) for c in range(COLORS)], axis=0)
    source = lax.broadcasted_iota(jnp.int32, (LANES, LANES), 0)
    target = lax.broadcasted_iota(jnp.int32, (LANES, LANES), 1)
    same = (source // list_len) == (target // list_len)
    dims = (((1,), (0,)), ((), ()))
    before = (same & (source < target)).astype(jnp.float32)
    ranks = lax.dot_general(masks, before, dims, preferred_element_type=jnp.float32)
    counts = lax.dot_general(masks, same.astype(jnp.float32), dims, preferred_element_type=jnp.float32)
    rest = jnp.zeros((8, LANES), jnp.float32)
    room = [None] * COLORS
    for c in reversed(range(COLORS)):
        rest = rest + counts[c * 8 : c * 8 + 8]
        room[c] = list_len - rest
    end = jnp.zeros((8, LANES), jnp.float32)
    place = jnp.full((8, LANES), -1.0, jnp.float32)
    for c in range(COLORS):
        start = jnp.minimum(jnp.maximum(end, float(list_len * c // COLORS)), room[c])
        end = start + counts[c * 8 : c * 8 + 8]
        place = jnp.where(color == c, start + ranks[c * 8 : c * 8 + 8], place)
    place = place.astype(jnp.int32)
    sorted_fields = jnp.full((8, LANES), fields, jnp.int32)
    sorted_colors = jnp.full((8, LANES), -1, jnp.int32)
    for entry in range(list_len):
        picks = segment + entry
        hit = take(place, picks) == lane - segment
        sorted_fields = jnp.where(hit, take(listed, picks), sorted_fields)
        sorted_colors = jnp.where(hit, take(color, picks), sorted_colors)
    return place, sorted_fields, sorted_colors


def match(list_len, fields, lists_ref, rows_ref, pick_ref, color_ref):
    tiles, _, tile_rows, _ = lists_ref.shape
    pack = LANES // list_len
    levels, places, row_count, _ = pick_ref.shape
    lane = lax.broadcasted_iota(jnp.int32, (8, LANES), 1)
    for tile in range(tiles):
        start = tile * tile_rows
        rows_ref[8 + start : 8 + start + tile_rows, :] = lists_ref[tile, 0]
        color_ref[start : start + tile_rows, :] = lists_ref[tile, 1]
    rows_ref[0:8, :] = rows_ref[row_count : row_count + 8, :]
    rows_ref[row_count + 8 : row_count + 16, :] = rows_ref[8:16, :]

    def group_picks(group, carry):
        home = rows_ref[pl.ds(pl.multiple_of(group * 8 + 8, 8), 8), :]
        home = jnp.where(home < fields, home, -1)
        near = [rows_ref[pl.ds(group * 8 + 8 + place - places // 2, 8), :] for place in range(places)]
        found = [[] for _ in range(places)]
        for quarter in range(pack):
            picks = [jnp.full((8, LANES), LANES, jnp.int32) for _ in range(places)]
            for entry in range(list_len):
                source = quarter * list_len + entry
                for place in range(places):
                    other = jnp.broadcast_to(near[place][:, source : source + 1], (8, LANES))
                    picks[place] = jnp.where(other == home, source, picks[place])
            for place in range(places):
                found[place].append(picks[place])
        rows = pl.ds(pl.multiple_of(group * 8, 8), 8)
        for place in range(places):
            ranked = found[place]
            if place == places // 2:
                ranked = [jnp.where(pick == lane, LANES, pick) for pick in ranked]
            for turn in range(pack):
                for low in range(turn % 2, pack - 1, 2):
                    pair = ranked[low], ranked[low + 1]
                    ranked[low], ranked[low + 1] = jnp.minimum(*pair), jnp.maximum(*pair)
            for level in range(pack):
                pick_ref[level, place, rows, :] = ranked[level]
        return carry

    lax.fori_loop(0, row_count // 8, group_picks, 0)


def windows(list_len, pick_ref, color_ref, window_ref):
    levels, places, row_count, _ = pick_ref.shape
    lane = lax.broadcasted_iota(jnp.int32, (8, LANES), 1)
    position = (lane & (list_len - 1)).astype(jnp.float32)

    def rows_of(group):
        return pl.ds(pl.multiple_of(group * 8, 8), 8)

    def bounds(group, carry):
        lows, highs = carry
        color = color_ref[rows_of(group), :]
        new_lows, new_highs = [], []
        for c in range(COLORS):
            new_lows.append(jnp.minimum(lows[c], jnp.where(color == c, position, float(list_len))))
            new_highs.append(jnp.maximum(highs[c], jnp.where(color == c, position + 1.0, 0.0)))
        return new_lows, new_highs

    start = [jnp.full((8, LANES), float(list_len), jnp.float32)] * COLORS, [jnp.zeros((8, LANES), jnp.float32)] * COLORS
    lows, highs = lax.fori_loop(0, row_count // 8, bounds, start)
    lows = jnp.concatenate([jnp.min(value, axis=0, keepdims=True) for value in lows], axis=0)
    highs = jnp.concatenate([jnp.max(value, axis=0, keepdims=True) for value in highs], axis=0)
    lows = jnp.min(lows, axis=1, keepdims=True)
    highs = jnp.max(highs, axis=1, keepdims=True)
    deepest = jnp.full((8, LANES), 2.0, jnp.float32)
    for level in range(2, levels):
        def least(group, value, level=level):
            for place in range(places):
                value = jnp.minimum(value, pick_ref[level, place, rows_of(group), :])
            return value

        found = lax.fori_loop(0, row_count // 8, least, jnp.full((8, LANES), LANES, jnp.int32))
        deepest = jnp.where(found < LANES, level + 1.0, deepest)
    deepest = jnp.max(jnp.max(deepest, axis=0, keepdims=True), axis=1, keepdims=True)
    table = jnp.where(lane == 0, lows, jnp.where(lane == 1, highs, deepest))
    window_ref[...] = table.astype(jnp.int32)


def choose(tiles, fields, owner_ref, rows_ref, chosen_ref):
    field_rows = owner_ref.shape[0]
    tile_rows = (rows_ref.shape[0] - 16) // tiles
    my_tile = lax.axis_index("sky")
    lane = lax.broadcasted_iota(jnp.int32, (8, LANES), 1)
    below = lax.broadcasted_iota(jnp.int32, (8, LANES), 0)
    owned = owner_ref[...] == my_tile
    ones = owned.astype(jnp.float32)
    source = lax.broadcasted_iota(jnp.int32, (LANES, LANES), 0)
    target = lax.broadcasted_iota(jnp.int32, (LANES, LANES), 1)
    dims = (((1,), (0,)), ((), ()))
    inside = lax.dot_general(ones, (source < target).astype(jnp.float32), dims, preferred_element_type=jnp.float32)
    counts = lax.dot_general(ones, jnp.ones((LANES, LANES), jnp.float32), dims, preferred_element_type=jnp.float32)
    upper = lax.broadcasted_iota(jnp.int32, (field_rows, field_rows), 1)
    lower = lax.broadcasted_iota(jnp.int32, (field_rows, field_rows), 0)
    above = lax.dot_general((upper < lower).astype(jnp.float32), counts, dims, preferred_element_type=jnp.float32)
    rank = jnp.where(owned, (inside + above).astype(jnp.int32), -1)
    close = jnp.full((8, LANES), fields, jnp.int32)
    for offset in range(3):
        tile = lax.rem(my_tile + offset + tiles - 1, tiles)
        for row in range(tile_rows):
            value = rows_ref[pl.ds(8 + tile * tile_rows + row, 1), :]
            close = jnp.where(below == offset * tile_rows + row, jnp.broadcast_to(value, (8, LANES)), close)
    row_no, lane_no = close // LANES, close % LANES
    order = jnp.full((8, LANES), -1, jnp.int32)
    for row in range(field_rows):
        table = jnp.broadcast_to(rank[row : row + 1, :], (8, LANES))
        order = jnp.where(row_no == row, take(table, lane_no), order)
    own_rows = chosen_ref.shape[0]
    codes = [jnp.full((8, LANES), -1, jnp.int32) for _ in range(own_rows)]
    for entry in range(LANES):
        value = jnp.broadcast_to(order[:, entry : entry + 1], (8, LANES))
        for row in range(own_rows):
            codes[row] = jnp.where(value == row * LANES + lane, entry, codes[row])
    for row in range(own_rows):
        ranked = jnp.where(codes[row] >= 0, (below + 1).astype(jnp.float32), 0.0)
        last = jnp.max(ranked, axis=0, keepdims=True)
        keep = (ranked > 0.0) & (ranked == last)
        chosen_ref[row] = jnp.where(keep, codes[row], LANES)


def relabel(list_len, rows, block, offset, place_ref, slots_ref, out_ref):
    pack = LANES // list_len
    table = jnp.broadcast_to(place_ref[pl.ds(block // pack, 1), :], (slots_ref.shape[0], LANES))
    for half in range(rows // LANES):
        cols = pl.ds(offset + half * LANES, LANES)
        out_ref[:, cols] = take(table, slots_ref[:, cols] + block % pack * list_len)


def gather_kernel(
    tiles, bands, obs, list_len, rows, fields,
    terms_ref, tile_lists_ref, field_colors_ref, mags_ref, wts_ref, slots_ref, owner_ref,
    out_ref, pick_ref, color_ref, window_ref, chosen_ref, data_ref, data_places_ref, places_ref,
    all_ref, rows_ref, own_ref, listed_ref, place_ref, sorted_ref, lists_ref, data_slots_ref,
    send_sems, recv_sems, early_send_sems, early_recv_sems, plane_send_sems, plane_recv_sems, save_sems,
):
    high_count = tiles // 2
    blocks = tile_lists_ref.shape[0]
    pack = LANES // list_len
    tile_rows = blocks // pack
    mine = blocks // bands
    width = mine * rows
    sky, band = lax.axis_index("sky"), lax.axis_index("band")
    high, low = sky // 2, sky % 2
    side, core = band // 2, band % 2
    to_low = {"sky": high * 2 + (1 - low)}
    to_side = {"band": (1 - side) * 2 + core}
    to_core = {"band": side * 2 + (1 - core)}
    barrier = pltpu.get_barrier_semaphore()
    tile_peers = [lax.rem(sky + step, tiles) for step in range(1, tiles)]
    band_peers = [lax.rem(band + step, bands) for step in range(1, bands)]
    for peer in tile_peers:
        pl.semaphore_signal(barrier, inc=1, device_id={"sky": peer}, device_id_type=MESH)
    for peer in band_peers:
        pl.semaphore_signal(barrier, inc=1, device_id={"band": peer}, device_id_type=MESH)

    listed_ref[...] = jnp.full((8, LANES), fields, jnp.int32)
    for row in range(tile_rows):
        pieces = [tile_lists_ref[row * pack + part : row * pack + part + 1, :] for part in range(pack)]
        listed_ref[row : row + 1, :] = jnp.concatenate(pieces, axis=1)
    place, sorted_fields, sorted_colors = sort_entries(list_len, fields, listed_ref[...], field_colors_ref)
    place_ref[...] = place
    sorted_ref[0] = sorted_fields[0:tile_rows]
    sorted_ref[1] = sorted_colors[0:tile_rows]
    lists_ref[sky] = sorted_ref[...]
    pl.semaphore_wait(barrier, tiles + bands - 2)

    def early(number, source, target, device):
        copy = pltpu.make_async_remote_copy(
            src_ref=source,
            dst_ref=target,
            send_sem=early_send_sems.at[number],
            recv_sem=early_recv_sems.at[number],
            device_id=device,
            device_id_type=MESH,
        )
        copy.start()
        return copy

    def columns(peer):
        return pl.ds(pl.multiple_of(peer * width, LANES), width)

    data_copies, list_copies = [], []
    for step, peer in enumerate(band_peers):
        cols = columns(peer)
        for kind, (source, target) in enumerate((
            (slots_ref, data_slots_ref.at[band]),
            (wts_ref, data_ref.at[band, 1]),
            (mags_ref, data_ref.at[band, 0]),
        )):
            data_copies.append(early(3 * step + kind, source.at[:, cols], target, {"band": peer}))
    for step, peer in enumerate(tile_peers):
        list_copies.append(early(3 * (bands - 1) + step, sorted_ref, lists_ref.at[sky], {"sky": peer}))
    data_ref[band, 0] = mags_ref[:, columns(band)]
    data_ref[band, 1] = wts_ref[:, columns(band)]
    data_slots_ref[band] = slots_ref[:, columns(band)]
    for block in range(blocks):
        relabel(list_len, rows, block, block * rows, place_ref, slots_ref, places_ref)
    for copy in data_copies:
        copy.wait_recv()
    for other in range(bands):
        for block in range(mine):
            source, target = data_slots_ref.at[other], data_places_ref.at[other]
            relabel(list_len, rows, band * mine + block, block * rows, place_ref, source, target)

    def tables():
        for copy in list_copies:
            copy.wait_recv()
        match(list_len, fields, lists_ref, rows_ref, pick_ref, color_ref)

    def more_tables():
        windows(list_len, pick_ref, color_ref, window_ref)
        choose(tiles, fields, owner_ref, rows_ref, chosen_ref)
        for copy in data_copies + list_copies:
            copy.wait_send()

    if high_count > 4:
        highs = [lax.rem(high + step, high_count) for step in range(1, high_count)]
        peers = [{"sky": peer * 2 + low} for peer in highs]
        couple(bands, obs, list_len, rows, terms_ref, data_ref, data_places_ref, own_ref)
        count = [0]

        def send(source, target, peer):
            copy = pltpu.make_async_remote_copy(
                src_ref=source,
                dst_ref=target,
                send_sem=send_sems.at[count[0]],
                recv_sem=recv_sems.at[count[0]],
                device_id=peer,
                device_id_type=MESH,
            )
            count[0] += 1
            copy.start()
            return copy

        def wait(copies):
            for copy in copies:
                copy.wait()

        mine = all_ref.at[high, low, side, core]
        copies = [send(own_ref, mine, peer) for peer in peers]
        all_ref[high, low, side, core] = own_ref[...]
        tables()
        more_tables()
        wait(copies)

        column = all_ref.at[:, low, side, core]
        first = all_ref.at[:, low, side, core, 0]
        second = all_ref.at[:, low, side, core, 1]
        copies = [send(first, first, to_low), send(second, second, to_side)]
        late = [send(column, column, to_core)]
        wait(copies)

        first = all_ref.at[:, :, side, core, 0]
        second = all_ref.at[:, low, :, core, 1]
        copies = [send(first, first, to_side), send(second, second, to_low)]
        for part in (all_ref.at[:, 1 - low, side, core, 0], all_ref.at[:, low, 1 - side, core, 1]):
            late.append(send(part, part, to_core))
        wait(copies)

        for part in (all_ref.at[:, :, 1 - side, core, 0], all_ref.at[:, 1 - low, :, core, 1]):
            late.append(send(part, part, to_core))
        wait(late)
        save = pltpu.make_async_copy(all_ref, out_ref, save_sems.at[0])
        save.start()
        save.wait()
        return

    chunks = high_count * 8
    lower, upper = high > 0, high < high_count - 1
    own_chunk = all_ref.at[high, low, side, core]
    couple(bands, obs, list_len, rows, terms_ref, data_ref, data_places_ref, own_chunk)
    depth = all_ref.shape[5]
    ahead = depth // 32 * 8

    def copy_of(kind, z, y, x, part, peer, landing):
        chunk = all_ref.at[z, y, x, core, part, ahead:depth]
        number = ((z * 2 + y) * 2 + x) * 2 + part
        return pltpu.make_async_remote_copy(
            src_ref=chunk,
            dst_ref=chunk,
            send_sem=send_sems.at[kind * chunks + number],
            recv_sem=recv_sems.at[landing * chunks + number],
            device_id=peer,
            device_id_type=MESH,
        )

    def plane_copy(chunk, number, landing, peer):
        return pltpu.make_async_remote_copy(
            src_ref=chunk,
            dst_ref=chunk,
            send_sem=plane_send_sems.at[number],
            recv_sem=plane_recv_sems.at[landing],
            device_id=peer,
            device_id_type=MESH,
        )

    def head_x(y, part, number):
        chunk = all_ref.at[high, y, side, core, part, 0:ahead]
        return plane_copy(chunk, number, (y * 2 + side) * 2 + part, to_side)

    def head_y(x, part, number):
        chunk = all_ref.at[high, low, x, core, part, 0:ahead]
        return plane_copy(chunk, number, (low * 2 + x) * 2 + part, to_low)

    def head_arrived(y, x, part):
        chunk = all_ref.at[high, y, x, core, part, 0:ahead]
        plane_copy(chunk, 0, (y * 2 + x) * 2 + part, to_core).wait_recv()

    def plane_along(z, step):
        chunk = all_ref.at[z, :, :, core, :, 0:ahead]
        number = 6 + high_count * ((step + 1) // 2) + z
        return plane_copy(chunk, number, 8 + z, {"sky": (high + step) * 2 + low})

    def plane_over(z):
        chunk = all_ref.at[z, :, :, core, :, 0:ahead]
        return plane_copy(chunk, 6 + 2 * high_count + z, 8 + high_count + z, to_core)

    def along(z, part, step):
        return copy_of((step + 1) // 2, z, low, side, part, {"sky": (high + step) * 2 + low}, 0)

    def across_x(z, y, part):
        return copy_of(2, z, y, side, part, to_side, 0)

    def across_y(z, x, part):
        return copy_of(3, z, low, x, part, to_low, 0)

    def over(z, y, x, part):
        return copy_of(4, z, y, x, part, to_core, 1)

    def arrived(z, y, x, part):
        copy_of(4, z, y, x, part, to_core, 0).wait_recv()

    ends = {-1: lower, 1: upper}

    def along_if(z, part, step):
        @pl.when(ends[step])
        def _():
            along(z, part, step).start()

    def first_hop(z, part):
        if part == 0:
            across_x(z, low, part).start()
        else:
            across_y(z, side, part).start()

    def second_hop(z, part):
        if part == 0:
            across_y(z, side, part).start()
        else:
            across_x(z, low, part).start()

    head_x(low, 0, 0).start()
    head_y(side, 1, 3).start()
    for part in range(2):
        along_if(high, part, 1)
        along_if(high, part, -1)
        first_hop(high, part)
        if part == 0:
            head_y(side, 0, 4).start()
            head_x(low, 1, 1).start()
    for part in range(2):
        second_hop(high, part)
        over(high, low, side, part).start()
    tables()

    def heads_turn():
        head_arrived(low, 1 - side, 0)
        head_y(1 - side, 0, 5).start()
        head_arrived(1 - low, side, 1)
        head_x(1 - low, 1, 2).start()

    def send_plane(z, steps):
        for step in steps:
            @pl.when(ends[step])
            def _(step=step):
                plane_along(z, step).start()

        plane_over(z).start()

    def heads_done():
        for y, x, part in ((1 - low, side, 0), (low, 1 - side, 1), (1 - low, 1 - side, 0), (1 - low, 1 - side, 1)):
            head_arrived(y, x, part)
        send_plane(high, (-1, 1))

    def plane_arrival(distance):
        for step in (-1, 1):
            z = high - step * distance

            @pl.when(z >= 0 if step == 1 else z < high_count)
            def _(z=z, step=step):
                plane_copy(all_ref.at[z, :, :, core, :, 0:ahead], 0, 8 + z, to_core).wait_recv()
                send_plane(z, (step,))

    def column_arrival(distance, part):
        for step in (-1, 1):
            z = high - step * distance
            here = z >= 0 if step == 1 else z < high_count

            @pl.when(here)
            def _(z=z, step=step):
                arrived(z, low, side, part)
                along_if(z, part, step)
                first_hop(z, part)
                second_hop(z, part)
                over(z, low, side, part).start()

    def at_distance(distance, action):
        if distance == 0:
            action(high)
            return
        for step in (-1, 1):
            z = high - step * distance

            @pl.when(z >= 0 if step == 1 else z < high_count)
            def _(z=z):
                action(z)

    def turn(z):
        arrived(z, low, 1 - side, 0)
        across_y(z, 1 - side, 0).start()
        over(z, low, 1 - side, 0).start()
        arrived(z, 1 - low, side, 1)
        across_x(z, 1 - low, 1).start()
        over(z, 1 - low, side, 1).start()

    def last(z):
        for y, x, part in ((1 - low, side, 0), (low, 1 - side, 1), (1 - low, 1 - side, 0), (1 - low, 1 - side, 1)):
            arrived(z, y, x, part)
            over(z, y, x, part).start()

    def save(z, k):
        return pltpu.make_async_copy(all_ref.at[z, :, :, k], out_ref.at[z, :, :, k], save_sems.at[z * 2 + k])

    def save_own(z):
        save(z, core).start()

    def save_other(z):
        for y in range(2):
            for x in range(2):
                for part in range(2):
                    copy_of(4, z, y, x, part, to_core, 1).wait_recv()
        plane_over(z).wait_recv()
        save(z, 1 - core).start()

    heads_turn()
    for distance in range(1, high_count):
        column_arrival(distance, 0)
        at_distance(distance - 1, turn)
        column_arrival(distance, 1)
        if distance == 1:
            heads_done()
            more_tables()
        else:
            plane_arrival(distance - 1)
            at_distance(distance - 2, last)
            at_distance(distance - 2, save_own)
    at_distance(high_count - 1, turn)
    plane_arrival(high_count - 1)
    for distance in range(max(high_count - 2, 0), high_count):
        at_distance(distance, last)
        at_distance(distance, save_own)
    for distance in range(high_count):
        at_distance(distance, save_other)
    for z in range(high_count):
        for y in range(2):
            for x in range(2):
                for part in range(2):
                    copy_of(4, z, y, x, part, to_core, 1).wait_send()
        plane_over(z).wait_send()
        for step in (-1, 1):
            passing = (z >= high) if step == -1 else (z <= high)

            @pl.when(ends[step] & passing)
            def _(z=z, step=step):
                plane_along(z, step).wait_send()

    for y, part, number in ((low, 0, 0), (low, 1, 1), (1 - low, 1, 2)):
        head_x(y, part, number).wait_send()
    for x, part, number in ((side, 1, 3), (side, 0, 4), (1 - side, 0, 5)):
        head_y(x, part, number).wait_send()
    for z in range(high_count):
        for part in range(2):
            for step in (-1, 1):
                passing = (z >= high) if step == -1 else (z <= high)

                @pl.when(ends[step] & passing)
                def _(z=z, part=part, step=step):
                    along(z, part, step).wait_send()

            for other in range(2):
                if part == 0:
                    across_y(z, other, part).wait_send()
                else:
                    across_x(z, other, part).wait_send()
            first = across_x(z, low, part) if part == 0 else across_y(z, side, part)
            first.wait_send()
    for z in range(high_count):
        for k in range(2):
            save(z, k).wait()


def total_kernel(tiles, bands, scale, sums_ref, misfit_ref, all_sums, send_sems, recv_sems):
    my_tile, my_band = lax.axis_index("sky"), lax.axis_index("band")
    me = my_tile * bands + my_band
    peers = []
    for sky_step in range(tiles):
        for band_step in range(bands):
            if sky_step or band_step:
                peers.append({"sky": lax.rem(my_tile + sky_step, tiles), "band": lax.rem(my_band + band_step, bands)})
    barrier = pltpu.get_barrier_semaphore()
    for peer in peers:
        pl.semaphore_signal(barrier, inc=1, device_id=peer, device_id_type=MESH)
    all_sums[pl.ds(me, 1), :] = sums_ref[0:1, :]
    pl.semaphore_wait(barrier, len(peers))
    copies = []
    for number, peer in enumerate(peers):
        copy = pltpu.make_async_remote_copy(
            src_ref=sums_ref.at[0:1],
            dst_ref=all_sums.at[pl.ds(me, 1)],
            send_sem=send_sems.at[number],
            recv_sem=recv_sems.at[number],
            device_id=peer,
            device_id_type=MESH,
        )
        copy.start()
        copies.append(copy)
    for copy in copies:
        copy.wait()
    total = jnp.sum(all_sums[...], axis=0, keepdims=True) / scale
    lane = lax.broadcasted_iota(jnp.int32, (8, LANES), 1)
    picks = (lane * bands + my_band) & (LANES - 1)
    misfit_ref[...] = take(jnp.broadcast_to(total, (8, LANES)), picks)[0:1, 0:SWEEPS]


def body(magnitudes, weights, slots, block_fields, owner, colors, color_terms):
    bands = color_terms.shape[0]
    tiles = lax.axis_size("sky")
    _, obs, stars = magnitudes.shape
    blocks, list_len = block_fields.shape
    rows = stars // blocks
    fields = owner.shape[0]
    owned = fields // tiles
    mine = blocks // bands
    pack = LANES // list_len
    tile_rows = blocks // pack
    row_count = tiles * tile_rows
    vmem = pl.BlockSpec(memory_space=pltpu.VMEM)
    smem = pl.BlockSpec(memory_space=pltpu.SMEM)
    hbm = pl.BlockSpec(memory_space=pl.ANY)
    magnitudes, weights, slots = magnitudes[0], weights[0], slots[0]

    earlier = 3 * (bands - 1) + tiles - 1
    reach = 2 * (REACH * tile_rows + tile_rows - 1) + 1
    own_rows = -(-owned // LANES)
    part = (bands // 2, LANES + EXTRA, LANES)
    everyone = (tiles // 2, 2, bands // 2, 2) + part
    listed = (tiles, 2, tile_rows, LANES)
    if tiles > 8:
        sends = landings = tiles // 2 - 1 + 9
    else:
        sends, landings = 5 * tiles * 4, 2 * tiles * 4
    coupled, pick, entry_colors, window, chosen, data, data_places, places = pl.pallas_call(
        functools.partial(gather_kernel, tiles, bands, obs, list_len, rows, fields),
        out_shape=(
            jax.ShapeDtypeStruct(everyone, jnp.float32),
            jax.ShapeDtypeStruct((pack, reach, row_count, LANES), jnp.int32),
            jax.ShapeDtypeStruct((row_count, LANES), jnp.int32),
            jax.ShapeDtypeStruct((8, LANES), jnp.int32),
            jax.ShapeDtypeStruct((own_rows, 8, LANES), jnp.int32),
            jax.ShapeDtypeStruct((bands, 2, obs, mine * rows), jnp.float32),
            jax.ShapeDtypeStruct((bands, obs, mine * rows), jnp.int32),
            jax.ShapeDtypeStruct((obs, stars), jnp.int32),
        ),
        in_specs=[smem] + [vmem] * 6,
        out_specs=(hbm,) + (vmem,) * 7,
        scratch_shapes=[
            pltpu.VMEM(everyone, jnp.float32),
            pltpu.VMEM((row_count + 16, LANES), jnp.int32),
            pltpu.VMEM(part, jnp.float32),
            pltpu.VMEM((8, LANES), jnp.int32),
            pltpu.VMEM((8, LANES), jnp.int32),
            pltpu.VMEM(listed[1:], jnp.int32),
            pltpu.VMEM(listed, jnp.int32),
            pltpu.VMEM((bands, obs, mine * rows), jnp.int32),
            pltpu.SemaphoreType.DMA((sends,)),
            pltpu.SemaphoreType.DMA((landings,)),
            pltpu.SemaphoreType.DMA((earlier,)),
            pltpu.SemaphoreType.DMA((earlier,)),
            pltpu.SemaphoreType.DMA((6 + 3 * (tiles // 2),)),
            pltpu.SemaphoreType.DMA((8 + tiles,)),
            pltpu.SemaphoreType.DMA((tiles,)),
        ],
        compiler_params=pltpu.CompilerParams(
            collective_id=0, has_side_effects=True, vmem_limit_bytes=60 * 1024 * 1024
        ),
        name="gather",
    )(color_terms, block_fields, colors.reshape(-1, LANES), magnitudes, weights, slots, owner.reshape(-1, LANES))
    coupled = coupled.reshape((-1,) + coupled.shape[-2:])

    big = (bands, row_count, LANES)
    depth = min(row_count, 16)
    own_zp, star_means, sums = pl.pallas_call(
        functools.partial(sweep_kernel, tiles, bands, obs, list_len, rows, row_count),
        out_shape=(
            jax.ShapeDtypeStruct((1, owned), jnp.float32),
            jax.ShapeDtypeStruct((1, stars), jnp.float32),
            jax.ShapeDtypeStruct((8, LANES), jnp.float32),
        ),
        in_specs=[smem, smem, hbm] + [vmem] * 8,
        out_specs=(vmem,) * 3,
        scratch_shapes=[
            pltpu.VMEM((row_count * bands * LANES, LANES), jnp.float32),
            pltpu.VMEM(big, jnp.float32),
            pltpu.VMEM((bands, row_count + 16, LANES), jnp.float32),
            pltpu.VMEM(big, jnp.float32),
            pltpu.VMEM(big, jnp.float32),
            pltpu.VMEM(big, jnp.float32),
            pltpu.VMEM((LANES, LANES), jnp.float32),
            pltpu.VMEM((depth, bands, LANES + EXTRA, LANES), jnp.float32),
            pltpu.SemaphoreType.DMA((depth,)),
        ],
        compiler_params=pltpu.CompilerParams(vmem_limit_bytes=60 * 1024 * 1024),
        name="sweeps",
    )(window, color_terms, coupled, pick, entry_colors, data, data_places, magnitudes, weights, places, chosen)

    devices = tiles * bands
    misfit = pl.pallas_call(
        functools.partial(total_kernel, tiles, bands, float(obs * stars * tiles)),
        out_shape=jax.ShapeDtypeStruct((1, SWEEPS), jnp.float32),
        in_specs=[vmem],
        out_specs=vmem,
        scratch_shapes=[
            pltpu.VMEM((devices, LANES), jnp.float32),
            pltpu.SemaphoreType.DMA((devices - 1,)),
            pltpu.SemaphoreType.DMA((devices - 1,)),
        ],
        compiler_params=pltpu.CompilerParams(collective_id=1, has_side_effects=True),
        name="total",
    )(sums)
    return own_zp, star_means, misfit.reshape(SWEEPS, 1)


def solution(mesh):
    in_specs = (
        P("band", None, "sky"),
        P("band", None, "sky"),
        P("band", None, "sky"),
        P("sky", None),
        P(),
        P(),
        P(),
    )
    out_specs = (P("band", "sky"), P("band", "sky"), P(None, "band"))
    return jax.shard_map(body, mesh=mesh, in_specs=in_specs, out_specs=out_specs, check_vma=False)
```

```python
import functools

import jax
import jax.numpy as jnp
from jax import lax
from jax.experimental import pallas as pl
from jax.experimental.pallas import tpu as pltpu
from jax.sharding import PartitionSpec as P

COLORS = 8
SWEEPS = 4
PRIOR_WEIGHT = 1.0
REACH = 2
HIGHEST = lax.Precision.HIGHEST
LANES = 128
EXTRA = 8
MESH = pl.DeviceIdType.MESH


def contract_lanes(left, right):
    dims = (((1,), (1,)), ((), ()))
    return lax.dot_general(left, right, dims, precision=HIGHEST, preferred_element_type=jnp.float32)


def mixing_of(terms_ref, bands):
    mixing = []
    for band in range(bands):
        total = terms_ref[band, 0]
        for other in range(1, bands):
            total = total + terms_ref[band, other]
        row = [terms_ref[band, other] for other in range(bands)]
        row[band] = (1.0 + row[band]) - total
        mixing.append(row)
    return mixing


def mixed(mixing, band, means):
    predicted = mixing[band][0] * means[0]
    for other in range(1, len(means)):
        predicted = predicted + mixing[band][other] * means[other]
    return predicted


def couple(bands, obs, list_len, rows, terms_ref, data_ref, places_ref, out_ref):
    blocks = data_ref.shape[3] // rows
    mixing = mixing_of(terms_ref, bands)
    row_band = lax.broadcasted_iota(jnp.int32, (LANES, LANES), 0) // list_len
    lane_band = lax.broadcasted_iota(jnp.int32, (LANES, LANES), 1) // list_len
    mix_grid = jnp.zeros((LANES, LANES), jnp.float32)
    for band in range(bands):
        for other in range(bands):
            here = (row_band == other) & (lane_band == band)
            mix_grid = jnp.where(here, mixing[band][other], mix_grid)
    full = []
    entry = lax.broadcasted_iota(jnp.int32, (list_len, rows), 0)
    for block in range(blocks):
        cols = pl.ds(block * rows, rows)
        one_hot, one_hot_mag, star_weight, means = [], [], [], []
        for band in range(bands):
            mags = data_ref[band, 0, :, cols]
            wts = data_ref[band, 1, :, cols]
            slots = places_ref[band, :, cols]
            scaled = wts * mags
            weight_sum = jnp.sum(wts, axis=0, keepdims=True)
            star_weight.append(weight_sum)
            means.append(jnp.sum(scaled, axis=0, keepdims=True) / weight_sum)
            hot = jnp.zeros((list_len, rows), jnp.float32)
            hot_mag = jnp.zeros((list_len, rows), jnp.float32)
            for k in range(obs):
                hit = slots[k : k + 1] == entry
                hot = hot + jnp.where(hit, wts[k : k + 1], 0.0)
                hot_mag = hot_mag + jnp.where(hit, scaled[k : k + 1], 0.0)
            one_hot.append(hot)
            one_hot_mag.append(hot_mag)
        rest = []
        shares = []
        for band in range(bands):
            rest.append(one_hot_mag[band] - one_hot[band] * mixed(mixing, band, means))
            shares.append(one_hot[band] / star_weight[band])
        hot_all = jnp.concatenate(one_hot, axis=0)
        share_all = jnp.concatenate(shares, axis=0)
        rest_all = jnp.concatenate(rest, axis=0)
        coupling = contract_lanes(share_all, hot_all) * mix_grid
        ones = jnp.ones((8, rows), jnp.float32)
        rest_row = contract_lanes(ones, rest_all)
        weight_row = contract_lanes(ones, hot_all)
        first = lax.broadcasted_iota(jnp.int32, (EXTRA, LANES), 0) == 0
        full.append(jnp.concatenate([coupling, jnp.where(first, rest_row, weight_row)], axis=0))
    split = bands // 2
    for part in range(split):
        pieces = []
        for half in range(2):
            band = half * split + part
            for block in range(blocks):
                pieces.append(full[block][:, band * list_len : (band + 1) * list_len])
        out_ref[part] = jnp.concatenate(pieces, axis=1)


def sweep_kernel(
    tiles, bands, obs, list_len, rows, row_count,
    window_ref, terms_ref, coupled_ref, pick_ref, color_ref,
    data_ref, data_places_ref, mags_ref, wts_ref, places_ref, chosen_ref,
    own_zp_ref, means_ref, sums_ref,
    kt, base, tot, rden, zp, move, lines, stage, sems,
):
    groups = row_count // 8
    pack = LANES // list_len
    split = bands // 2
    levels, places = pick_ref.shape[:2]
    depth = stage.shape[0]
    lane = lax.broadcasted_iota(jnp.int32, (8, LANES), 1)
    lane_wide = lax.broadcasted_iota(jnp.int32, (LANES + EXTRA, LANES), 1)

    def fetch(row, slot):
        return pltpu.make_async_copy(
            coupled_ref.at[pl.ds(row * (2 * split), 2 * split)], stage.at[slot], sems.at[slot]
        )

    for row in range(depth - 1):
        fetch(row, row).start()

    def unpack(row, carry):
        slot = lax.rem(row, depth)
        ahead = row + depth - 1

        @pl.when(ahead < row_count)
        def _():
            fetch(ahead, lax.rem(ahead, depth)).start()

        fetch(row, slot).wait()
        group = lax.div(row, 8)
        place = lax.rem(row, 8)
        for part in range(split):
            left = stage[slot, part]
            right = stage[slot, split + part]
            low = jnp.where(lane_wide < LANES // 2, left, pltpu.roll(right, LANES // 2, 1))
            high = jnp.where(lane_wide < LANES // 2, pltpu.roll(left, LANES // 2, 1), right)
            for band, value in ((part, low), (split + part, high)):
                start = (group * bands + band) * (LANES * 8) + place
                kt[pl.ds(start, LANES, stride=8), :] = value[0:LANES]
                base[band, pl.ds(row, 1), :] = value[LANES : LANES + 1]
                tot[band, pl.ds(row + 8, 1), :] = value[LANES + 1 : LANES + 2]
        return carry

    lax.fori_loop(0, row_count, unpack, 0)

    def rows_of(group):
        return pl.ds(pl.multiple_of(group * 8, 8), 8)

    def wrap():
        for band in range(bands):
            tot[band, 0:8, :] = tot[band, row_count : row_count + 8, :]
            tot[band, row_count + 8 : row_count + 16, :] = tot[band, 8:16, :]

    def gather(group, first, count, sums):
        for place in range(places):
            start = group * 8 + (8 + place - places // 2)
            near = [tot[band, pl.ds(start, 8), :] for band in range(bands)]
            for level in range(count):
                pick = pick_ref[first + level, place, rows_of(group), :]
                mask = pick < LANES
                lanes = pick & (LANES - 1)
                for band in range(bands):
                    index = 2 * band + level % 2
                    sums[index] = sums[index] + jnp.where(mask, take(near[band], lanes), 0.0)
        return sums

    span = 2 if groups % 2 == 0 else 1

    def gathered(batch):
        around = [batch * span + part for part in range(span)]
        first = []
        for group in around:
            sums = []
            for band in range(bands):
                middle = pl.ds(pl.multiple_of(group * 8 + 8, 8), 8)
                sums += [tot[band, middle, :], jnp.zeros((8, LANES), jnp.float32)]
            first.append(gather(group, 0, 2, sums))

        def deeper(level, sums):
            return [gather(group, level, 1, part) for group, part in zip(around, sums)]

        result = lax.fori_loop(2, window_ref[0, 2], deeper, first)
        return [(group, [part[2 * b] + part[2 * b + 1] for b in range(bands)]) for group, part in zip(around, result)]

    def weigh(batch, carry):
        for group, values in gathered(batch):
            for band, value in enumerate(values):
                rden[band, rows_of(group), :] = 1.0 / (value + PRIOR_WEIGHT)
        return carry

    wrap()
    lax.fori_loop(0, groups // span, weigh, 0)
    zp[...] = jnp.zeros_like(zp)
    tot[:, 8 : row_count + 8, :] = base[...]
    wrap()

    def push(width, origin):
        def add(group, inner):
            here = [move[band, rows_of(group), :] for band in range(bands)]
            middle = pl.ds(pl.multiple_of(group * 8 + 8, 8), 8)
            sums = [tot[band, middle, :] for band in range(bands)]
            for entry in range(width):
                lanes = (lane & (LANES - list_len)) + (origin + entry)
                values = [take(here[band], lanes) for band in range(bands)]
                for band in range(bands):
                    for other in range(bands):
                        start = (group * bands + band) * (LANES * 8) + (other * list_len + origin + entry) * 8
                        rows = pl.ds(pl.multiple_of(start, 8), 8)
                        sums[band] = sums[band] + values[other] * kt[rows, :]
            for band in range(bands):
                tot[band, middle, :] = sums[band]
            return inner

        lax.fori_loop(0, groups, add, 0, unroll=2)

    halves = rows // LANES
    stars = mags_ref.shape[1]
    blocks = stars // rows
    tile_rows = blocks // pack
    mine = data_ref.shape[3] // rows
    my_tile, my_band = lax.axis_index("sky"), lax.axis_index("band")
    first = lax.rem(my_band * mine, pack)
    my_row = my_tile * tile_rows + lax.div(my_band * mine, pack)
    mixing = mixing_of(terms_ref, bands)
    lines[...] = jnp.zeros_like(lines)

    def spread(row, picks):
        return take(jnp.broadcast_to(row, (obs, LANES)), picks)

    def misfit_lines(sweep):
        partial = [jnp.zeros((obs, LANES), jnp.float32) for _ in range(bands)]
        for block in range(mine):
            for half in range(halves):
                cols = pl.ds(block * rows + half * LANES, LANES)
                left, means = [], []
                for band in range(bands):
                    wts = data_ref[band, 1, :, cols]
                    picks = data_places_ref[band, :, cols] + (first + block) * list_len
                    mags = data_ref[band, 0, :, cols] - spread(zp[band, pl.ds(my_row, 1), :], picks)
                    left.append(mags)
                    means.append(jnp.sum(wts * mags, axis=0, keepdims=True) / jnp.sum(wts, axis=0, keepdims=True))
                for band in range(bands):
                    wts = data_ref[band, 1, :, cols]
                    partial[band] = partial[band] + wts * (left[band] - mixed(mixing, band, means)) ** 2
        for band in range(bands):
            lines[pl.ds(sweep * bands + band, 1), :] = jnp.sum(partial[band], axis=0, keepdims=True)

    def step(number, carry):
        color_no = lax.rem(number, COLORS)

        def update(batch, inner):
            for group, values in gathered(batch):
                rows = rows_of(group)
                now = color_ref[rows, :] == color_no
                for band, value in enumerate(values):
                    old = zp[band, rows, :]
                    new = jnp.where(now, value * rden[band, rows, :], old)
                    zp[band, rows, :] = new
                    move[band, rows, :] = new - old
            return inner

        lax.fori_loop(0, groups // span, update, 0)

        @pl.when(color_no == COLORS - 1)
        def _():
            misfit_lines(lax.div(number, COLORS))

        low, high = window_ref[color_no, 0], window_ref[color_no, 1]
        widths = [list_len * eighths // 16 for eighths in range(4, 9)]
        more = number < SWEEPS * COLORS - 1
        for index, width in enumerate(widths):
            fits = more & (high - low <= width)
            if index:
                fits = fits & (high - low > widths[index - 1])

            @pl.when(fits)
            def _(width=width):
                push(width, jnp.minimum(low, list_len - width))

        @pl.when(more & (high - low > widths[-1]))
        def _():
            lax.fori_loop(0, 2, lambda part, inner: (push(widths[-1], part * widths[-1]), inner)[1], 0)

        wrap()
        return carry

    lax.fori_loop(0, SWEEPS * COLORS, step, 0)
    sums_ref[...] = contract_lanes(jnp.ones((8, LANES), jnp.float32), lines[...])
    for block in range(blocks):
        row = zp[my_band, pl.ds(my_tile * tile_rows + block // pack, 1), :]
        for half in range(halves):
            cols = pl.ds(block * rows + half * LANES, LANES)
            wts = wts_ref[:, cols]
            picks = places_ref[:, cols] + block % pack * list_len
            left = wts * (mags_ref[:, cols] - spread(row, picks))
            means_ref[0:1, cols] = jnp.sum(left, axis=0, keepdims=True) / jnp.sum(wts, axis=0, keepdims=True)
    below = lax.broadcasted_iota(jnp.int32, (8, LANES), 0)
    close = jnp.zeros((8, LANES), jnp.float32)
    for offset in range(3):
        tile = lax.rem(my_tile + offset + tiles - 1, tiles)
        for row in range(tile_rows):
            value = zp[my_band, pl.ds(tile * tile_rows + row, 1), :]
            close = jnp.where(below == offset * tile_rows + row, jnp.broadcast_to(value, (8, LANES)), close)
    owned = own_zp_ref.shape[1]
    for row in range(chosen_ref.shape[0]):
        pick = chosen_ref[row]
        value = jnp.where(pick < LANES, take(close, pick & (LANES - 1)), 0.0)
        value = jnp.sum(value, axis=0, keepdims=True)
        width = min(LANES, owned - row * LANES)
        own_zp_ref[0:1, row * LANES : row * LANES + width] = value[:, 0:width]


def take(value, picks):
    return jnp.take_along_axis(value, picks, axis=1, mode="promise_in_bounds")


def sort_entries(list_len, fields, listed, color_ref):
    lane = lax.broadcasted_iota(jnp.int32, (8, LANES), 1)
    segment = lane & (LANES - list_len)
    live = listed < fields
    row_no, lane_no = listed // LANES, listed % LANES
    color = jnp.full((8, LANES), -1, jnp.int32)
    for row in range(color_ref.shape[0]):
        table = jnp.broadcast_to(color_ref[row : row + 1, :], (8, LANES))
        color = jnp.where(row_no == row, take(table, lane_no), color)
    color = jnp.where(live, color, -1)
    masks = jnp.concatenate([(color == c).astype(jnp.float32) for c in range(COLORS)], axis=0)
    source = lax.broadcasted_iota(jnp.int32, (LANES, LANES), 0)
    target = lax.broadcasted_iota(jnp.int32, (LANES, LANES), 1)
    same = (source // list_len) == (target // list_len)
    dims = (((1,), (0,)), ((), ()))
    before = (same & (source < target)).astype(jnp.float32)
    ranks = lax.dot_general(masks, before, dims, preferred_element_type=jnp.float32)
    counts = lax.dot_general(masks, same.astype(jnp.float32), dims, preferred_element_type=jnp.float32)
    rest = jnp.zeros((8, LANES), jnp.float32)
    room = [None] * COLORS
    for c in reversed(range(COLORS)):
        rest = rest + counts[c * 8 : c * 8 + 8]
        room[c] = list_len - rest
    end = jnp.zeros((8, LANES), jnp.float32)
    place = jnp.full((8, LANES), -1.0, jnp.float32)
    for c in range(COLORS):
        start = jnp.minimum(jnp.maximum(end, float(list_len * c // COLORS)), room[c])
        end = start + counts[c * 8 : c * 8 + 8]
        place = jnp.where(color == c, start + ranks[c * 8 : c * 8 + 8], place)
    place = place.astype(jnp.int32)
    sorted_fields = jnp.full((8, LANES), fields, jnp.int32)
    sorted_colors = jnp.full((8, LANES), -1, jnp.int32)
    for entry in range(list_len):
        picks = segment + entry
        hit = take(place, picks) == lane - segment
        sorted_fields = jnp.where(hit, take(listed, picks), sorted_fields)
        sorted_colors = jnp.where(hit, take(color, picks), sorted_colors)
    return place, sorted_fields, sorted_colors


def match(list_len, fields, lists_ref, rows_ref, pick_ref, color_ref):
    tiles, _, tile_rows, _ = lists_ref.shape
    pack = LANES // list_len
    levels, places, row_count, _ = pick_ref.shape
    lane = lax.broadcasted_iota(jnp.int32, (8, LANES), 1)
    for tile in range(tiles):
        start = tile * tile_rows
        rows_ref[8 + start : 8 + start + tile_rows, :] = lists_ref[tile, 0]
        color_ref[start : start + tile_rows, :] = lists_ref[tile, 1]
    rows_ref[0:8, :] = rows_ref[row_count : row_count + 8, :]
    rows_ref[row_count + 8 : row_count + 16, :] = rows_ref[8:16, :]

    def group_picks(group, carry):
        home = rows_ref[pl.ds(pl.multiple_of(group * 8 + 8, 8), 8), :]
        home = jnp.where(home < fields, home, -1)
        near = [rows_ref[pl.ds(group * 8 + 8 + place - places // 2, 8), :] for place in range(places)]
        found = [[] for _ in range(places)]
        for quarter in range(pack):
            picks = [jnp.full((8, LANES), LANES, jnp.int32) for _ in range(places)]
            for entry in range(list_len):
                source = quarter * list_len + entry
                for place in range(places):
                    other = jnp.broadcast_to(near[place][:, source : source + 1], (8, LANES))
                    picks[place] = jnp.where(other == home, source, picks[place])
            for place in range(places):
                found[place].append(picks[place])
        rows = pl.ds(pl.multiple_of(group * 8, 8), 8)
        for place in range(places):
            ranked = found[place]
            if place == places // 2:
                ranked = [jnp.where(pick == lane, LANES, pick) for pick in ranked]
            for turn in range(pack):
                for low in range(turn % 2, pack - 1, 2):
                    pair = ranked[low], ranked[low + 1]
                    ranked[low], ranked[low + 1] = jnp.minimum(*pair), jnp.maximum(*pair)
            for level in range(pack):
                pick_ref[level, place, rows, :] = ranked[level]
        return carry

    lax.fori_loop(0, row_count // 8, group_picks, 0)


def windows(list_len, pick_ref, color_ref, window_ref):
    levels, places, row_count, _ = pick_ref.shape
    lane = lax.broadcasted_iota(jnp.int32, (8, LANES), 1)
    position = (lane & (list_len - 1)).astype(jnp.float32)

    def rows_of(group):
        return pl.ds(pl.multiple_of(group * 8, 8), 8)

    def bounds(group, carry):
        lows, highs = carry
        color = color_ref[rows_of(group), :]
        new_lows, new_highs = [], []
        for c in range(COLORS):
            new_lows.append(jnp.minimum(lows[c], jnp.where(color == c, position, float(list_len))))
            new_highs.append(jnp.maximum(highs[c], jnp.where(color == c, position + 1.0, 0.0)))
        return new_lows, new_highs

    start = [jnp.full((8, LANES), float(list_len), jnp.float32)] * COLORS, [jnp.zeros((8, LANES), jnp.float32)] * COLORS
    lows, highs = lax.fori_loop(0, row_count // 8, bounds, start)
    lows = jnp.concatenate([jnp.min(value, axis=0, keepdims=True) for value in lows], axis=0)
    highs = jnp.concatenate([jnp.max(value, axis=0, keepdims=True) for value in highs], axis=0)
    lows = jnp.min(lows, axis=1, keepdims=True)
    highs = jnp.max(highs, axis=1, keepdims=True)
    deepest = jnp.full((8, LANES), 2.0, jnp.float32)
    for level in range(2, levels):
        def least(group, value, level=level):
            for place in range(places):
                value = jnp.minimum(value, pick_ref[level, place, rows_of(group), :])
            return value

        found = lax.fori_loop(0, row_count // 8, least, jnp.full((8, LANES), LANES, jnp.int32))
        deepest = jnp.where(found < LANES, level + 1.0, deepest)
    deepest = jnp.max(jnp.max(deepest, axis=0, keepdims=True), axis=1, keepdims=True)
    table = jnp.where(lane == 0, lows, jnp.where(lane == 1, highs, deepest))
    window_ref[...] = table.astype(jnp.int32)


def choose(tiles, fields, owner_ref, rows_ref, chosen_ref):
    field_rows = owner_ref.shape[0]
    tile_rows = (rows_ref.shape[0] - 16) // tiles
    my_tile = lax.axis_index("sky")
    lane = lax.broadcasted_iota(jnp.int32, (8, LANES), 1)
    below = lax.broadcasted_iota(jnp.int32, (8, LANES), 0)
    owned = owner_ref[...] == my_tile
    ones = owned.astype(jnp.float32)
    source = lax.broadcasted_iota(jnp.int32, (LANES, LANES), 0)
    target = lax.broadcasted_iota(jnp.int32, (LANES, LANES), 1)
    dims = (((1,), (0,)), ((), ()))
    inside = lax.dot_general(ones, (source < target).astype(jnp.float32), dims, preferred_element_type=jnp.float32)
    counts = lax.dot_general(ones, jnp.ones((LANES, LANES), jnp.float32), dims, preferred_element_type=jnp.float32)
    upper = lax.broadcasted_iota(jnp.int32, (field_rows, field_rows), 1)
    lower = lax.broadcasted_iota(jnp.int32, (field_rows, field_rows), 0)
    above = lax.dot_general((upper < lower).astype(jnp.float32), counts, dims, preferred_element_type=jnp.float32)
    rank = jnp.where(owned, (inside + above).astype(jnp.int32), -1)
    close = jnp.full((8, LANES), fields, jnp.int32)
    for offset in range(3):
        tile = lax.rem(my_tile + offset + tiles - 1, tiles)
        for row in range(tile_rows):
            value = rows_ref[pl.ds(8 + tile * tile_rows + row, 1), :]
            close = jnp.where(below == offset * tile_rows + row, jnp.broadcast_to(value, (8, LANES)), close)
    row_no, lane_no = close // LANES, close % LANES
    order = jnp.full((8, LANES), -1, jnp.int32)
    for row in range(field_rows):
        table = jnp.broadcast_to(rank[row : row + 1, :], (8, LANES))
        order = jnp.where(row_no == row, take(table, lane_no), order)
    own_rows = chosen_ref.shape[0]
    codes = [jnp.full((8, LANES), -1, jnp.int32) for _ in range(own_rows)]
    for entry in range(LANES):
        value = jnp.broadcast_to(order[:, entry : entry + 1], (8, LANES))
        for row in range(own_rows):
            codes[row] = jnp.where(value == row * LANES + lane, entry, codes[row])
    for row in range(own_rows):
        ranked = jnp.where(codes[row] >= 0, (below + 1).astype(jnp.float32), 0.0)
        last = jnp.max(ranked, axis=0, keepdims=True)
        keep = (ranked > 0.0) & (ranked == last)
        chosen_ref[row] = jnp.where(keep, codes[row], LANES)


def relabel(list_len, rows, block, offset, place_ref, slots_ref, out_ref):
    pack = LANES // list_len
    table = jnp.broadcast_to(place_ref[pl.ds(block // pack, 1), :], (slots_ref.shape[0], LANES))
    for half in range(rows // LANES):
        cols = pl.ds(offset + half * LANES, LANES)
        out_ref[:, cols] = take(table, slots_ref[:, cols] + block % pack * list_len)


def gather_kernel(
    tiles, bands, obs, list_len, rows, fields,
    terms_ref, tile_lists_ref, field_colors_ref, mags_ref, wts_ref, slots_ref, owner_ref,
    out_ref, pick_ref, color_ref, window_ref, chosen_ref, data_ref, data_places_ref, places_ref,
    all_ref, rows_ref, own_ref, listed_ref, place_ref, sorted_ref, lists_ref, data_slots_ref,
    send_sems, recv_sems, early_send_sems, early_recv_sems, plane_send_sems, plane_recv_sems, save_sems,
):
    high_count = tiles // 2
    blocks = tile_lists_ref.shape[0]
    pack = LANES // list_len
    tile_rows = blocks // pack
    mine = blocks // bands
    width = mine * rows
    sky, band = lax.axis_index("sky"), lax.axis_index("band")
    high, low = sky // 2, sky % 2
    side, core = band // 2, band % 2
    to_low = {"sky": high * 2 + (1 - low)}
    to_side = {"band": (1 - side) * 2 + core}
    to_core = {"band": side * 2 + (1 - core)}
    barrier = pltpu.get_barrier_semaphore()
    tile_peers = [lax.rem(sky + step, tiles) for step in range(1, tiles)]
    band_peers = [lax.rem(band + step, bands) for step in range(1, bands)]
    for peer in tile_peers:
        pl.semaphore_signal(barrier, inc=1, device_id={"sky": peer}, device_id_type=MESH)
    for peer in band_peers:
        pl.semaphore_signal(barrier, inc=1, device_id={"band": peer}, device_id_type=MESH)

    listed_ref[...] = jnp.full((8, LANES), fields, jnp.int32)
    for row in range(tile_rows):
        pieces = [tile_lists_ref[row * pack + part : row * pack + part + 1, :] for part in range(pack)]
        listed_ref[row : row + 1, :] = jnp.concatenate(pieces, axis=1)
    place, sorted_fields, sorted_colors = sort_entries(list_len, fields, listed_ref[...], field_colors_ref)
    place_ref[...] = place
    sorted_ref[0] = sorted_fields[0:tile_rows]
    sorted_ref[1] = sorted_colors[0:tile_rows]
    lists_ref[sky] = sorted_ref[...]
    pl.semaphore_wait(barrier, tiles + bands - 2)

    def early(number, source, target, device):
        copy = pltpu.make_async_remote_copy(
            src_ref=source,
            dst_ref=target,
            send_sem=early_send_sems.at[number],
            recv_sem=early_recv_sems.at[number],
            device_id=device,
            device_id_type=MESH,
        )
        copy.start()
        return copy

    def columns(peer):
        return pl.ds(pl.multiple_of(peer * width, LANES), width)

    data_copies, list_copies = [], []
    for step, peer in enumerate(band_peers):
        cols = columns(peer)
        for kind, (source, target) in enumerate((
            (slots_ref, data_slots_ref.at[band]),
            (wts_ref, data_ref.at[band, 1]),
            (mags_ref, data_ref.at[band, 0]),
        )):
            data_copies.append(early(3 * step + kind, source.at[:, cols], target, {"band": peer}))
    for step, peer in enumerate(tile_peers):
        list_copies.append(early(3 * (bands - 1) + step, sorted_ref, lists_ref.at[sky], {"sky": peer}))
    data_ref[band, 0] = mags_ref[:, columns(band)]
    data_ref[band, 1] = wts_ref[:, columns(band)]
    data_slots_ref[band] = slots_ref[:, columns(band)]
    for block in range(blocks):
        relabel(list_len, rows, block, block * rows, place_ref, slots_ref, places_ref)
    for copy in data_copies:
        copy.wait_recv()
    for other in range(bands):
        for block in range(mine):
            source, target = data_slots_ref.at[other], data_places_ref.at[other]
            relabel(list_len, rows, band * mine + block, block * rows, place_ref, source, target)

    def tables():
        for copy in list_copies:
            copy.wait_recv()
        match(list_len, fields, lists_ref, rows_ref, pick_ref, color_ref)

    def more_tables():
        windows(list_len, pick_ref, color_ref, window_ref)
        choose(tiles, fields, owner_ref, rows_ref, chosen_ref)
        for copy in data_copies + list_copies:
            copy.wait_send()

    if high_count > 4:
        highs = [lax.rem(high + step, high_count) for step in range(1, high_count)]
        peers = [{"sky": peer * 2 + low} for peer in highs]
        couple(bands, obs, list_len, rows, terms_ref, data_ref, data_places_ref, own_ref)
        count = [0]

        def send(source, target, peer):
            copy = pltpu.make_async_remote_copy(
                src_ref=source,
                dst_ref=target,
                send_sem=send_sems.at[count[0]],
                recv_sem=recv_sems.at[count[0]],
                device_id=peer,
                device_id_type=MESH,
            )
            count[0] += 1
            copy.start()
            return copy

        def wait(copies):
            for copy in copies:
                copy.wait()

        mine = all_ref.at[high, low, side, core]
        copies = [send(own_ref, mine, peer) for peer in peers]
        all_ref[high, low, side, core] = own_ref[...]
        tables()
        more_tables()
        wait(copies)

        column = all_ref.at[:, low, side, core]
        first = all_ref.at[:, low, side, core, 0]
        second = all_ref.at[:, low, side, core, 1]
        copies = [send(first, first, to_low), send(second, second, to_side)]
        late = [send(column, column, to_core)]
        wait(copies)

        first = all_ref.at[:, :, side, core, 0]
        second = all_ref.at[:, low, :, core, 1]
        copies = [send(first, first, to_side), send(second, second, to_low)]
        for part in (all_ref.at[:, 1 - low, side, core, 0], all_ref.at[:, low, 1 - side, core, 1]):
            late.append(send(part, part, to_core))
        wait(copies)

        for part in (all_ref.at[:, :, 1 - side, core, 0], all_ref.at[:, 1 - low, :, core, 1]):
            late.append(send(part, part, to_core))
        wait(late)
        save = pltpu.make_async_copy(all_ref, out_ref, save_sems.at[0])
        save.start()
        save.wait()
        return

    chunks = high_count * 8
    lower, upper = high > 0, high < high_count - 1
    own_chunk = all_ref.at[high, low, side, core]
    couple(bands, obs, list_len, rows, terms_ref, data_ref, data_places_ref, own_chunk)
    depth = all_ref.shape[5]
    ahead = depth // 32 * 8

    def copy_of(kind, z, y, x, part, peer, landing):
        chunk = all_ref.at[z, y, x, core, part, ahead:depth]
        number = ((z * 2 + y) * 2 + x) * 2 + part
        return pltpu.make_async_remote_copy(
            src_ref=chunk,
            dst_ref=chunk,
            send_sem=send_sems.at[kind * chunks + number],
            recv_sem=recv_sems.at[landing * chunks + number],
            device_id=peer,
            device_id_type=MESH,
        )

    def plane_copy(chunk, number, landing, peer):
        return pltpu.make_async_remote_copy(
            src_ref=chunk,
            dst_ref=chunk,
            send_sem=plane_send_sems.at[number],
            recv_sem=plane_recv_sems.at[landing],
            device_id=peer,
            device_id_type=MESH,
        )

    def head_x(y, part, number):
        chunk = all_ref.at[high, y, side, core, part, 0:ahead]
        return plane_copy(chunk, number, (y * 2 + side) * 2 + part, to_side)

    def head_y(x, part, number):
        chunk = all_ref.at[high, low, x, core, part, 0:ahead]
        return plane_copy(chunk, number, (low * 2 + x) * 2 + part, to_low)

    def head_arrived(y, x, part):
        chunk = all_ref.at[high, y, x, core, part, 0:ahead]
        plane_copy(chunk, 0, (y * 2 + x) * 2 + part, to_core).wait_recv()

    def plane_along(z, step):
        chunk = all_ref.at[z, :, :, core, :, 0:ahead]
        number = 6 + high_count * ((step + 1) // 2) + z
        return plane_copy(chunk, number, 8 + z, {"sky": (high + step) * 2 + low})

    def plane_over(z):
        chunk = all_ref.at[z, :, :, core, :, 0:ahead]
        return plane_copy(chunk, 6 + 2 * high_count + z, 8 + high_count + z, to_core)

    def along(z, part, step):
        return copy_of((step + 1) // 2, z, low, side, part, {"sky": (high + step) * 2 + low}, 0)

    def across_x(z, y, part):
        return copy_of(2, z, y, side, part, to_side, 0)

    def across_y(z, x, part):
        return copy_of(3, z, low, x, part, to_low, 0)

    def over(z, y, x, part):
        return copy_of(4, z, y, x, part, to_core, 1)

    def arrived(z, y, x, part):
        copy_of(4, z, y, x, part, to_core, 0).wait_recv()

    ends = {-1: lower, 1: upper}

    def along_if(z, part, step):
        @pl.when(ends[step])
        def _():
            along(z, part, step).start()

    def first_hop(z, part):
        if part == 0:
            across_x(z, low, part).start()
        else:
            across_y(z, side, part).start()

    def second_hop(z, part):
        if part == 0:
            across_y(z, side, part).start()
        else:
            across_x(z, low, part).start()

    head_x(low, 0, 0).start()
    head_y(side, 1, 3).start()
    for part in range(2):
        along_if(high, part, 1)
        along_if(high, part, -1)
        first_hop(high, part)
        if part == 0:
            head_y(side, 0, 4).start()
            head_x(low, 1, 1).start()
    for part in range(2):
        second_hop(high, part)
        over(high, low, side, part).start()
    tables()

    def heads_turn():
        head_arrived(low, 1 - side, 0)
        head_y(1 - side, 0, 5).start()
        head_arrived(1 - low, side, 1)
        head_x(1 - low, 1, 2).start()

    def send_plane(z, steps):
        for step in steps:
            @pl.when(ends[step])
            def _(step=step):
                plane_along(z, step).start()

        plane_over(z).start()

    def heads_done():
        for y, x, part in ((1 - low, side, 0), (low, 1 - side, 1), (1 - low, 1 - side, 0), (1 - low, 1 - side, 1)):
            head_arrived(y, x, part)
        send_plane(high, (-1, 1))

    def plane_arrival(distance):
        for step in (-1, 1):
            z = high - step * distance

            @pl.when(z >= 0 if step == 1 else z < high_count)
            def _(z=z, step=step):
                plane_copy(all_ref.at[z, :, :, core, :, 0:ahead], 0, 8 + z, to_core).wait_recv()
                send_plane(z, (step,))

    def column_arrival(distance, part):
        for step in (-1, 1):
            z = high - step * distance
            here = z >= 0 if step == 1 else z < high_count

            @pl.when(here)
            def _(z=z, step=step):
                arrived(z, low, side, part)
                along_if(z, part, step)
                first_hop(z, part)
                second_hop(z, part)
                over(z, low, side, part).start()

    def at_distance(distance, action):
        if distance == 0:
            action(high)
            return
        for step in (-1, 1):
            z = high - step * distance

            @pl.when(z >= 0 if step == 1 else z < high_count)
            def _(z=z):
                action(z)

    def turn(z):
        arrived(z, low, 1 - side, 0)
        across_y(z, 1 - side, 0).start()
        over(z, low, 1 - side, 0).start()
        arrived(z, 1 - low, side, 1)
        across_x(z, 1 - low, 1).start()
        over(z, 1 - low, side, 1).start()

    def last(z):
        for y, x, part in ((1 - low, side, 0), (low, 1 - side, 1), (1 - low, 1 - side, 0), (1 - low, 1 - side, 1)):
            arrived(z, y, x, part)
            over(z, y, x, part).start()

    def save(z, k):
        return pltpu.make_async_copy(all_ref.at[z, :, :, k], out_ref.at[z, :, :, k], save_sems.at[z * 2 + k])

    def save_own(z):
        save(z, core).start()

    def save_other(z):
        for y in range(2):
            for x in range(2):
                for part in range(2):
                    copy_of(4, z, y, x, part, to_core, 1).wait_recv()
        plane_over(z).wait_recv()
        save(z, 1 - core).start()

    heads_turn()
    for distance in range(1, high_count):
        column_arrival(distance, 0)
        at_distance(distance - 1, turn)
        column_arrival(distance, 1)
        if distance == 1:
            heads_done()
            more_tables()
        else:
            plane_arrival(distance - 1)
            at_distance(distance - 2, last)
            at_distance(distance - 2, save_own)
    at_distance(high_count - 1, turn)
    plane_arrival(high_count - 1)
    for distance in range(max(high_count - 2, 0), high_count):
        at_distance(distance, last)
        at_distance(distance, save_own)
    for distance in range(high_count):
        at_distance(distance, save_other)
    for z in range(high_count):
        for y in range(2):
            for x in range(2):
                for part in range(2):
                    copy_of(4, z, y, x, part, to_core, 1).wait_send()
        plane_over(z).wait_send()
        for step in (-1, 1):
            passing = (z >= high) if step == -1 else (z <= high)

            @pl.when(ends[step] & passing)
            def _(z=z, step=step):
                plane_along(z, step).wait_send()

    for y, part, number in ((low, 0, 0), (low, 1, 1), (1 - low, 1, 2)):
        head_x(y, part, number).wait_send()
    for x, part, number in ((side, 1, 3), (side, 0, 4), (1 - side, 0, 5)):
        head_y(x, part, number).wait_send()
    for z in range(high_count):
        for part in range(2):
            for step in (-1, 1):
                passing = (z >= high) if step == -1 else (z <= high)

                @pl.when(ends[step] & passing)
                def _(z=z, part=part, step=step):
                    along(z, part, step).wait_send()

            for other in range(2):
                if part == 0:
                    across_y(z, other, part).wait_send()
                else:
                    across_x(z, other, part).wait_send()
            first = across_x(z, low, part) if part == 0 else across_y(z, side, part)
            first.wait_send()
    for z in range(high_count):
        for k in range(2):
            save(z, k).wait()


def total_kernel(tiles, bands, scale, sums_ref, misfit_ref, all_sums, send_sems, recv_sems):
    my_tile, my_band = lax.axis_index("sky"), lax.axis_index("band")
    me = my_tile * bands + my_band
    peers = []
    for sky_step in range(tiles):
        for band_step in range(bands):
            if sky_step or band_step:
                peers.append({"sky": lax.rem(my_tile + sky_step, tiles), "band": lax.rem(my_band + band_step, bands)})
    barrier = pltpu.get_barrier_semaphore()
    for peer in peers:
        pl.semaphore_signal(barrier, inc=1, device_id=peer, device_id_type=MESH)
    all_sums[pl.ds(me, 1), :] = sums_ref[0:1, :]
    pl.semaphore_wait(barrier, len(peers))
    copies = []
    for number, peer in enumerate(peers):
        copy = pltpu.make_async_remote_copy(
            src_ref=sums_ref.at[0:1],
            dst_ref=all_sums.at[pl.ds(me, 1)],
            send_sem=send_sems.at[number],
            recv_sem=recv_sems.at[number],
            device_id=peer,
            device_id_type=MESH,
        )
        copy.start()
        copies.append(copy)
    for copy in copies:
        copy.wait()
    total = jnp.sum(all_sums[...], axis=0, keepdims=True) / scale
    lane = lax.broadcasted_iota(jnp.int32, (8, LANES), 1)
    picks = (lane * bands + my_band) & (LANES - 1)
    misfit_ref[...] = take(jnp.broadcast_to(total, (8, LANES)), picks)[0:1, 0:SWEEPS]


def body(magnitudes, weights, slots, block_fields, owner, colors, color_terms):
    bands = color_terms.shape[0]
    tiles = lax.axis_size("sky")
    _, obs, stars = magnitudes.shape
    blocks, list_len = block_fields.shape
    rows = stars // blocks
    fields = owner.shape[0]
    owned = fields // tiles
    mine = blocks // bands
    pack = LANES // list_len
    tile_rows = blocks // pack
    row_count = tiles * tile_rows
    vmem = pl.BlockSpec(memory_space=pltpu.VMEM)
    smem = pl.BlockSpec(memory_space=pltpu.SMEM)
    hbm = pl.BlockSpec(memory_space=pl.ANY)
    magnitudes, weights, slots = magnitudes[0], weights[0], slots[0]

    earlier = 3 * (bands - 1) + tiles - 1
    reach = 2 * (REACH * tile_rows + tile_rows - 1) + 1
    own_rows = -(-owned // LANES)
    part = (bands // 2, LANES + EXTRA, LANES)
    everyone = (tiles // 2, 2, bands // 2, 2) + part
    listed = (tiles, 2, tile_rows, LANES)
    if tiles > 8:
        sends = landings = tiles // 2 - 1 + 9
    else:
        sends, landings = 5 * tiles * 4, 2 * tiles * 4
    coupled, pick, entry_colors, window, chosen, data, data_places, places = pl.pallas_call(
        functools.partial(gather_kernel, tiles, bands, obs, list_len, rows, fields),
        out_shape=(
            jax.ShapeDtypeStruct(everyone, jnp.float32),
            jax.ShapeDtypeStruct((pack, reach, row_count, LANES), jnp.int32),
            jax.ShapeDtypeStruct((row_count, LANES), jnp.int32),
            jax.ShapeDtypeStruct((8, LANES), jnp.int32),
            jax.ShapeDtypeStruct((own_rows, 8, LANES), jnp.int32),
            jax.ShapeDtypeStruct((bands, 2, obs, mine * rows), jnp.float32),
            jax.ShapeDtypeStruct((bands, obs, mine * rows), jnp.int32),
            jax.ShapeDtypeStruct((obs, stars), jnp.int32),
        ),
        in_specs=[smem] + [vmem] * 6,
        out_specs=(hbm,) + (vmem,) * 7,
        scratch_shapes=[
            pltpu.VMEM(everyone, jnp.float32),
            pltpu.VMEM((row_count + 16, LANES), jnp.int32),
            pltpu.VMEM(part, jnp.float32),
            pltpu.VMEM((8, LANES), jnp.int32),
            pltpu.VMEM((8, LANES), jnp.int32),
            pltpu.VMEM(listed[1:], jnp.int32),
            pltpu.VMEM(listed, jnp.int32),
            pltpu.VMEM((bands, obs, mine * rows), jnp.int32),
            pltpu.SemaphoreType.DMA((sends,)),
            pltpu.SemaphoreType.DMA((landings,)),
            pltpu.SemaphoreType.DMA((earlier,)),
            pltpu.SemaphoreType.DMA((earlier,)),
            pltpu.SemaphoreType.DMA((6 + 3 * (tiles // 2),)),
            pltpu.SemaphoreType.DMA((8 + tiles,)),
            pltpu.SemaphoreType.DMA((tiles,)),
        ],
        compiler_params=pltpu.CompilerParams(
            collective_id=0, has_side_effects=True, vmem_limit_bytes=60 * 1024 * 1024
        ),
        name="gather",
    )(color_terms, block_fields, colors.reshape(-1, LANES), magnitudes, weights, slots, owner.reshape(-1, LANES))
    coupled = coupled.reshape((-1,) + coupled.shape[-2:])

    big = (bands, row_count, LANES)
    depth = min(row_count, 16)
    own_zp, star_means, sums = pl.pallas_call(
        functools.partial(sweep_kernel, tiles, bands, obs, list_len, rows, row_count),
        out_shape=(
            jax.ShapeDtypeStruct((1, owned), jnp.float32),
            jax.ShapeDtypeStruct((1, stars), jnp.float32),
            jax.ShapeDtypeStruct((8, LANES), jnp.float32),
        ),
        in_specs=[smem, smem, hbm] + [vmem] * 8,
        out_specs=(vmem,) * 3,
        scratch_shapes=[
            pltpu.VMEM((row_count * bands * LANES, LANES), jnp.float32),
            pltpu.VMEM(big, jnp.float32),
            pltpu.VMEM((bands, row_count + 16, LANES), jnp.float32),
            pltpu.VMEM(big, jnp.float32),
            pltpu.VMEM(big, jnp.float32),
            pltpu.VMEM(big, jnp.float32),
            pltpu.VMEM((LANES, LANES), jnp.float32),
            pltpu.VMEM((depth, bands, LANES + EXTRA, LANES), jnp.float32),
            pltpu.SemaphoreType.DMA((depth,)),
        ],
        compiler_params=pltpu.CompilerParams(vmem_limit_bytes=60 * 1024 * 1024),
        name="sweeps",
    )(window, color_terms, coupled, pick, entry_colors, data, data_places, magnitudes, weights, places, chosen)

    devices = tiles * bands
    misfit = pl.pallas_call(
        functools.partial(total_kernel, tiles, bands, float(obs * stars * tiles)),
        out_shape=jax.ShapeDtypeStruct((1, SWEEPS), jnp.float32),
        in_specs=[vmem],
        out_specs=vmem,
        scratch_shapes=[
            pltpu.VMEM((devices, LANES), jnp.float32),
            pltpu.SemaphoreType.DMA((devices - 1,)),
            pltpu.SemaphoreType.DMA((devices - 1,)),
        ],
        compiler_params=pltpu.CompilerParams(collective_id=1, has_side_effects=True),
        name="total",
    )(sums)
    return own_zp, star_means, misfit.reshape(SWEEPS, 1)


def solution(mesh):
    in_specs = (
        P("band", None, "sky"),
        P("band", None, "sky"),
        P("band", None, "sky"),
        P("sky", None),
        P(),
        P(),
        P(),
    )
    out_specs = (P("band", "sky"), P("band", "sky"), P(None, "band"))
    return jax.shard_map(body, mesh=mesh, in_specs=in_specs, out_specs=out_specs, check_vma=False)
```

```python
import functools

import jax
import jax.numpy as jnp
from jax import lax
from jax.experimental import pallas as pl
from jax.experimental.pallas import tpu as pltpu
from jax.sharding import PartitionSpec as P

COLORS = 8
SWEEPS = 4
PRIOR_WEIGHT = 1.0
REACH = 2
HIGHEST = lax.Precision.HIGHEST
LANES = 128
EXTRA = 8
MESH = pl.DeviceIdType.MESH


def contract_lanes(left, right):
    dims = (((1,), (1,)), ((), ()))
    return lax.dot_general(left, right, dims, precision=HIGHEST, preferred_element_type=jnp.float32)


def mixing_of(terms_ref, bands):
    mixing = []
    for band in range(bands):
        total = terms_ref[band, 0]
        for other in range(1, bands):
            total = total + terms_ref[band, other]
        row = [terms_ref[band, other] for other in range(bands)]
        row[band] = (1.0 + row[band]) - total
        mixing.append(row)
    return mixing


def mixed(mixing, band, means):
    predicted = mixing[band][0] * means[0]
    for other in range(1, len(means)):
        predicted = predicted + mixing[band][other] * means[other]
    return predicted


def couple(bands, obs, list_len, rows, terms_ref, data_ref, places_ref, out_ref):
    blocks = data_ref.shape[3] // rows
    mixing = mixing_of(terms_ref, bands)
    row_band = lax.broadcasted_iota(jnp.int32, (LANES, LANES), 0) // list_len
    lane_band = lax.broadcasted_iota(jnp.int32, (LANES, LANES), 1) // list_len
    mix_grid = jnp.zeros((LANES, LANES), jnp.float32)
    for band in range(bands):
        for other in range(bands):
            here = (row_band == other) & (lane_band == band)
            mix_grid = jnp.where(here, mixing[band][other], mix_grid)
    full = []
    entry = lax.broadcasted_iota(jnp.int32, (list_len, rows), 0)
    for block in range(blocks):
        cols = pl.ds(block * rows, rows)
        one_hot, one_hot_mag, star_weight, means = [], [], [], []
        for band in range(bands):
            mags = data_ref[band, 0, :, cols]
            wts = data_ref[band, 1, :, cols]
            slots = places_ref[band, :, cols]
            scaled = wts * mags
            weight_sum = jnp.sum(wts, axis=0, keepdims=True)
            star_weight.append(weight_sum)
            means.append(jnp.sum(scaled, axis=0, keepdims=True) / weight_sum)
            hot = jnp.zeros((list_len, rows), jnp.float32)
            hot_mag = jnp.zeros((list_len, rows), jnp.float32)
            for k in range(obs):
                hit = slots[k : k + 1] == entry
                hot = hot + jnp.where(hit, wts[k : k + 1], 0.0)
                hot_mag = hot_mag + jnp.where(hit, scaled[k : k + 1], 0.0)
            one_hot.append(hot)
            one_hot_mag.append(hot_mag)
        rest = []
        shares = []
        for band in range(bands):
            rest.append(one_hot_mag[band] - one_hot[band] * mixed(mixing, band, means))
            shares.append(one_hot[band] / star_weight[band])
        hot_all = jnp.concatenate(one_hot, axis=0)
        share_all = jnp.concatenate(shares, axis=0)
        rest_all = jnp.concatenate(rest, axis=0)
        coupling = contract_lanes(share_all, hot_all) * mix_grid
        ones = jnp.ones((8, rows), jnp.float32)
        rest_row = contract_lanes(ones, rest_all)
        weight_row = contract_lanes(ones, hot_all)
        first = lax.broadcasted_iota(jnp.int32, (EXTRA, LANES), 0) == 0
        full.append(jnp.concatenate([coupling, jnp.where(first, rest_row, weight_row)], axis=0))
    split = bands // 2
    for part in range(split):
        pieces = []
        for half in range(2):
            band = half * split + part
            for block in range(blocks):
                pieces.append(full[block][:, band * list_len : (band + 1) * list_len])
        out_ref[part] = jnp.concatenate(pieces, axis=1)


def sweep_kernel(
    tiles, bands, obs, list_len, rows, row_count,
    window_ref, terms_ref, coupled_ref, pick_ref, color_ref,
    data_ref, data_places_ref, mags_ref, wts_ref, places_ref, chosen_ref,
    own_zp_ref, means_ref, sums_ref,
    kt, base, tot, rden, zp, move, lines, stage, sems,
):
    groups = row_count // 8
    pack = LANES // list_len
    split = bands // 2
    levels, places = pick_ref.shape[:2]
    depth = stage.shape[0]
    lane = lax.broadcasted_iota(jnp.int32, (8, LANES), 1)
    lane_wide = lax.broadcasted_iota(jnp.int32, (LANES + EXTRA, LANES), 1)

    def fetch(row, slot):
        return pltpu.make_async_copy(
            coupled_ref.at[pl.ds(row * (2 * split), 2 * split)], stage.at[slot], sems.at[slot]
        )

    whole = depth == row_count
    for row in range(depth if whole else depth - 1):
        fetch(row, row).start()

    def unpack(row, carry):
        slot = lax.rem(row, depth)
        ahead = row + depth - 1

        if not whole:
            @pl.when(ahead < row_count)
            def _():
                fetch(ahead, lax.rem(ahead, depth)).start()

        fetch(row, slot).wait()
        group = lax.div(row, 8)
        place = lax.rem(row, 8)
        for part in range(split):
            left = stage[slot, part]
            right = stage[slot, split + part]
            low = jnp.where(lane_wide < LANES // 2, left, pltpu.roll(right, LANES // 2, 1))
            high = jnp.where(lane_wide < LANES // 2, pltpu.roll(left, LANES // 2, 1), right)
            for band, value in ((part, low), (split + part, high)):
                start = (group * bands + band) * (LANES * 8) + place
                kt[pl.ds(start, LANES, stride=8), :] = value[0:LANES]
                base[band, pl.ds(row, 1), :] = value[LANES : LANES + 1]
                tot[band, pl.ds(row + 8, 1), :] = value[LANES + 1 : LANES + 2]
        return carry

    lax.fori_loop(0, row_count, unpack, 0, unroll=2)

    def rows_of(group):
        return pl.ds(pl.multiple_of(group * 8, 8), 8)

    def wrap():
        for band in range(bands):
            tot[band, 0:8, :] = tot[band, row_count : row_count + 8, :]
            tot[band, row_count + 8 : row_count + 16, :] = tot[band, 8:16, :]

    def gather(group, first, count, sums):
        for place in range(places):
            start = group * 8 + (8 + place - places // 2)
            near = [tot[band, pl.ds(start, 8), :] for band in range(bands)]
            for level in range(count):
                pick = pick_ref[first + level, place, rows_of(group), :]
                mask = pick < LANES
                lanes = pick & (LANES - 1)
                for band in range(bands):
                    index = 2 * band + level % 2
                    sums[index] = sums[index] + jnp.where(mask, take(near[band], lanes), 0.0)
        return sums

    span = 2 if groups % 2 == 0 else 1

    def gathered(batch):
        around = [batch * span + part for part in range(span)]
        first = []
        for group in around:
            sums = []
            for band in range(bands):
                middle = pl.ds(pl.multiple_of(group * 8 + 8, 8), 8)
                sums += [tot[band, middle, :], jnp.zeros((8, LANES), jnp.float32)]
            first.append(gather(group, 0, 2, sums))

        def deeper(level, sums):
            return [gather(group, level, 1, part) for group, part in zip(around, sums)]

        result = lax.fori_loop(2, window_ref[0, 2], deeper, first)
        return [(group, [part[2 * b] + part[2 * b + 1] for b in range(bands)]) for group, part in zip(around, result)]

    def weigh(batch, carry):
        for group, values in gathered(batch):
            for band, value in enumerate(values):
                rden[band, rows_of(group), :] = 1.0 / (value + PRIOR_WEIGHT)
        return carry

    wrap()
    lax.fori_loop(0, groups // span, weigh, 0)
    zp[...] = jnp.zeros_like(zp)
    tot[:, 8 : row_count + 8, :] = base[...]
    wrap()

    def push(width, origin):
        def add(group, inner):
            here = [move[band, rows_of(group), :] for band in range(bands)]
            middle = pl.ds(pl.multiple_of(group * 8 + 8, 8), 8)
            sums = [tot[band, middle, :] for band in range(bands)]
            for entry in range(width):
                lanes = (lane & (LANES - list_len)) + (origin + entry)
                values = [take(here[band], lanes) for band in range(bands)]
                for band in range(bands):
                    for other in range(bands):
                        start = (group * bands + band) * (LANES * 8) + (other * list_len + origin + entry) * 8
                        rows = pl.ds(pl.multiple_of(start, 8), 8)
                        sums[band] = sums[band] + values[other] * kt[rows, :]
            for band in range(bands):
                tot[band, middle, :] = sums[band]
            return inner

        lax.fori_loop(0, groups, add, 0, unroll=2)

    halves = rows // LANES
    stars = mags_ref.shape[1]
    blocks = stars // rows
    tile_rows = blocks // pack
    mine = data_ref.shape[3] // rows
    my_tile, my_band = lax.axis_index("sky"), lax.axis_index("band")
    first = lax.rem(my_band * mine, pack)
    my_row = my_tile * tile_rows + lax.div(my_band * mine, pack)
    mixing = mixing_of(terms_ref, bands)
    lines[...] = jnp.zeros_like(lines)

    def spread(row, picks):
        return take(jnp.broadcast_to(row, (obs, LANES)), picks)

    def misfit_lines(sweep):
        partial = [jnp.zeros((obs, LANES), jnp.float32) for _ in range(bands)]
        for block in range(mine):
            for half in range(halves):
                cols = pl.ds(block * rows + half * LANES, LANES)
                left, means = [], []
                for band in range(bands):
                    wts = data_ref[band, 1, :, cols]
                    picks = data_places_ref[band, :, cols] + (first + block) * list_len
                    mags = data_ref[band, 0, :, cols] - spread(zp[band, pl.ds(my_row, 1), :], picks)
                    left.append(mags)
                    means.append(jnp.sum(wts * mags, axis=0, keepdims=True) / jnp.sum(wts, axis=0, keepdims=True))
                for band in range(bands):
                    wts = data_ref[band, 1, :, cols]
                    partial[band] = partial[band] + wts * (left[band] - mixed(mixing, band, means)) ** 2
        for band in range(bands):
            lines[pl.ds(sweep * bands + band, 1), :] = jnp.sum(partial[band], axis=0, keepdims=True)

    def step(number, carry):
        color_no = lax.rem(number, COLORS)

        def update(batch, inner):
            for group, values in gathered(batch):
                rows = rows_of(group)
                now = color_ref[rows, :] == color_no
                for band, value in enumerate(values):
                    old = zp[band, rows, :]
                    new = jnp.where(now, value * rden[band, rows, :], old)
                    zp[band, rows, :] = new
                    move[band, rows, :] = new - old
            return inner

        lax.fori_loop(0, groups // span, update, 0)

        @pl.when(color_no == COLORS - 1)
        def _():
            misfit_lines(lax.div(number, COLORS))

        low, high = window_ref[color_no, 0], window_ref[color_no, 1]
        widths = [list_len * eighths // 16 for eighths in range(4, 9)]
        more = number < SWEEPS * COLORS - 1
        for index, width in enumerate(widths):
            fits = more & (high - low <= width)
            if index:
                fits = fits & (high - low > widths[index - 1])

            @pl.when(fits)
            def _(width=width):
                push(width, jnp.minimum(low, list_len - width))

        @pl.when(more & (high - low > widths[-1]))
        def _():
            lax.fori_loop(0, 2, lambda part, inner: (push(widths[-1], part * widths[-1]), inner)[1], 0)

        wrap()
        return carry

    lax.fori_loop(0, SWEEPS * COLORS, step, 0)
    sums_ref[...] = contract_lanes(jnp.ones((8, LANES), jnp.float32), lines[...])
    for block in range(blocks):
        row = zp[my_band, pl.ds(my_tile * tile_rows + block // pack, 1), :]
        for half in range(halves):
            cols = pl.ds(block * rows + half * LANES, LANES)
            wts = wts_ref[:, cols]
            picks = places_ref[:, cols] + block % pack * list_len
            left = wts * (mags_ref[:, cols] - spread(row, picks))
            means_ref[0:1, cols] = jnp.sum(left, axis=0, keepdims=True) / jnp.sum(wts, axis=0, keepdims=True)
    below = lax.broadcasted_iota(jnp.int32, (8, LANES), 0)
    close = jnp.zeros((8, LANES), jnp.float32)
    for offset in range(3):
        tile = lax.rem(my_tile + offset + tiles - 1, tiles)
        for row in range(tile_rows):
            value = zp[my_band, pl.ds(tile * tile_rows + row, 1), :]
            close = jnp.where(below == offset * tile_rows + row, jnp.broadcast_to(value, (8, LANES)), close)
    owned = own_zp_ref.shape[1]
    for row in range(chosen_ref.shape[0]):
        pick = chosen_ref[row]
        value = jnp.where(pick < LANES, take(close, pick & (LANES - 1)), 0.0)
        value = jnp.sum(value, axis=0, keepdims=True)
        width = min(LANES, owned - row * LANES)
        own_zp_ref[0:1, row * LANES : row * LANES + width] = value[:, 0:width]


def take(value, picks):
    return jnp.take_along_axis(value, picks, axis=1, mode="promise_in_bounds")


def sort_entries(list_len, fields, listed, color_ref):
    lane = lax.broadcasted_iota(jnp.int32, (8, LANES), 1)
    segment = lane & (LANES - list_len)
    live = listed < fields
    row_no, lane_no = listed // LANES, listed % LANES
    color = jnp.full((8, LANES), -1, jnp.int32)
    for row in range(color_ref.shape[0]):
        table = jnp.broadcast_to(color_ref[row : row + 1, :], (8, LANES))
        color = jnp.where(row_no == row, take(table, lane_no), color)
    color = jnp.where(live, color, -1)
    masks = jnp.concatenate([(color == c).astype(jnp.float32) for c in range(COLORS)], axis=0)
    source = lax.broadcasted_iota(jnp.int32, (LANES, LANES), 0)
    target = lax.broadcasted_iota(jnp.int32, (LANES, LANES), 1)
    same = (source // list_len) == (target // list_len)
    dims = (((1,), (0,)), ((), ()))
    before = (same & (source < target)).astype(jnp.float32)
    ranks = lax.dot_general(masks, before, dims, preferred_element_type=jnp.float32)
    counts = lax.dot_general(masks, same.astype(jnp.float32), dims, preferred_element_type=jnp.float32)
    rest = jnp.zeros((8, LANES), jnp.float32)
    room = [None] * COLORS
    for c in reversed(range(COLORS)):
        rest = rest + counts[c * 8 : c * 8 + 8]
        room[c] = list_len - rest
    end = jnp.zeros((8, LANES), jnp.float32)
    place = jnp.full((8, LANES), -1.0, jnp.float32)
    for c in range(COLORS):
        start = jnp.minimum(jnp.maximum(end, float(list_len * c // COLORS)), room[c])
        end = start + counts[c * 8 : c * 8 + 8]
        place = jnp.where(color == c, start + ranks[c * 8 : c * 8 + 8], place)
    place = place.astype(jnp.int32)
    sorted_fields = jnp.full((8, LANES), fields, jnp.int32)
    sorted_colors = jnp.full((8, LANES), -1, jnp.int32)
    for entry in range(list_len):
        picks = segment + entry
        hit = take(place, picks) == lane - segment
        sorted_fields = jnp.where(hit, take(listed, picks), sorted_fields)
        sorted_colors = jnp.where(hit, take(color, picks), sorted_colors)
    return place, sorted_fields, sorted_colors


def match(list_len, fields, lists_ref, rows_ref, pick_ref, color_ref):
    tiles, _, tile_rows, _ = lists_ref.shape
    pack = LANES // list_len
    levels, places, row_count, _ = pick_ref.shape
    lane = lax.broadcasted_iota(jnp.int32, (8, LANES), 1)
    for tile in range(tiles):
        start = tile * tile_rows
        rows_ref[8 + start : 8 + start + tile_rows, :] = lists_ref[tile, 0]
        color_ref[start : start + tile_rows, :] = lists_ref[tile, 1]
    rows_ref[0:8, :] = rows_ref[row_count : row_count + 8, :]
    rows_ref[row_count + 8 : row_count + 16, :] = rows_ref[8:16, :]

    def group_picks(group, carry):
        home = rows_ref[pl.ds(pl.multiple_of(group * 8 + 8, 8), 8), :]
        home = jnp.where(home < fields, home, -1)
        near = [rows_ref[pl.ds(group * 8 + 8 + place - places // 2, 8), :] for place in range(places)]
        found = [[] for _ in range(places)]
        for quarter in range(pack):
            picks = [jnp.full((8, LANES), LANES, jnp.int32) for _ in range(places)]
            for entry in range(list_len):
                source = quarter * list_len + entry
                for place in range(places):
                    other = jnp.broadcast_to(near[place][:, source : source + 1], (8, LANES))
                    picks[place] = jnp.where(other == home, source, picks[place])
            for place in range(places):
                found[place].append(picks[place])
        rows = pl.ds(pl.multiple_of(group * 8, 8), 8)
        for place in range(places):
            ranked = found[place]
            if place == places // 2:
                ranked = [jnp.where(pick == lane, LANES, pick) for pick in ranked]
            for turn in range(pack):
                for low in range(turn % 2, pack - 1, 2):
                    pair = ranked[low], ranked[low + 1]
                    ranked[low], ranked[low + 1] = jnp.minimum(*pair), jnp.maximum(*pair)
            for level in range(pack):
                pick_ref[level, place, rows, :] = ranked[level]
        return carry

    lax.fori_loop(0, row_count // 8, group_picks, 0)


def windows(list_len, pick_ref, color_ref, window_ref):
    levels, places, row_count, _ = pick_ref.shape
    lane = lax.broadcasted_iota(jnp.int32, (8, LANES), 1)
    position = (lane & (list_len - 1)).astype(jnp.float32)

    def rows_of(group):
        return pl.ds(pl.multiple_of(group * 8, 8), 8)

    def bounds(group, carry):
        lows, highs = carry
        color = color_ref[rows_of(group), :]
        new_lows, new_highs = [], []
        for c in range(COLORS):
            new_lows.append(jnp.minimum(lows[c], jnp.where(color == c, position, float(list_len))))
            new_highs.append(jnp.maximum(highs[c], jnp.where(color == c, position + 1.0, 0.0)))
        return new_lows, new_highs

    start = [jnp.full((8, LANES), float(list_len), jnp.float32)] * COLORS, [jnp.zeros((8, LANES), jnp.float32)] * COLORS
    lows, highs = lax.fori_loop(0, row_count // 8, bounds, start)
    lows = jnp.concatenate([jnp.min(value, axis=0, keepdims=True) for value in lows], axis=0)
    highs = jnp.concatenate([jnp.max(value, axis=0, keepdims=True) for value in highs], axis=0)
    lows = jnp.min(lows, axis=1, keepdims=True)
    highs = jnp.max(highs, axis=1, keepdims=True)
    deepest = jnp.full((8, LANES), 2.0, jnp.float32)
    for level in range(2, levels):
        def least(group, value, level=level):
            for place in range(places):
                value = jnp.minimum(value, pick_ref[level, place, rows_of(group), :])
            return value

        found = lax.fori_loop(0, row_count // 8, least, jnp.full((8, LANES), LANES, jnp.int32))
        deepest = jnp.where(found < LANES, level + 1.0, deepest)
    deepest = jnp.max(jnp.max(deepest, axis=0, keepdims=True), axis=1, keepdims=True)
    table = jnp.where(lane == 0, lows, jnp.where(lane == 1, highs, deepest))
    window_ref[...] = table.astype(jnp.int32)


def choose(tiles, fields, owner_ref, rows_ref, chosen_ref):
    field_rows = owner_ref.shape[0]
    tile_rows = (rows_ref.shape[0] - 16) // tiles
    my_tile = lax.axis_index("sky")
    lane = lax.broadcasted_iota(jnp.int32, (8, LANES), 1)
    below = lax.broadcasted_iota(jnp.int32, (8, LANES), 0)
    owned = owner_ref[...] == my_tile
    ones = owned.astype(jnp.float32)
    source = lax.broadcasted_iota(jnp.int32, (LANES, LANES), 0)
    target = lax.broadcasted_iota(jnp.int32, (LANES, LANES), 1)
    dims = (((1,), (0,)), ((), ()))
    inside = lax.dot_general(ones, (source < target).astype(jnp.float32), dims, preferred_element_type=jnp.float32)
    counts = lax.dot_general(ones, jnp.ones((LANES, LANES), jnp.float32), dims, preferred_element_type=jnp.float32)
    upper = lax.broadcasted_iota(jnp.int32, (field_rows, field_rows), 1)
    lower = lax.broadcasted_iota(jnp.int32, (field_rows, field_rows), 0)
    above = lax.dot_general((upper < lower).astype(jnp.float32), counts, dims, preferred_element_type=jnp.float32)
    rank = jnp.where(owned, (inside + above).astype(jnp.int32), -1)
    close = jnp.full((8, LANES), fields, jnp.int32)
    for offset in range(3):
        tile = lax.rem(my_tile + offset + tiles - 1, tiles)
        for row in range(tile_rows):
            value = rows_ref[pl.ds(8 + tile * tile_rows + row, 1), :]
            close = jnp.where(below == offset * tile_rows + row, jnp.broadcast_to(value, (8, LANES)), close)
    row_no, lane_no = close // LANES, close % LANES
    order = jnp.full((8, LANES), -1, jnp.int32)
    for row in range(field_rows):
        table = jnp.broadcast_to(rank[row : row + 1, :], (8, LANES))
        order = jnp.where(row_no == row, take(table, lane_no), order)
    own_rows = chosen_ref.shape[0]
    codes = [jnp.full((8, LANES), -1, jnp.int32) for _ in range(own_rows)]
    for entry in range(LANES):
        value = jnp.broadcast_to(order[:, entry : entry + 1], (8, LANES))
        for row in range(own_rows):
            codes[row] = jnp.where(value == row * LANES + lane, entry, codes[row])
    for row in range(own_rows):
        ranked = jnp.where(codes[row] >= 0, (below + 1).astype(jnp.float32), 0.0)
        last = jnp.max(ranked, axis=0, keepdims=True)
        keep = (ranked > 0.0) & (ranked == last)
        chosen_ref[row] = jnp.where(keep, codes[row], LANES)


def relabel(list_len, rows, block, offset, place_ref, slots_ref, out_ref):
    pack = LANES // list_len
    table = jnp.broadcast_to(place_ref[pl.ds(block // pack, 1), :], (slots_ref.shape[0], LANES))
    for half in range(rows // LANES):
        cols = pl.ds(offset + half * LANES, LANES)
        out_ref[:, cols] = take(table, slots_ref[:, cols] + block % pack * list_len)


def gather_kernel(
    tiles, bands, obs, list_len, rows, fields,
    terms_ref, tile_lists_ref, field_colors_ref, mags_ref, wts_ref, slots_ref, owner_ref,
    out_ref, pick_ref, color_ref, window_ref, chosen_ref, data_ref, data_places_ref, places_ref,
    all_ref, rows_ref, own_ref, listed_ref, place_ref, sorted_ref, lists_ref, data_slots_ref,
    send_sems, recv_sems, early_send_sems, early_recv_sems, plane_send_sems, plane_recv_sems, save_sems,
):
    high_count = tiles // 2
    blocks = tile_lists_ref.shape[0]
    pack = LANES // list_len
    tile_rows = blocks // pack
    mine = blocks // bands
    width = mine * rows
    sky, band = lax.axis_index("sky"), lax.axis_index("band")
    high, low = sky // 2, sky % 2
    side, core = band // 2, band % 2
    to_low = {"sky": high * 2 + (1 - low)}
    to_side = {"band": (1 - side) * 2 + core}
    to_core = {"band": side * 2 + (1 - core)}
    barrier = pltpu.get_barrier_semaphore()
    tile_peers = [lax.rem(sky + step, tiles) for step in range(1, tiles)]
    band_peers = [lax.rem(band + step, bands) for step in range(1, bands)]
    for peer in tile_peers:
        pl.semaphore_signal(barrier, inc=1, device_id={"sky": peer}, device_id_type=MESH)
    for peer in band_peers:
        pl.semaphore_signal(barrier, inc=1, device_id={"band": peer}, device_id_type=MESH)

    listed_ref[...] = jnp.full((8, LANES), fields, jnp.int32)
    for row in range(tile_rows):
        pieces = [tile_lists_ref[row * pack + part : row * pack + part + 1, :] for part in range(pack)]
        listed_ref[row : row + 1, :] = jnp.concatenate(pieces, axis=1)
    place, sorted_fields, sorted_colors = sort_entries(list_len, fields, listed_ref[...], field_colors_ref)
    place_ref[...] = place
    sorted_ref[0] = sorted_fields[0:tile_rows]
    sorted_ref[1] = sorted_colors[0:tile_rows]
    lists_ref[sky] = sorted_ref[...]
    pl.semaphore_wait(barrier, tiles + bands - 2)

    def early(number, source, target, device):
        copy = pltpu.make_async_remote_copy(
            src_ref=source,
            dst_ref=target,
            send_sem=early_send_sems.at[number],
            recv_sem=early_recv_sems.at[number],
            device_id=device,
            device_id_type=MESH,
        )
        copy.start()
        return copy

    def columns(peer):
        return pl.ds(pl.multiple_of(peer * width, LANES), width)

    data_copies, list_copies = [], []
    for step, peer in enumerate(band_peers):
        cols = columns(peer)
        for kind, (source, target) in enumerate((
            (slots_ref, data_slots_ref.at[band]),
            (wts_ref, data_ref.at[band, 1]),
            (mags_ref, data_ref.at[band, 0]),
        )):
            data_copies.append(early(3 * step + kind, source.at[:, cols], target, {"band": peer}))
    for step, peer in enumerate(tile_peers):
        list_copies.append(early(3 * (bands - 1) + step, sorted_ref, lists_ref.at[sky], {"sky": peer}))
    data_ref[band, 0] = mags_ref[:, columns(band)]
    data_ref[band, 1] = wts_ref[:, columns(band)]
    data_slots_ref[band] = slots_ref[:, columns(band)]
    for block in range(blocks):
        relabel(list_len, rows, block, block * rows, place_ref, slots_ref, places_ref)
    for copy in data_copies:
        copy.wait_recv()
    for other in range(bands):
        for block in range(mine):
            source, target = data_slots_ref.at[other], data_places_ref.at[other]
            relabel(list_len, rows, band * mine + block, block * rows, place_ref, source, target)

    def tables():
        for copy in list_copies:
            copy.wait_recv()
        match(list_len, fields, lists_ref, rows_ref, pick_ref, color_ref)

    def more_tables():
        windows(list_len, pick_ref, color_ref, window_ref)
        choose(tiles, fields, owner_ref, rows_ref, chosen_ref)
        for copy in data_copies + list_copies:
            copy.wait_send()

    if high_count > 4:
        highs = [lax.rem(high + step, high_count) for step in range(1, high_count)]
        peers = [{"sky": peer * 2 + low} for peer in highs]
        couple(bands, obs, list_len, rows, terms_ref, data_ref, data_places_ref, own_ref)
        count = [0]

        def send(source, target, peer):
            copy = pltpu.make_async_remote_copy(
                src_ref=source,
                dst_ref=target,
                send_sem=send_sems.at[count[0]],
                recv_sem=recv_sems.at[count[0]],
                device_id=peer,
                device_id_type=MESH,
            )
            count[0] += 1
            copy.start()
            return copy

        def wait(copies):
            for copy in copies:
                copy.wait()

        mine = all_ref.at[high, low, side, core]
        copies = [send(own_ref, mine, peer) for peer in peers]
        all_ref[high, low, side, core] = own_ref[...]
        tables()
        more_tables()
        wait(copies)

        column = all_ref.at[:, low, side, core]
        first = all_ref.at[:, low, side, core, 0]
        second = all_ref.at[:, low, side, core, 1]
        copies = [send(first, first, to_low), send(second, second, to_side)]
        late = [send(column, column, to_core)]
        wait(copies)

        first = all_ref.at[:, :, side, core, 0]
        second = all_ref.at[:, low, :, core, 1]
        copies = [send(first, first, to_side), send(second, second, to_low)]
        for part in (all_ref.at[:, 1 - low, side, core, 0], all_ref.at[:, low, 1 - side, core, 1]):
            late.append(send(part, part, to_core))
        wait(copies)

        for part in (all_ref.at[:, :, 1 - side, core, 0], all_ref.at[:, 1 - low, :, core, 1]):
            late.append(send(part, part, to_core))
        wait(late)
        save = pltpu.make_async_copy(all_ref, out_ref, save_sems.at[0])
        save.start()
        save.wait()
        return

    chunks = high_count * 8
    lower, upper = high > 0, high < high_count - 1
    own_chunk = all_ref.at[high, low, side, core]
    couple(bands, obs, list_len, rows, terms_ref, data_ref, data_places_ref, own_chunk)
    depth = all_ref.shape[5]
    ahead = depth // 32 * 8

    def copy_of(kind, z, y, x, part, peer, landing):
        chunk = all_ref.at[z, y, x, core, part, ahead:depth]
        number = ((z * 2 + y) * 2 + x) * 2 + part
        return pltpu.make_async_remote_copy(
            src_ref=chunk,
            dst_ref=chunk,
            send_sem=send_sems.at[kind * chunks + number],
            recv_sem=recv_sems.at[landing * chunks + number],
            device_id=peer,
            device_id_type=MESH,
        )

    def plane_copy(chunk, number, landing, peer):
        return pltpu.make_async_remote_copy(
            src_ref=chunk,
            dst_ref=chunk,
            send_sem=plane_send_sems.at[number],
            recv_sem=plane_recv_sems.at[landing],
            device_id=peer,
            device_id_type=MESH,
        )

    def head_x(y, part, number):
        chunk = all_ref.at[high, y, side, core, part, 0:ahead]
        return plane_copy(chunk, number, (y * 2 + side) * 2 + part, to_side)

    def head_y(x, part, number):
        chunk = all_ref.at[high, low, x, core, part, 0:ahead]
        return plane_copy(chunk, number, (low * 2 + x) * 2 + part, to_low)

    def head_arrived(y, x, part):
        chunk = all_ref.at[high, y, x, core, part, 0:ahead]
        plane_copy(chunk, 0, (y * 2 + x) * 2 + part, to_core).wait_recv()

    def plane_along(z, step):
        chunk = all_ref.at[z, :, :, core, :, 0:ahead]
        number = 6 + high_count * ((step + 1) // 2) + z
        return plane_copy(chunk, number, 8 + z, {"sky": (high + step) * 2 + low})

    def plane_over(z):
        chunk = all_ref.at[z, :, :, core, :, 0:ahead]
        return plane_copy(chunk, 6 + 2 * high_count + z, 8 + high_count + z, to_core)

    def along(z, part, step):
        return copy_of((step + 1) // 2, z, low, side, part, {"sky": (high + step) * 2 + low}, 0)

    def across_x(z, y, part):
        return copy_of(2, z, y, side, part, to_side, 0)

    def across_y(z, x, part):
        return copy_of(3, z, low, x, part, to_low, 0)

    def over(z, y, x, part):
        return copy_of(4, z, y, x, part, to_core, 1)

    def arrived(z, y, x, part):
        copy_of(4, z, y, x, part, to_core, 0).wait_recv()

    ends = {-1: lower, 1: upper}

    def along_if(z, part, step):
        @pl.when(ends[step])
        def _():
            along(z, part, step).start()

    def first_hop(z, part):
        if part == 0:
            across_x(z, low, part).start()
        else:
            across_y(z, side, part).start()

    def second_hop(z, part):
        if part == 0:
            across_y(z, side, part).start()
        else:
            across_x(z, low, part).start()

    head_x(low, 0, 0).start()
    head_y(side, 1, 3).start()
    for part in range(2):
        along_if(high, part, 1)
        along_if(high, part, -1)
        first_hop(high, part)
        if part == 0:
            head_y(side, 0, 4).start()
            head_x(low, 1, 1).start()
    for part in range(2):
        second_hop(high, part)
        over(high, low, side, part).start()
    tables()

    def heads_turn():
        head_arrived(low, 1 - side, 0)
        head_y(1 - side, 0, 5).start()
        head_arrived(1 - low, side, 1)
        head_x(1 - low, 1, 2).start()

    def send_plane(z, steps):
        for step in steps:
            @pl.when(ends[step])
            def _(step=step):
                plane_along(z, step).start()

        plane_over(z).start()

    def heads_done():
        for y, x, part in ((1 - low, side, 0), (low, 1 - side, 1), (1 - low, 1 - side, 0), (1 - low, 1 - side, 1)):
            head_arrived(y, x, part)
        send_plane(high, (-1, 1))

    def plane_arrival(distance):
        for step in (-1, 1):
            z = high - step * distance

            @pl.when(z >= 0 if step == 1 else z < high_count)
            def _(z=z, step=step):
                plane_copy(all_ref.at[z, :, :, core, :, 0:ahead], 0, 8 + z, to_core).wait_recv()
                send_plane(z, (step,))

    def column_arrival(distance, part):
        for step in (-1, 1):
            z = high - step * distance
            here = z >= 0 if step == 1 else z < high_count

            @pl.when(here)
            def _(z=z, step=step):
                arrived(z, low, side, part)
                along_if(z, part, step)
                first_hop(z, part)
                second_hop(z, part)
                over(z, low, side, part).start()

    def at_distance(distance, action):
        if distance == 0:
            action(high)
            return
        for step in (-1, 1):
            z = high - step * distance

            @pl.when(z >= 0 if step == 1 else z < high_count)
            def _(z=z):
                action(z)

    def turn(z):
        arrived(z, low, 1 - side, 0)
        across_y(z, 1 - side, 0).start()
        over(z, low, 1 - side, 0).start()
        arrived(z, 1 - low, side, 1)
        across_x(z, 1 - low, 1).start()
        over(z, 1 - low, side, 1).start()

    def last(z):
        for y, x, part in ((1 - low, side, 0), (low, 1 - side, 1), (1 - low, 1 - side, 0), (1 - low, 1 - side, 1)):
            arrived(z, y, x, part)
            over(z, y, x, part).start()

    def save(z, k):
        return pltpu.make_async_copy(all_ref.at[z, :, :, k], out_ref.at[z, :, :, k], save_sems.at[z * 2 + k])

    def save_own(z):
        save(z, core).start()

    def save_other(z):
        for y in range(2):
            for x in range(2):
                for part in range(2):
                    copy_of(4, z, y, x, part, to_core, 1).wait_recv()
        plane_over(z).wait_recv()
        save(z, 1 - core).start()

    heads_turn()
    for distance in range(1, high_count):
        column_arrival(distance, 0)
        at_distance(distance - 1, turn)
        column_arrival(distance, 1)
        if distance == 1:
            heads_done()
            more_tables()
        else:
            plane_arrival(distance - 1)
            at_distance(distance - 2, last)
            at_distance(distance - 2, save_own)
    at_distance(high_count - 1, turn)
    plane_arrival(high_count - 1)
    for distance in range(max(high_count - 2, 0), high_count):
        at_distance(distance, last)
        at_distance(distance, save_own)
    for distance in range(high_count):
        at_distance(distance, save_other)
    for z in range(high_count):
        for y in range(2):
            for x in range(2):
                for part in range(2):
                    copy_of(4, z, y, x, part, to_core, 1).wait_send()
        plane_over(z).wait_send()
        for step in (-1, 1):
            passing = (z >= high) if step == -1 else (z <= high)

            @pl.when(ends[step] & passing)
            def _(z=z, step=step):
                plane_along(z, step).wait_send()

    for y, part, number in ((low, 0, 0), (low, 1, 1), (1 - low, 1, 2)):
        head_x(y, part, number).wait_send()
    for x, part, number in ((side, 1, 3), (side, 0, 4), (1 - side, 0, 5)):
        head_y(x, part, number).wait_send()
    for z in range(high_count):
        for part in range(2):
            for step in (-1, 1):
                passing = (z >= high) if step == -1 else (z <= high)

                @pl.when(ends[step] & passing)
                def _(z=z, part=part, step=step):
                    along(z, part, step).wait_send()

            for other in range(2):
                if part == 0:
                    across_y(z, other, part).wait_send()
                else:
                    across_x(z, other, part).wait_send()
            first = across_x(z, low, part) if part == 0 else across_y(z, side, part)
            first.wait_send()
    for z in range(high_count):
        for k in range(2):
            save(z, k).wait()


def total_kernel(tiles, bands, scale, sums_ref, misfit_ref, all_sums, send_sems, recv_sems):
    my_tile, my_band = lax.axis_index("sky"), lax.axis_index("band")
    me = my_tile * bands + my_band
    peers = []
    for sky_step in range(tiles):
        for band_step in range(bands):
            if sky_step or band_step:
                peers.append({"sky": lax.rem(my_tile + sky_step, tiles), "band": lax.rem(my_band + band_step, bands)})
    barrier = pltpu.get_barrier_semaphore()
    for peer in peers:
        pl.semaphore_signal(barrier, inc=1, device_id=peer, device_id_type=MESH)
    all_sums[pl.ds(me, 1), :] = sums_ref[0:1, :]
    pl.semaphore_wait(barrier, len(peers))
    copies = []
    for number, peer in enumerate(peers):
        copy = pltpu.make_async_remote_copy(
            src_ref=sums_ref.at[0:1],
            dst_ref=all_sums.at[pl.ds(me, 1)],
            send_sem=send_sems.at[number],
            recv_sem=recv_sems.at[number],
            device_id=peer,
            device_id_type=MESH,
        )
        copy.start()
        copies.append(copy)
    for copy in copies:
        copy.wait()
    total = jnp.sum(all_sums[...], axis=0, keepdims=True) / scale
    lane = lax.broadcasted_iota(jnp.int32, (8, LANES), 1)
    picks = (lane * bands + my_band) & (LANES - 1)
    misfit_ref[...] = take(jnp.broadcast_to(total, (8, LANES)), picks)[0:1, 0:SWEEPS]


def body(magnitudes, weights, slots, block_fields, owner, colors, color_terms):
    bands = color_terms.shape[0]
    tiles = lax.axis_size("sky")
    _, obs, stars = magnitudes.shape
    blocks, list_len = block_fields.shape
    rows = stars // blocks
    fields = owner.shape[0]
    owned = fields // tiles
    mine = blocks // bands
    pack = LANES // list_len
    tile_rows = blocks // pack
    row_count = tiles * tile_rows
    vmem = pl.BlockSpec(memory_space=pltpu.VMEM)
    smem = pl.BlockSpec(memory_space=pltpu.SMEM)
    hbm = pl.BlockSpec(memory_space=pl.ANY)
    magnitudes, weights, slots = magnitudes[0], weights[0], slots[0]

    earlier = 3 * (bands - 1) + tiles - 1
    reach = 2 * (REACH * tile_rows + tile_rows - 1) + 1
    own_rows = -(-owned // LANES)
    part = (bands // 2, LANES + EXTRA, LANES)
    everyone = (tiles // 2, 2, bands // 2, 2) + part
    listed = (tiles, 2, tile_rows, LANES)
    if tiles > 8:
        sends = landings = tiles // 2 - 1 + 9
    else:
        sends, landings = 5 * tiles * 4, 2 * tiles * 4
    coupled, pick, entry_colors, window, chosen, data, data_places, places = pl.pallas_call(
        functools.partial(gather_kernel, tiles, bands, obs, list_len, rows, fields),
        out_shape=(
            jax.ShapeDtypeStruct(everyone, jnp.float32),
            jax.ShapeDtypeStruct((pack, reach, row_count, LANES), jnp.int32),
            jax.ShapeDtypeStruct((row_count, LANES), jnp.int32),
            jax.ShapeDtypeStruct((8, LANES), jnp.int32),
            jax.ShapeDtypeStruct((own_rows, 8, LANES), jnp.int32),
            jax.ShapeDtypeStruct((bands, 2, obs, mine * rows), jnp.float32),
            jax.ShapeDtypeStruct((bands, obs, mine * rows), jnp.int32),
            jax.ShapeDtypeStruct((obs, stars), jnp.int32),
        ),
        in_specs=[smem] + [vmem] * 6,
        out_specs=(hbm,) + (vmem,) * 7,
        scratch_shapes=[
            pltpu.VMEM(everyone, jnp.float32),
            pltpu.VMEM((row_count + 16, LANES), jnp.int32),
            pltpu.VMEM(part, jnp.float32),
            pltpu.VMEM((8, LANES), jnp.int32),
            pltpu.VMEM((8, LANES), jnp.int32),
            pltpu.VMEM(listed[1:], jnp.int32),
            pltpu.VMEM(listed, jnp.int32),
            pltpu.VMEM((bands, obs, mine * rows), jnp.int32),
            pltpu.SemaphoreType.DMA((sends,)),
            pltpu.SemaphoreType.DMA((landings,)),
            pltpu.SemaphoreType.DMA((earlier,)),
            pltpu.SemaphoreType.DMA((earlier,)),
            pltpu.SemaphoreType.DMA((6 + 3 * (tiles // 2),)),
            pltpu.SemaphoreType.DMA((8 + tiles,)),
            pltpu.SemaphoreType.DMA((tiles,)),
        ],
        compiler_params=pltpu.CompilerParams(
            collective_id=0, has_side_effects=True, vmem_limit_bytes=60 * 1024 * 1024
        ),
        name="gather",
    )(color_terms, block_fields, colors.reshape(-1, LANES), magnitudes, weights, slots, owner.reshape(-1, LANES))
    coupled = coupled.reshape((-1,) + coupled.shape[-2:])

    big = (bands, row_count, LANES)
    depth = min(row_count, 16)
    own_zp, star_means, sums = pl.pallas_call(
        functools.partial(sweep_kernel, tiles, bands, obs, list_len, rows, row_count),
        out_shape=(
            jax.ShapeDtypeStruct((1, owned), jnp.float32),
            jax.ShapeDtypeStruct((1, stars), jnp.float32),
            jax.ShapeDtypeStruct((8, LANES), jnp.float32),
        ),
        in_specs=[smem, smem, hbm] + [vmem] * 8,
        out_specs=(vmem,) * 3,
        scratch_shapes=[
            pltpu.VMEM((row_count * bands * LANES, LANES), jnp.float32),
            pltpu.VMEM(big, jnp.float32),
            pltpu.VMEM((bands, row_count + 16, LANES), jnp.float32),
            pltpu.VMEM(big, jnp.float32),
            pltpu.VMEM(big, jnp.float32),
            pltpu.VMEM(big, jnp.float32),
            pltpu.VMEM((LANES, LANES), jnp.float32),
            pltpu.VMEM((depth, bands, LANES + EXTRA, LANES), jnp.float32),
            pltpu.SemaphoreType.DMA((depth,)),
        ],
        compiler_params=pltpu.CompilerParams(vmem_limit_bytes=60 * 1024 * 1024),
        name="sweeps",
    )(window, color_terms, coupled, pick, entry_colors, data, data_places, magnitudes, weights, places, chosen)

    devices = tiles * bands
    misfit = pl.pallas_call(
        functools.partial(total_kernel, tiles, bands, float(obs * stars * tiles)),
        out_shape=jax.ShapeDtypeStruct((1, SWEEPS), jnp.float32),
        in_specs=[vmem],
        out_specs=vmem,
        scratch_shapes=[
            pltpu.VMEM((devices, LANES), jnp.float32),
            pltpu.SemaphoreType.DMA((devices - 1,)),
            pltpu.SemaphoreType.DMA((devices - 1,)),
        ],
        compiler_params=pltpu.CompilerParams(collective_id=1, has_side_effects=True),
        name="total",
    )(sums)
    return own_zp, star_means, misfit.reshape(SWEEPS, 1)


def solution(mesh):
    in_specs = (
        P("band", None, "sky"),
        P("band", None, "sky"),
        P("band", None, "sky"),
        P("sky", None),
        P(),
        P(),
        P(),
    )
    out_specs = (P("band", "sky"), P("band", "sky"), P(None, "band"))
    return jax.shard_map(body, mesh=mesh, in_specs=in_specs, out_specs=out_specs, check_vma=False)
```
